32 devices in a mesh: groups: 2 (over y), dp: 4 (over z), mp: 4 (over x, core).
Axes of the slice: x: 2, y: 2, z: 4, core: 2. Of those that a mesh axis runs over, the one named last changes fastest.
Arguments:
- tokens: bfloat16 [1024, 7168], P(('groups', 'dp')), parts along dimension 0, may hold values from -20 to 20, as said below
- w_down: bfloat16 [7168, 1536], P('dp', 'mp'), may hold values from -3 to 3, as said below
- gain: float32 [1536], P('mp'), may hold values from 0.25 to 1.75
- w_up: bfloat16 [1536, 26112], P('dp', 'mp'), may hold values from -0.15625 to 0.15625
- head_counts: int32 [4], replicated, may hold values from 30 to 34, as said below
- cotangent: bfloat16 [1024, 26112], P(('groups', 'dp'), 'mp'), parts along dimension 0, may hold values from -6 to 6
Outputs:
- queries: bfloat16 [1024, 26112], P(('groups', 'dp'), 'mp'), parts along dimension 0
- grad_tokens: bfloat16 [1024, 7168], P(('groups', 'dp'), 'mp'), parts along dimension 0
The draws below stay inside these ranges and needn't reach their ends.
There are 2 independent parts, one for each index of `groups`. The reference program is written for one: setup_inputs(seed, part) draws one part's arguments, and reference() takes and returns one part's arrays. A program takes and returns all parts, laid end to end along the dimension named above; an argument that names none is the same for every part. Nothing has to cross between parts.
Inputs may be any that keep to these rules, and one draw needn't show every extreme that they name: `tokens`: hidden states of order one with token scales that differ. `w_down`: entries of order 7168^(-1/2). `head_counts`: the entries sum to 128; one of them is 34.
All inputs are finite; a program needn't handle non-finite values.
Results may differ from the reference program's by a relative error of at most 0.018.
Values may be sent and summed in bfloat16 or wider, within the bound.
A program may use at most 128 MiB of HBM per device.

```python
import math
import jax
import jax.numpy as jnp
from jax import lax

D = 7168
LAT = 1536
HEADS = 128
HD = 192
HSLOT = 34
TOKENS = 512
COLS = 26112
N_MP = 4


def draw_tokens(key, part):
    base_key, scale_key = jax.random.split(key, 2)
    values = jnp.clip(jax.random.normal(base_key, (TOKENS, D), jnp.float32), -6.0, 6.0)
    scales = jnp.exp(jax.random.uniform(scale_key, (TOKENS, 1), jnp.float32, math.log(0.3), math.log(3.0)))
    return (values * scales).astype(jnp.bfloat16)


def draw_w_down(key, part):
    base_key, scale_key = jax.random.split(key, 2)
    values = jax.random.normal(base_key, (D, LAT), jnp.float32)
    values = jnp.clip(values, -6.0, 6.0)
    rising = 0.55 + 1.1 * jnp.arange(LAT, dtype=jnp.float32) / LAT
    col_scale = jnp.exp(jax.random.uniform(scale_key, (1, LAT), jnp.float32, -0.7, 0.7)) * rising
    return (values * col_scale * D ** (-0.5)).astype(jnp.bfloat16)


def draw_head_counts(key, part):
    order_key, extra_key = jax.random.split(jax.random.fold_in(key, 11))
    rank_of = jax.random.permutation(order_key, N_MP).astype(jnp.int32)
    excess = HSLOT - HEADS // N_MP
    extra = jax.random.randint(extra_key, (), 0, excess + 1).astype(jnp.int32)
    delta = jnp.where(rank_of == 0, excess, jnp.where(rank_of == 1, -excess, jnp.where(rank_of == 2, extra, jnp.where(rank_of == 3, -extra, 0))))
    return (HEADS // N_MP + delta).astype(jnp.int32)


def shard_levels(stream_key, extent, shards, smallest, top_value):
    def one(axis_at, blocks):
        steps = jax.random.uniform(jax.random.fold_in(jax.random.fold_in(stream_key, 6), axis_at), (blocks,), jnp.float32, smallest / len(shards), top_value / len(shards))
        return jnp.repeat(jnp.exp(steps), extent[axis_at] // blocks).reshape((-1,) + (1,) * (len(extent) - axis_at - 1))

    level = one(*shards[0])
    for cut in shards[1:]:
        level = level * one(*cut)
    return level


def gaussian(own_key, dims, deviation, most, cuts=(), held_as=jnp.bfloat16):
    array = jax.random.normal(own_key, dims, jnp.float32) * deviation
    if len(cuts) > 0:
        array = shard_levels(own_key, dims, cuts, -0.22, 0.18) * array
    return jnp.clip(array, min=-most, max=most).astype(held_as)


def setup_inputs(seed: int = 0, part: int = 0) -> dict:
    keys = jax.random.split(jax.random.key(seed), 7)
    part_keys = jax.random.split(jax.random.fold_in(keys[6], part), 7)
    return {
        "tokens": draw_tokens(jax.random.fold_in(jax.random.fold_in(keys[6], part), 71), part),
        "w_down": draw_w_down(jax.random.fold_in(keys[6], 71), part),
        "gain": jnp.clip(1.0 + 0.15 * jax.random.normal(keys[2], (LAT,), jnp.float32), 0.25, 1.75),
        "w_up": gaussian(keys[3], (LAT, COLS), LAT ** -0.5, 0.15625, ((0, 4), (1, 4))),
        "head_counts": draw_head_counts(jax.random.fold_in(keys[6], 71), part),
        "cotangent": gaussian(part_keys[5], (TOKENS, COLS), 1.0, 6.0, ((0, 4), (1, 4))),
    }


def reference(tokens, w_down, gain, w_up, head_counts, cotangent):
    latent_raw = jnp.dot(tokens, w_down, preferred_element_type=jnp.float32)
    root_mean = jnp.sqrt(lax.optimization_barrier(jnp.mean(latent_raw * latent_raw, axis=1, keepdims=True)) + 1e-06)
    latent = (latent_raw / root_mean * gain).astype(jnp.bfloat16)
    block_cols = HSLOT * HD
    column = jnp.arange(N_MP * block_cols, dtype=jnp.int32)
    owner = column // block_cols
    slot_index = column % block_cols // HD
    keep_mask = (slot_index < head_counts[owner]).astype(jnp.float32)
    queries = (jnp.dot(latent, w_up, preferred_element_type=jnp.float32) * keep_mask).astype(jnp.bfloat16)
    masked = cotangent * keep_mask.astype(jnp.bfloat16)
    grad_latent = lax.dot_general(masked, w_up, (((1,), (1,)), ((), ())), preferred_element_type=jnp.float32)
    inner_dot = lax.optimization_barrier(jnp.sum(gain * grad_latent * latent_raw, axis=1, keepdims=True))
    grad_raw = (gain * grad_latent / root_mean - latent_raw * inner_dot / (LAT * root_mean ** 3)).astype(jnp.bfloat16)
    width = LAT // N_MP
    running = jnp.zeros((tokens.shape[0], D), jnp.float32)
    for block in range(N_MP):
        product = lax.dot_general(grad_raw[:, block * width:(block + 1) * width], w_down[:, block * width:(block + 1) * width], (((1,), (1,)), ((), ())), preferred_element_type=jnp.float32)
        running = running + lax.optimization_barrier(product.astype(jnp.bfloat16)).astype(jnp.float32)
    return (queries, running.astype(jnp.bfloat16))
```

```python
import functools

import jax
import jax.numpy as jnp
from jax import lax
from jax.experimental import pallas as pl
from jax.experimental.pallas import tpu as pltpu
from jax.sharding import PartitionSpec as P

HD = 192
MESH = pl.DeviceIdType.MESH


def contract_last(left, right):
    return lax.dot_general(
        left, right, (((1,), (1,)), ((), ())), preferred_element_type=jnp.float32
    )


def keep_mask_of(head_counts, block_cols):
    position = lax.axis_index("mp")
    held_heads = lax.dynamic_slice_in_dim(head_counts, position, 1, 0)
    slot_index = jnp.arange(block_cols, dtype=jnp.int32) // HD
    return (slot_index < held_heads).astype(jnp.float32)


def gather_weights_body(tokens, w_down, gain, w_up, head_counts, cotangent):
    latent_width = w_down.shape[1] * lax.axis_size("mp")
    keep_mask = keep_mask_of(head_counts, w_up.shape[1])
    down_whole = lax.all_gather(w_down, "dp", axis=0, tiled=True)
    latent_raw = jnp.dot(tokens, down_whole, preferred_element_type=jnp.float32)
    squares = lax.psum(jnp.sum(latent_raw * latent_raw, axis=1, keepdims=True), "mp")
    root_mean = jnp.sqrt(squares / latent_width + 1e-06)
    latent_local = (latent_raw / root_mean * gain).astype(jnp.bfloat16)
    latent = lax.all_gather(latent_local, "mp", axis=1, tiled=True)
    masked = cotangent * keep_mask.astype(jnp.bfloat16)
    up_whole = lax.all_gather(w_up, "dp", axis=0, tiled=True)
    query_total = jnp.dot(latent, up_whole, preferred_element_type=jnp.float32)
    grad_partial = contract_last(masked, up_whole)
    queries = (query_total * keep_mask).astype(jnp.bfloat16)
    grad_latent = lax.psum_scatter(
        grad_partial.astype(jnp.bfloat16), "mp", scatter_dimension=1, tiled=True
    ).astype(jnp.float32)
    inner_dot = lax.psum(jnp.sum(gain * grad_latent * latent_raw, axis=1, keepdims=True), "mp")
    grad_raw = (
        gain * grad_latent / root_mean - latent_raw * inner_dot / (latent_width * root_mean**3)
    ).astype(jnp.bfloat16)
    partial_value = contract_last(grad_raw, down_whole).astype(jnp.bfloat16)
    grad_tokens = lax.psum_scatter(partial_value, "mp", scatter_dimension=1, tiled=True)
    return (queries, grad_tokens)


def project_kernel(
    n, spans, tile, pieces, tokens_ref, down_ref, gain_ref, w_ref, keep_ref, cot_ref,
    queries_ref, grad_tokens_ref, down_all, w_all, cots, query_out, latents, latent_out,
    grad_out, grad_in, total, last_total, raw_ref, square_out, square_in, dot_out, dot_in,
    grad_raw, products, near_in, pair_out, far_in, local_sem, down_send, down_recv,
    across_send, across_recv, cot_send, cot_recv, latent_send, latent_recv, w_send, w_recv,
    query_send, query_recv, query_local, grad_send, grad_recv, small_send, small_recv,
):
    g, d, m = lax.axis_index("groups"), lax.axis_index("dp"), lax.axis_index("mp")
    other = 1 - g
    upper = (d >= 2).astype(jnp.int32)
    mid, edge = 1 + upper, 3 * upper
    far_mid, far_edge = 2 - upper, 3 - 3 * upper
    inner = d == mid
    outer = jnp.logical_not(inner)
    role = 1 - inner.astype(jnp.int32)
    count, cols = cot_ref.shape
    depth = w_ref.shape[0]
    down_rows, width = down_ref.shape
    half = cots.shape[1]
    step = cols - half
    extra = half - step
    half_rows = down_rows // 2
    piece_rows = half_rows // pieces
    chunks = len(spans)

    barrier = pltpu.get_barrier_semaphore()
    everyone = 2 * n * n

    @pl.loop(0, everyone)
    def _(who):
        @pl.when(who != (g * n + d) * n + m)
        def _():
            pl.semaphore_signal(
                barrier, inc=1, device_id_type=MESH,
                device_id={
                    "groups": who // (n * n), "dp": lax.rem(who // n, n), "mp": lax.rem(who, n),
                },
            )

    pl.semaphore_wait(barrier, everyone - 1)

    def remote(source, target, send, recv, **where):
        return pltpu.make_async_remote_copy(
            src_ref=source, dst_ref=target, send_sem=send, recv_sem=recv,
            device_id=where, device_id_type=MESH,
        )

    def at_rows(k, size):
        return pl.ds(pl.multiple_of(k * size, size), size)

    def down_piece(shard, plane, k):
        start = shard * down_rows + plane * half_rows + k * piece_rows
        return down_all.at[pl.ds(pl.multiple_of(start, piece_rows), piece_rows)]

    def own_piece(k):
        start = g * half_rows + k * piece_rows
        return down_ref.at[pl.ds(pl.multiple_of(start, piece_rows), piece_rows)]

    def down_copy(way, shard, k, source, to):
        return remote(
            source, down_piece(shard, g, k), down_send.at[way, shard, k],
            down_recv.at[shard, k], dp=to,
        )

    def down_across(shard, k, plane):
        held = down_piece(shard, plane, k)
        return remote(
            held, held, across_send.at[shard, k], across_recv.at[shard, k], groups=other
        )

    def cot_half(plane):
        return cot_ref.at[:, pl.ds(pl.multiple_of(plane * step, 128), half)]

    def cot_copy(to):
        slot = 2 * g + role
        return remote(
            cot_half(to), cots.at[at_rows(slot, count)], cot_send.at[to], cot_recv.at[slot],
            groups=to, dp=mid,
        )

    def cot_arrival(slot):
        held = cots.at[at_rows(slot, count)]
        return remote(held, held, cot_send.at[0], cot_recv.at[slot], dp=far_mid)

    def w_piece(shard, j):
        first, size = spans[j]
        return w_all.at[at_rows(shard, depth), pl.ds(first, size)]

    def w_own(j):
        first, size = spans[j]
        return w_ref.at[:, pl.ds(pl.multiple_of(g * step + first, 128), size)]

    def w_copy(shard, j, source, to):
        return remote(source, w_piece(shard, j), w_send.at[shard, j], w_recv.at[shard, j], dp=to)

    keep_down = pltpu.make_async_copy(
        down_ref, down_all.at[at_rows(d, down_rows)], local_sem.at[0]
    )
    keep_w = pltpu.make_async_copy(
        w_ref.at[:, pl.ds(pl.multiple_of(g * step, 128), half)],
        w_all.at[at_rows(d, depth)], local_sem.at[1],
    )
    keep_cot = pltpu.make_async_copy(
        cot_half(g), cots.at[at_rows(2 * g, count)], local_sem.at[2]
    )

    @pl.when(inner)
    def _():
        for k in range(pieces):
            down_copy(0, d, k, own_piece(k), far_mid).start()
            down_copy(1, d, k, own_piece(k), edge).start()
        cot_copy(other).start()
        keep_down.start()
        keep_w.start()
        keep_cot.start()
        for k in range(pieces):
            for shard, way, to in ((edge, 0, far_mid), (far_mid, 1, edge)):
                held = down_piece(shard, g, k)
                down_copy(way, shard, k, held, to).wait_recv()
                down_copy(way, shard, k, held, to).start()
                down_across(shard, k, g).start()
        for j in range(chunks):
            w_copy(d, j, w_own(j), far_mid).start()
        for k in range(pieces):
            held = down_piece(far_edge, g, k)
            down_copy(1, far_edge, k, held, edge).wait_recv()
            down_copy(1, far_edge, k, held, edge).start()
            down_across(far_edge, k, g).start()

    @pl.when(outer)
    def _():
        for k in range(pieces):
            down_copy(0, d, k, own_piece(k), mid).start()
        cot_copy(g).start()
        cot_copy(other).start()
        keep_down.start()
        for shard in (mid, far_mid, far_edge):
            for k in range(pieces):
                held = down_piece(shard, g, k)
                down_copy(0, shard, k, held, mid).wait_recv()
                down_across(shard, k, g).start()

    for shard in range(n):

        @pl.when(shard != d)
        def _():
            for k in range(pieces):
                down_across(shard, k, other).wait_recv()

    keep_down.wait()
    raw_ref[...] = jnp.zeros_like(raw_ref)

    @pl.loop(0, 2 * n)
    def _(c):
        at = at_rows(c, half_rows)
        raw_ref[...] += jnp.dot(
            tokens_ref[:, at], down_all[at, :], preferred_element_type=jnp.float32
        )

    def to_peer(kind, o, source, target, mp):
        return remote(source, target, small_send.at[kind, o], small_recv.at[kind, o], mp=mp)

    raw = raw_ref[...]
    square_out[...] = jnp.broadcast_to(
        jnp.sum(raw * raw, axis=1, keepdims=True), square_out.shape
    )
    for o in range(1, n):
        to_peer(0, o, square_out, square_in.at[o - 1], lax.rem(m + o, n)).start()
    squares = square_out[...]
    for o in range(1, n):
        to_peer(0, o, square_out, square_in.at[o - 1], lax.rem(m + o, n)).wait_recv()
        squares += square_in[o - 1]
    root = jnp.sqrt(squares / (width * n) + 1e-06)[:, :1]
    latent_out[...] = (raw / root * gain_ref[...]).astype(latent_out.dtype)

    def latent_at(slot, who):
        return latents.at[at_rows(slot, count), at_rows(who, width)]

    def latent_inward(to):
        return remote(
            latent_out, latent_at(2 * g + role, m), latent_send.at[n, to],
            latent_recv.at[2 * g + role, m], groups=to, dp=mid,
        )

    def latent_spread(slot, o):
        held = latent_at(slot, m)
        return remote(
            held, held, latent_send.at[slot, o], latent_recv.at[slot, m],
            mp=lax.rem(m + o, n),
        )

    def latent_arrival(slot, who):
        held = latent_at(slot, who)
        return remote(held, held, latent_send.at[0, 0], latent_recv.at[slot, who], dp=far_mid)

    slots = (2 * g, 2 * other, 2 * g + 1, 2 * other + 1)

    def add_grad(sum_ref, shard, t):
        at = at_rows(t, tile)
        sum_ref[...] += contract_last(cots[:, at], w_all[at_rows(shard, depth), at])

    def grad_copy(shard, slot):
        return remote(
            grad_out.at[at_rows(slot, count), at_rows(shard, depth)], grad_in.at[g * n + m],
            grad_send.at[shard, slot], grad_recv.at[g * n + m],
            groups=slot // 2, dp=mid if slot % 2 == 0 else edge, mp=shard,
        )

    def is_self(shard, slot):
        if slot % 2 == 1:
            return None
        return jnp.logical_and(g == slot // 2, m == shard)

    def send_grad(sum_ref, shard):
        grad_out[:, at_rows(shard, depth)] = sum_ref[...].astype(grad_out.dtype)
        for slot in range(n):
            itself = is_self(shard, slot)
            if itself is None:
                grad_copy(shard, slot).start()
                continue
            pl.when(jnp.logical_not(itself))(
                lambda slot=slot: grad_copy(shard, slot).start()
            )

            @pl.when(itself)
            def _():
                grad_in[g * n + m] = grad_out[at_rows(slot, count), at_rows(shard, depth)]

    def whole_grad(shard):
        total[...] = jnp.zeros_like(total)

        @pl.loop(0, half // tile)
        def _(t):
            add_grad(total, shard, t)

        send_grad(total, shard)

    def query_parts(j):
        first, size = spans[j]
        if j == 0:
            return ((extra, size - extra, 0), (0, extra, chunks))
        return ((first, size, j),)

    def query_copy(slot, first, size, sem):
        return remote(
            query_out.at[at_rows(slot, count), pl.ds(first, size)],
            queries_ref.at[:, pl.ds(pl.multiple_of(g * step + first, 128), size)],
            query_send.at[slot, sem], query_recv.at[g, sem],
            groups=slot // 2, dp=mid if slot % 2 == 0 else edge,
        )

    def query_keep(first, size, sem):
        return pltpu.make_async_copy(
            query_out.at[at_rows(2 * g, count), pl.ds(first, size)],
            queries_ref.at[:, pl.ds(pl.multiple_of(g * step + first, 128), size)],
            query_local.at[sem],
        )

    def each_query_part(j, remote_act, local_act):
        for first, size, sem in query_parts(j):

            def act():
                for slot in range(n):
                    if slot % 2 == 1:
                        remote_act(query_copy(slot, first, size, sem))
                        continue
                    mine = g == slot // 2
                    pl.when(jnp.logical_not(mine))(
                        lambda slot=slot: remote_act(query_copy(slot, first, size, sem))
                    )
                    pl.when(mine)(lambda: local_act(query_keep(first, size, sem)))

            if sem == chunks:
                pl.when(g == 0)(act)
            else:
                act()

    def query_tile(t):
        at = at_rows(t, tile)
        keep = keep_ref[:, pl.ds(pl.multiple_of(g * step + t * tile, 128), tile)]
        product = jnp.dot(latents[...], w_all[:, at], preferred_element_type=jnp.float32)
        query_out[:, at] = (product * keep.astype(jnp.float32)).astype(query_out.dtype)

    def finish_chunk(j):
        first, size = spans[j]
        held = w_piece(far_edge, j)
        w_copy(far_edge, j, held, far_mid).wait_recv()

        @pl.loop(first // tile, (first + size) // tile)
        def _(t):
            add_grad(last_total, far_edge, t)

        if j == chunks - 1:
            send_grad(last_total, far_edge)

        pl.loop(first // tile, (first + size) // tile)(query_tile)
        each_query_part(j, lambda c: c.start(), lambda c: c.start())

    @pl.when(outer)
    def _():
        latent_inward(0).start()
        latent_inward(1).start()
        for j in range(chunks):
            w_copy(d, j, w_own(j), mid).start()

    @pl.when(inner)
    def _():
        latents[at_rows(2 * g, count), at_rows(m, width)] = latent_out[...]
        latent_inward(other).start()
        for o in range(1, n):
            latent_spread(slots[0], o).start()

        keep_cot.wait()
        for slot in slots[1:]:
            cot_arrival(slot).wait_recv()

        @pl.loop(0, half // tile)
        def _(t):
            at = at_rows(t, tile)
            keep = keep_ref[:, pl.ds(pl.multiple_of(g * step + t * tile, 128), tile)]
            cots[:, at] = cots[:, at] * keep

        @pl.when(g == 1)
        def _():
            cots[:, :extra] = jnp.zeros((n * count, extra), cots.dtype)

        keep_w.wait()
        whole_grad(d)
        for slot in slots[1:]:
            latent_arrival(slot, m).wait_recv()
            for o in range(1, n):
                latent_spread(slot, o).start()
        last_total[...] = jnp.zeros_like(last_total)
        lag = 2
        for j in range(chunks):
            held = w_piece(edge, j)
            w_copy(edge, j, held, far_mid).wait_recv()
            w_copy(edge, j, held, far_mid).start()
            if j == lag - 1:
                for i in range(chunks):
                    w_copy(far_mid, i, w_piece(far_mid, i), far_mid).wait_recv()
                whole_grad(far_mid)
                for slot in slots:
                    for o in range(1, n):
                        latent_arrival(slot, lax.rem(m + o, n)).wait_recv()
            if j == chunks - 1:
                whole_grad(edge)
            if j >= lag:
                finish_chunk(j - lag)
        for j in range(chunks - lag, chunks):
            finish_chunk(j)

    for plane in range(2):
        for who in range(n):
            source = plane * n + who
            itself = jnp.logical_and(inner, jnp.logical_and(g == plane, m == who))

            @pl.when(jnp.logical_not(itself))
            def _():
                remote(
                    grad_in.at[source], grad_in.at[source], grad_send.at[0, 0],
                    grad_recv.at[source], groups=other,
                ).wait_recv()

    grad_latent = grad_in[0].astype(jnp.float32)
    for source in range(1, 2 * n):
        grad_latent += grad_in[source].astype(jnp.float32)
    scaled = gain_ref[...] * grad_latent
    raw = raw_ref[...]
    dot_out[...] = jnp.broadcast_to(
        jnp.sum(scaled * raw, axis=1, keepdims=True), dot_out.shape
    )
    for o in range(1, n):
        to_peer(1, o, dot_out, dot_in.at[o - 1], lax.rem(m + o, n)).start()
    squares = square_out[...]
    for o in range(1, n):
        squares += square_in[o - 1]
    inner_dot = dot_out[...]
    for o in range(1, n):
        to_peer(1, o, dot_out, dot_in.at[o - 1], lax.rem(m + o, n)).wait_recv()
        inner_dot += dot_in[o - 1]
    root = jnp.sqrt(squares / (width * n) + 1e-06)
    slope = (inner_dot / (width * n * (root * root * root)))[:, :1]
    grad_raw[...] = (scaled / root[:, :1] - raw * slope).astype(grad_raw.dtype)

    far, near = lax.rem(m + 2, n), m + 1 - 2 * lax.rem(m, 2)
    far_near = lax.rem(near + 2, n)
    row_tile = 256 if down_rows % 256 == 0 else 128

    def row_tiles(body):
        @pl.loop(0, down_rows // row_tile)
        def _(c):
            body(at_rows(c, row_tile))

    def product(block):
        @pl.loop(0, down_rows // row_tile)
        def _(c):
            start = block * down_rows + c * row_tile
            rows = down_all[pl.ds(pl.multiple_of(start, row_tile), row_tile), :]
            value = contract_last(grad_raw[...], rows)
            products[block, :, at_rows(c, row_tile)] = value.astype(products.dtype)

    product(far_near)
    to_peer(2, 0, products.at[far_near], near_in.at[1], near).start()
    product(far)
    product(near)
    to_peer(2, 1, products.at[near], near_in.at[0], near).start()
    to_peer(2, 0, products.at[far_near], near_in.at[1], near).wait_recv()

    def pair_tile(at):
        both = products[far, :, at].astype(jnp.float32) + near_in[1, :, at].astype(jnp.float32)
        pair_out[:, at] = both.astype(pair_out.dtype)

    row_tiles(pair_tile)
    to_peer(2, 2, pair_out, far_in, far).start()
    product(m)
    to_peer(2, 1, products.at[near], near_in.at[0], near).wait_recv()

    for plane in range(2):
        away = jnp.logical_not(jnp.logical_and(inner, g == plane))

        @pl.when(away)
        def _():
            for j in range(chunks):
                for first, size, sem in query_parts(j):
                    if sem == chunks and plane == 1:
                        continue
                    held = queries_ref.at[:, pl.ds(plane * step + first, size)]
                    remote(
                        held, held, query_send.at[0, 0], query_recv.at[plane, sem],
                        groups=other,
                    ).wait_recv()

    to_peer(2, 2, pair_out, far_in, far).wait_recv()

    def sum_tile(at):
        both = products[m, :, at].astype(jnp.float32) + near_in[0, :, at].astype(jnp.float32)
        value = both + far_in[:, at].astype(jnp.float32)
        grad_tokens_ref[:, at] = value.astype(grad_tokens_ref.dtype)

    row_tiles(sum_tile)

    for kind in range(2):
        for o in range(1, n):
            source, target = (square_out, square_in) if kind == 0 else (dot_out, dot_in)
            to_peer(kind, o, source, target.at[o - 1], lax.rem(m + o, n)).wait_send()
    to_peer(2, 0, products.at[far_near], near_in.at[1], near).wait_send()
    to_peer(2, 1, products.at[near], near_in.at[0], near).wait_send()
    to_peer(2, 2, pair_out, far_in, far).wait_send()
    for shard in range(n):

        @pl.when(shard != d)
        def _():
            for k in range(pieces):
                down_across(shard, k, g).wait_send()

    @pl.when(outer)
    def _():
        for k in range(pieces):
            down_copy(0, d, k, own_piece(k), mid).wait_send()
        for plane in range(2):
            cot_copy(plane).wait_send()
            latent_inward(plane).wait_send()
        for j in range(chunks):
            w_copy(d, j, w_own(j), mid).wait_send()

    @pl.when(inner)
    def _():
        for k in range(pieces):
            for way, shard, to in (
                (0, d, far_mid), (1, d, edge), (0, edge, far_mid), (1, far_mid, edge),
                (1, far_edge, edge),
            ):
                down_copy(way, shard, k, own_piece(k), to).wait_send()
        cot_copy(other).wait_send()
        latent_inward(other).wait_send()
        for slot in slots:
            for o in range(1, n):
                latent_spread(slot, o).wait_send()
        for j in range(chunks):
            w_copy(d, j, w_own(j), far_mid).wait_send()
            w_copy(edge, j, w_piece(edge, j), far_mid).wait_send()
            each_query_part(j, lambda c: c.wait_send(), lambda c: c.wait())
        for shard in range(n):
            for slot in range(n):
                itself = is_self(shard, slot)
                if itself is None:
                    grad_copy(shard, slot).wait_send()
                    continue
                pl.when(jnp.logical_not(itself))(
                    lambda shard=shard, slot=slot: grad_copy(shard, slot).wait_send()
                )


def project(tokens, w_down, gain, w_up, keep, cotangent):
    n = lax.axis_size("dp")
    count, cols = cotangent.shape
    depth = w_up.shape[0]
    down_rows, width = w_down.shape
    half = (cols // 128 + 1) // 2 * 128
    tile = 256 if half % 256 == 0 else 128
    tiles = half // tile
    parts = min(5, tiles)
    sizes = [tiles // parts + (i < tiles % parts) for i in range(parts)]
    spans = tuple((sum(sizes[:i]) * tile, sizes[i] * tile) for i in range(parts))
    pieces = 2
    vmem = pl.BlockSpec(memory_space=pltpu.VMEM)
    bf16, f32 = jnp.bfloat16, jnp.float32
    dma = pltpu.SemaphoreType.DMA
    return pl.pallas_call(
        functools.partial(project_kernel, n, spans, tile, pieces),
        out_shape=(
            jax.ShapeDtypeStruct((count, cols), bf16),
            jax.ShapeDtypeStruct((count, down_rows), bf16),
        ),
        in_specs=[vmem] * 6,
        out_specs=(vmem,) * 2,
        scratch_shapes=[
            pltpu.VMEM((n * down_rows, width), bf16),
            pltpu.VMEM((n * depth, half), bf16),
            pltpu.VMEM((n * count, half), bf16),
            pltpu.VMEM((n * count, half), bf16),
            pltpu.VMEM((n * count, n * width), bf16),
            pltpu.VMEM((count, width), bf16),
            pltpu.VMEM((n * count, n * depth), bf16),
            pltpu.VMEM((2 * n, count, depth), bf16),
            pltpu.VMEM((n * count, depth), f32),
            pltpu.VMEM((n * count, depth), f32),
            pltpu.VMEM((count, width), f32),
            pltpu.VMEM((count, 128), f32),
            pltpu.VMEM((n - 1, count, 128), f32),
            pltpu.VMEM((count, 128), f32),
            pltpu.VMEM((n - 1, count, 128), f32),
            pltpu.VMEM((count, width), bf16),
            pltpu.VMEM((n, count, down_rows), bf16),
            pltpu.VMEM((2, count, down_rows), bf16),
            pltpu.VMEM((count, down_rows), bf16),
            pltpu.VMEM((count, down_rows), bf16),
            dma((3,)),
            dma((2, n, pieces)),
            dma((n, pieces)),
            dma((n, pieces)),
            dma((n, pieces)),
            dma((2,)),
            dma((n,)),
            dma((n + 1, n)),
            dma((n, n)),
            dma((n, parts)),
            dma((n, parts)),
            dma((n, parts + 1)),
            dma((2, parts + 1)),
            dma((parts + 1,)),
            dma((n, n)),
            dma((2 * n,)),
            dma((3, n)),
            dma((3, n)),
        ],
        compiler_params=pltpu.CompilerParams(
            collective_id=0, has_side_effects=True, vmem_limit_bytes=60 * 2**20
        ),
    )(tokens, w_down, gain, w_up, keep, cotangent)


def move_weights_body(tokens, w_down, gain, w_up, head_counts, cotangent):
    keep_row = keep_mask_of(head_counts, w_up.shape[1]).astype(jnp.bfloat16)[None, :]
    return project(tokens, w_down, gain[None, :], w_up, keep_row, cotangent)


def solution(mesh):
    in_specs = (
        P(("groups", "dp"), None),
        P("dp", "mp"),
        P("mp"),
        P("dp", "mp"),
        P(),
        P(("groups", "dp"), "mp"),
    )
    out_specs = (P(("groups", "dp"), "mp"), P(("groups", "dp"), "mp"))
    square = mesh.shape["dp"] == mesh.shape["mp"] == 4 and mesh.shape["groups"] == 2
    body = move_weights_body if square else gather_weights_body
    return jax.shard_map(body, mesh=mesh, in_specs=in_specs, out_specs=out_specs, check_vma=False)
```

```python
import functools

import jax
import jax.numpy as jnp
from jax import lax
from jax.experimental import pallas as pl
from jax.experimental.pallas import tpu as pltpu
from jax.sharding import PartitionSpec as P

HD = 192
MESH = pl.DeviceIdType.MESH


def contract_last(left, right):
    return lax.dot_general(
        left, right, (((1,), (1,)), ((), ())), preferred_element_type=jnp.float32
    )


def keep_mask_of(head_counts, block_cols):
    position = lax.axis_index("mp")
    held_heads = lax.dynamic_slice_in_dim(head_counts, position, 1, 0)
    slot_index = jnp.arange(block_cols, dtype=jnp.int32) // HD
    return (slot_index < held_heads).astype(jnp.float32)


def gather_weights_body(tokens, w_down, gain, w_up, head_counts, cotangent):
    latent_width = w_down.shape[1] * lax.axis_size("mp")
    keep_mask = keep_mask_of(head_counts, w_up.shape[1])
    down_whole = lax.all_gather(w_down, "dp", axis=0, tiled=True)
    latent_raw = jnp.dot(tokens, down_whole, preferred_element_type=jnp.float32)
    squares = lax.psum(jnp.sum(latent_raw * latent_raw, axis=1, keepdims=True), "mp")
    root_mean = jnp.sqrt(squares / latent_width + 1e-06)
    latent_local = (latent_raw / root_mean * gain).astype(jnp.bfloat16)
    latent = lax.all_gather(latent_local, "mp", axis=1, tiled=True)
    masked = cotangent * keep_mask.astype(jnp.bfloat16)
    up_whole = lax.all_gather(w_up, "dp", axis=0, tiled=True)
    query_total = jnp.dot(latent, up_whole, preferred_element_type=jnp.float32)
    grad_partial = contract_last(masked, up_whole)
    queries = (query_total * keep_mask).astype(jnp.bfloat16)
    grad_latent = lax.psum_scatter(
        grad_partial.astype(jnp.bfloat16), "mp", scatter_dimension=1, tiled=True
    ).astype(jnp.float32)
    inner_dot = lax.psum(jnp.sum(gain * grad_latent * latent_raw, axis=1, keepdims=True), "mp")
    grad_raw = (
        gain * grad_latent / root_mean - latent_raw * inner_dot / (latent_width * root_mean**3)
    ).astype(jnp.bfloat16)
    partial_value = contract_last(grad_raw, down_whole).astype(jnp.bfloat16)
    grad_tokens = lax.psum_scatter(partial_value, "mp", scatter_dimension=1, tiled=True)
    return (queries, grad_tokens)


def project_kernel(
    n, spans, tile, pieces, tokens_hbm, down_hbm, gain_ref, w_hbm, counts_ref, cot_hbm,
    queries_ref, grad_tokens_ref, tokens_ref, cot_ref, cot_pass, down_all, down_feat, w_all, cots,
    query_out, latents, latent_out, grad_out, grad_in, total, last_total, raw_ref,
    root_ref, square_out, square_in, dot_out, dot_in, grad_raw, grad_all, token_total, local_sem,
    down_send, down_recv, across_send, across_recv, feat_send, feat_recv, cot_send, cot_recv,
    latent_send, latent_recv, w_send, w_recv, query_send, query_recv,
    grad_send, grad_recv, small_send, small_recv,
):
    g, d, m = lax.axis_index("groups"), lax.axis_index("dp"), lax.axis_index("mp")
    other = 1 - g
    upper = (d >= 2).astype(jnp.int32)
    mid, edge = 1 + upper, 3 * upper
    far_mid, far_edge = 2 - upper, 3 - 3 * upper
    inner = d == mid
    outer = jnp.logical_not(inner)
    role = 1 - inner.astype(jnp.int32)
    count, cols = cot_ref.shape
    depth = w_hbm.shape[0]
    down_rows, width = down_hbm.shape
    half = cots.shape[1]
    step = cols - half
    extra = half - step
    half_rows = down_rows // 2
    piece_rows = half_rows // pieces
    chunks = len(spans)

    def at_rows(k, size):
        return pl.ds(pl.multiple_of(k * size, size), size)

    down_load = pltpu.make_async_copy(
        down_hbm, down_all.at[at_rows(d, down_rows)], local_sem.at[0]
    )
    cot_load = pltpu.make_async_copy(cot_hbm, cot_ref, local_sem.at[1])
    w_load = pltpu.make_async_copy(
        w_hbm.at[:, pl.ds(pl.multiple_of(g * step, 128), half)],
        w_all.at[at_rows(d, depth)], local_sem.at[2],
    )
    tokens_load = pltpu.make_async_copy(tokens_hbm, tokens_ref, local_sem.at[3])
    down_load.start()
    cot_load.start()
    w_load.start()
    tokens_load.start()

    barrier = pltpu.get_barrier_semaphore()
    everyone = 2 * n * n

    @pl.loop(0, everyone)
    def _(who):
        @pl.when(who != (g * n + d) * n + m)
        def _():
            pl.semaphore_signal(
                barrier, inc=1, device_id_type=MESH,
                device_id={
                    "groups": who // (n * n), "dp": lax.rem(who // n, n), "mp": lax.rem(who, n),
                },
            )

    down_load.wait()
    pl.semaphore_wait(barrier, everyone - 1)

    def remote(source, target, send, recv, **where):
        return pltpu.make_async_remote_copy(
            src_ref=source, dst_ref=target, send_sem=send, recv_sem=recv,
            device_id=where, device_id_type=MESH,
        )

    def down_piece(shard, plane, k):
        start = shard * down_rows + plane * half_rows + k * piece_rows
        return down_all.at[pl.ds(pl.multiple_of(start, piece_rows), piece_rows)]

    def own_piece(k):
        return down_piece(d, g, k)

    def down_copy(way, shard, k, source, to):
        return remote(
            source, down_piece(shard, g, k), down_send.at[way, shard, k],
            down_recv.at[shard, k], dp=to,
        )

    def down_across(shard, k, plane):
        held = down_piece(shard, plane, k)
        return remote(
            held, held, across_send.at[shard, k], across_recv.at[shard, k], groups=other
        )

    def cot_half(plane):
        return cot_ref.at[:, pl.ds(pl.multiple_of(plane * step, 128), half)]

    def cot_copy(way, source, slot, plane, to):
        return remote(
            source, cots.at[at_rows(slot, count)], cot_send.at[way], cot_recv.at[slot],
            groups=plane, dp=to,
        )

    def cot_across():
        return remote(
            cot_half(other), cot_pass, cot_send.at[2], cot_recv.at[n], groups=other
        )

    def cot_arrival(slot):
        held = cots.at[at_rows(slot, count)]
        return remote(held, held, cot_send.at[0], cot_recv.at[slot], dp=far_mid)

    def w_piece(shard, j):
        first, size = spans[j]
        return w_all.at[at_rows(shard, depth), pl.ds(first, size)]

    def w_own(j):
        return w_piece(d, j)

    def w_copy(shard, j, source, to):
        return remote(source, w_piece(shard, j), w_send.at[shard, j], w_recv.at[shard, j], dp=to)

    def keep_cot():
        cots[at_rows(2 * g, count), :] = cot_ref[
            :, pl.ds(pl.multiple_of(g * step, 128), half)
        ]

    def feat_copy(shard, plane, k):
        start = plane * half_rows + k * piece_rows
        rows = pl.ds(pl.multiple_of(start, piece_rows), piece_rows)
        return remote(
            down_piece(shard, plane, k), down_feat.at[rows, at_rows(m, width)],
            feat_send.at[shard, plane, k], feat_recv.at[m, plane, k], mp=shard,
        )

    def start_feat(shard, plane):
        @pl.when(shard != m)
        def _():
            for k in range(pieces):
                feat_copy(shard, plane, k).start()

    def feat_arrival(who, plane, k):
        held = down_feat.at[at_rows(plane * pieces + k, piece_rows), at_rows(who, width)]
        return remote(held, held, feat_send.at[0, 0, 0], feat_recv.at[who, plane, k], groups=other)

    def keep_feat():
        @pl.loop(0, pieces * 2)
        def _(k):
            source = m * down_rows + k * piece_rows
            down_feat[at_rows(k, piece_rows), at_rows(m, width)] = down_all[
                pl.ds(pl.multiple_of(source, piece_rows), piece_rows), :
            ]

    def feat_piece(shard, plane, k):
        pl.when(shard != m)(lambda: feat_copy(shard, plane, k).start())

    early = 2

    @pl.when(inner)
    def _():
        for k in range(pieces):
            down_copy(0, d, k, own_piece(k), far_mid).start()
            down_copy(1, d, k, own_piece(k), edge).start()
        start_feat(d, 0)
        start_feat(d, 1)
        cot_load.wait()
        keep_cot()
        for k in range(pieces):
            for shard, way, to in ((edge, 0, far_mid), (far_mid, 1, edge)):
                held = down_piece(shard, g, k)
                down_copy(way, shard, k, held, to).wait_recv()
                down_copy(way, shard, k, held, to).start()
                down_across(shard, k, g).start()
                feat_piece(shard, g, k)
        w_load.wait()
        for j in range(chunks):
            w_copy(d, j, w_own(j), far_mid).start()
        for k in range(pieces):
            held = down_piece(far_edge, g, k)
            down_copy(1, far_edge, k, held, edge).wait_recv()
            down_copy(1, far_edge, k, held, edge).start()
            down_across(far_edge, k, g).start()
            feat_piece(far_edge, g, k)
        cot_copy(0, cot_half(other), 2 * g, other, d).start()

    @pl.when(outer)
    def _():
        for k in range(pieces):
            down_copy(0, d, k, own_piece(k), mid).start()
        cot_load.wait()
        cot_across().start()
        cot_copy(0, cot_half(g), 2 * g + 1, g, mid).start()
        start_feat(d, 0)
        start_feat(d, 1)
        w_load.wait()
        for shard in (mid, far_mid, far_edge):
            for k in range(pieces):
                held = down_piece(shard, g, k)
                down_copy(0, shard, k, held, mid).wait_recv()
                down_across(shard, k, g).start()
                feat_piece(shard, g, k)
            if shard is mid:
                cot_across().wait_recv()
                cot_copy(1, cot_pass, 2 * other + 1, g, mid).start()
                for j in range(early):
                    w_copy(d, j, w_own(j), mid).start()

    for shard in (jnp.where(inner, edge, mid), far_mid, far_edge):
        for k in range(pieces):
            down_across(shard, k, other).wait_recv()
            if shard is not far_edge:
                feat_piece(shard, other, k)

    tokens_load.wait()
    raw_ref[...] = jnp.zeros_like(raw_ref)

    @pl.loop(0, 2 * n)
    def _(c):
        at = at_rows(c, half_rows)
        raw_ref[...] += jnp.dot(
            tokens_ref[:, at], down_all[at, :], preferred_element_type=jnp.float32
        )

    def to_peer(kind, o, source, target, mp):
        return remote(source, target, small_send.at[kind, o], small_recv.at[kind, o], mp=mp)

    def sum_over_mp(kind, column, out_ref, in_ref):
        out_ref[...] = jnp.broadcast_to(column, (count, 128)).T[:8]
        for o in range(1, n):
            to_peer(kind, o, out_ref, in_ref.at[o - 1], lax.rem(m + o, n)).start()
        value = out_ref[...]
        for o in range(1, n):
            to_peer(kind, o, out_ref, in_ref.at[o - 1], lax.rem(m + o, n)).wait_recv()
            value += in_ref[o - 1]
        return jnp.broadcast_to(value[:1], (128, count)).T[:, :1]

    raw = raw_ref[...]
    squares = sum_over_mp(
        0, jnp.sum(raw * raw, axis=1, keepdims=True), square_out, square_in
    )
    root = jnp.sqrt(squares / (width * n) + 1e-06)
    root_ref[...] = jnp.broadcast_to(root, root_ref.shape)
    gain = gain_ref[...].reshape(1, width)
    latent_out[...] = (raw / root * gain).astype(latent_out.dtype)

    def latent_at(slot, who):
        return latents.at[at_rows(slot, count), at_rows(who, width)]

    def latent_inward(to):
        return remote(
            latent_out, latent_at(2 * g + role, m), latent_send.at[n, to],
            latent_recv.at[2 * g + role, m], groups=to, dp=mid,
        )

    def latent_spread(slot, o):
        held = latent_at(slot, m)
        return remote(
            held, held, latent_send.at[slot, o], latent_recv.at[slot, m],
            mp=lax.rem(m + o, n),
        )

    def latent_arrival(slot, who):
        held = latent_at(slot, who)
        return remote(held, held, latent_send.at[0, 0], latent_recv.at[slot, who], dp=far_mid)

    slots = (2 * g, 2 * other, 2 * g + 1, 2 * other + 1)

    def add_grad(sum_ref, shard, t):
        at = at_rows(t, tile)
        sum_ref[...] += contract_last(cots[:, at], w_all[at_rows(shard, depth), at])

    def grad_copy(shard, slot):
        return remote(
            grad_out.at[at_rows(slot, count), at_rows(shard, depth)], grad_in.at[g * n + m],
            grad_send.at[shard, slot], grad_recv.at[g * n + m],
            groups=slot // 2, dp=mid if slot % 2 == 0 else edge, mp=shard,
        )

    def is_self(shard, slot):
        if slot % 2 == 1:
            return None
        return jnp.logical_and(g == slot // 2, m == shard)

    def send_grad(sum_ref, shard):
        grad_out[:, at_rows(shard, depth)] = sum_ref[...].astype(grad_out.dtype)
        for slot in range(n):
            itself = is_self(shard, slot)
            if itself is None:
                grad_copy(shard, slot).start()
                continue
            pl.when(jnp.logical_not(itself))(
                lambda slot=slot: grad_copy(shard, slot).start()
            )

            @pl.when(itself)
            def _():
                grad_in[g * n + m] = grad_out[at_rows(slot, count), at_rows(shard, depth)]

    def whole_grad(shard):
        total[...] = jnp.zeros_like(total)

        @pl.loop(0, half // tile)
        def _(t):
            add_grad(total, shard, t)

        send_grad(total, shard)

    def query_parts(j):
        first, size = spans[j]
        if j == 0:
            return ((extra, size - extra, 0), (0, extra, chunks))
        return ((first, size, j),)

    def query_copy(slot, first, size, sem):
        return remote(
            query_out.at[at_rows(slot, count), pl.ds(first, size)],
            queries_ref.at[:, pl.ds(pl.multiple_of(g * step + first, 128), size)],
            query_send.at[slot, sem], query_recv.at[g, sem],
            groups=slot // 2, dp=mid if slot % 2 == 0 else edge,
        )

    def keep_query(first, size):
        queries_ref[:, pl.ds(pl.multiple_of(g * step + first, 128), size)] = query_out[
            at_rows(2 * g, count), pl.ds(first, size)
        ]

    def each_query_part(j, remote_act, keep):
        for first, size, sem in query_parts(j):

            def act():
                for slot in range(n):
                    if slot % 2 == 1:
                        remote_act(query_copy(slot, first, size, sem))
                        continue
                    mine = g == slot // 2
                    pl.when(jnp.logical_not(mine))(
                        lambda slot=slot: remote_act(query_copy(slot, first, size, sem))
                    )
                if keep:
                    keep_query(first, size)

            if sem == chunks:
                pl.when(g == 0)(act)
            else:
                act()

    def keep_row(t):
        column = lax.broadcasted_iota(jnp.int32, (1, tile), 1) + (g * step + t * tile)
        return (column < counts_ref[m] * HD).astype(jnp.float32)

    def query_tile(t):
        at = at_rows(t, tile)
        product = jnp.dot(latents[...], w_all[:, at], preferred_element_type=jnp.float32)
        query_out[:, at] = (product * keep_row(t)).astype(query_out.dtype)

    def finish_chunk(j):
        first, size = spans[j]
        held = w_piece(far_edge, j)
        w_copy(far_edge, j, held, far_mid).wait_recv()

        @pl.loop(first // tile, (first + size) // tile)
        def _(t):
            add_grad(last_total, far_edge, t)

        if j == chunks - 1:
            send_grad(last_total, far_edge)

        pl.loop(first // tile, (first + size) // tile)(query_tile)
        each_query_part(j, lambda c: c.start(), True)

    @pl.when(outer)
    def _():
        latent_inward(0).start()
        latent_inward(1).start()
        for j in range(early, chunks):
            w_copy(d, j, w_own(j), mid).start()
        start_feat(far_edge, other)
        keep_feat()

    def pass_on(j):
        held = w_piece(edge, j)
        w_copy(edge, j, held, far_mid).wait_recv()
        w_copy(edge, j, held, far_mid).start()

    @pl.when(inner)
    def _():
        latents[at_rows(2 * g, count), at_rows(m, width)] = latent_out[...]
        latent_inward(other).start()
        for o in range(1, n):
            latent_spread(slots[0], o).start()
        start_feat(far_edge, other)
        keep_feat()
        for j in range(early):
            pass_on(j)
        for slot in slots[1:]:
            latent_arrival(slot, m).wait_recv()
            for o in range(1, n):
                latent_spread(slot, o).start()

        for slot in slots[1:]:
            cot_arrival(slot).wait_recv()

        @pl.loop(0, half // tile)
        def _(t):
            at = at_rows(t, tile)
            cots[:, at] = cots[:, at] * keep_row(t).astype(cots.dtype)

        @pl.when(g == 1)
        def _():
            cots[:, :extra] = jnp.zeros((n * count, extra), cots.dtype)

        whole_grad(d)
        for i in range(chunks):
            w_copy(far_mid, i, w_piece(far_mid, i), far_mid).wait_recv()
        whole_grad(far_mid)
        for slot in slots:
            for o in range(1, n):
                latent_arrival(slot, lax.rem(m + o, n)).wait_recv()
        last_total[...] = jnp.zeros_like(last_total)
        for j in range(early, chunks):
            pass_on(j)
            if j == chunks - 1:
                whole_grad(edge)
            finish_chunk(j - early)
        for j in range(chunks - early, chunks):
            finish_chunk(j)

    for plane in range(2):
        for who in range(n):
            source = plane * n + who
            itself = jnp.logical_and(inner, jnp.logical_and(g == plane, m == who))

            @pl.when(jnp.logical_not(itself))
            def _():
                remote(
                    grad_in.at[source], grad_in.at[source], grad_send.at[0, 0],
                    grad_recv.at[source], groups=other,
                ).wait_recv()

    grad_latent = grad_in[0].astype(jnp.float32)
    for source in range(1, 2 * n):
        grad_latent += grad_in[source].astype(jnp.float32)
    scaled = gain_ref[...].reshape(1, width) * grad_latent
    raw = raw_ref[...]
    inner_dot = sum_over_mp(1, jnp.sum(scaled * raw, axis=1, keepdims=True), dot_out, dot_in)
    root = root_ref[:, :1]
    slope = inner_dot / (width * n * (root * root * root))
    grad_raw[...] = (scaled / root - raw * slope).astype(grad_raw.dtype)

    far, near = lax.rem(m + 2, n), m + 1 - 2 * lax.rem(m, 2)
    far_near = lax.rem(near + 2, n)

    def block_copy(o):
        to = (far, far_near, near)[o]
        return remote(
            grad_raw, grad_all.at[at_rows(m, count)], small_send.at[2, o],
            small_recv.at[2, m], mp=to,
        )

    def block_arrival(who):
        held = grad_all.at[at_rows(who, count)]
        return remote(held, held, small_send.at[2, 0], small_recv.at[2, who], groups=other)

    for o in range(n - 1):
        block_copy(o).start()
    row_tile = 256 if down_rows % 256 == 0 else 128

    def add_block(read, who, first, last):
        @pl.loop(0, down_rows // row_tile)
        def _(c):
            rows = at_rows(c, row_tile)
            value = contract_last(read(), down_feat[rows, at_rows(who, width)])
            if not first:
                value += token_total[:, rows]
            if last:
                grad_tokens_ref[:, rows] = value.astype(grad_tokens_ref.dtype)
            else:
                token_total[:, rows] = value

    for o in range(1, n):
        for plane in range(2):
            for k in range(pieces):
                feat_arrival(lax.rem(m + o, n), plane, k).wait_recv()
    add_block(lambda: grad_raw[...], m, True, False)
    for who in (near, far, far_near):
        block_arrival(who).wait_recv()
        add_block(lambda: grad_all[at_rows(who, count), :], who, False, who is far_near)

    for plane in range(2):
        away = jnp.logical_not(jnp.logical_and(inner, g == plane))

        @pl.when(away)
        def _():
            for j in range(chunks):
                for first, size, sem in query_parts(j):
                    if sem == chunks and plane == 1:
                        continue
                    held = queries_ref.at[:, pl.ds(plane * step + first, size)]
                    remote(
                        held, held, query_send.at[0, 0], query_recv.at[plane, sem],
                        groups=other,
                    ).wait_recv()

    for kind in range(2):
        for o in range(1, n):
            source, target = (square_out, square_in) if kind == 0 else (dot_out, dot_in)
            to_peer(kind, o, source, target.at[o - 1], lax.rem(m + o, n)).wait_send()
    for o in range(n - 1):
        block_copy(o).wait_send()
        for plane in range(2):
            for k in range(pieces):
                feat_copy(lax.rem(m + o + 1, n), plane, k).wait_send()
    for shard in range(n):

        @pl.when(shard != d)
        def _():
            for k in range(pieces):
                down_across(shard, k, g).wait_send()

    @pl.when(outer)
    def _():
        for k in range(pieces):
            down_copy(0, d, k, own_piece(k), mid).wait_send()
        cot_across().wait_send()
        for plane in range(2):
            cot_copy(plane, cot_half(g), 2 * g + 1, g, mid).wait_send()
            latent_inward(plane).wait_send()
        for j in range(chunks):
            w_copy(d, j, w_own(j), mid).wait_send()

    @pl.when(inner)
    def _():
        for k in range(pieces):
            for way, shard, to in (
                (0, d, far_mid), (1, d, edge), (0, edge, far_mid), (1, far_mid, edge),
                (1, far_edge, edge),
            ):
                down_copy(way, shard, k, own_piece(k), to).wait_send()
        cot_copy(0, cot_half(other), 2 * g, other, d).wait_send()
        latent_inward(other).wait_send()
        for slot in slots:
            for o in range(1, n):
                latent_spread(slot, o).wait_send()
        for j in range(chunks):
            w_copy(d, j, w_own(j), far_mid).wait_send()
            w_copy(edge, j, w_piece(edge, j), far_mid).wait_send()
            each_query_part(j, lambda c: c.wait_send(), False)
        for shard in range(n):
            for slot in range(n):
                itself = is_self(shard, slot)
                if itself is None:
                    grad_copy(shard, slot).wait_send()
                    continue
                pl.when(jnp.logical_not(itself))(
                    lambda shard=shard, slot=slot: grad_copy(shard, slot).wait_send()
                )


def project(tokens, w_down, gain, w_up, head_counts, cotangent):
    n = lax.axis_size("dp")
    count, cols = cotangent.shape
    depth = w_up.shape[0]
    down_rows, width = w_down.shape
    half = (cols // 128 + 1) // 2 * 128
    tile = 256 if half % 256 == 0 else 128
    tiles = half // tile
    parts = min(5, tiles)
    sizes = [tiles // parts + (i < tiles % parts) for i in range(parts)]
    spans = tuple((sum(sizes[:i]) * tile, sizes[i] * tile) for i in range(parts))
    pieces = 2
    vmem = pl.BlockSpec(memory_space=pltpu.VMEM)
    hbm = pl.BlockSpec(memory_space=pl.ANY)
    bf16, f32 = jnp.bfloat16, jnp.float32
    dma = pltpu.SemaphoreType.DMA
    return pl.pallas_call(
        functools.partial(project_kernel, n, spans, tile, pieces),
        out_shape=(
            jax.ShapeDtypeStruct((count, cols), bf16),
            jax.ShapeDtypeStruct((count, down_rows), bf16),
        ),
        in_specs=[hbm, hbm, vmem, hbm, pl.BlockSpec(memory_space=pltpu.SMEM), hbm],
        out_specs=(vmem,) * 2,
        scratch_shapes=[
            pltpu.VMEM(tokens.shape, bf16),
            pltpu.VMEM((count, cols), bf16),
            pltpu.VMEM((count, half), bf16),
            pltpu.VMEM((n * down_rows, width), bf16),
            pltpu.VMEM((down_rows, n * width), bf16),
            pltpu.VMEM((n * depth, half), bf16),
            pltpu.VMEM((n * count, half), bf16),
            pltpu.VMEM((n * count, half), bf16),
            pltpu.VMEM((n * count, n * width), bf16),
            pltpu.VMEM((count, width), bf16),
            pltpu.VMEM((n * count, n * depth), bf16),
            pltpu.VMEM((2 * n, count, depth), bf16),
            pltpu.VMEM((n * count, depth), f32),
            pltpu.VMEM((n * count, depth), f32),
            pltpu.VMEM((count, width), f32),
            pltpu.VMEM((count, 128), f32),
            pltpu.VMEM((8, count), f32),
            pltpu.VMEM((n - 1, 8, count), f32),
            pltpu.VMEM((8, count), f32),
            pltpu.VMEM((n - 1, 8, count), f32),
            pltpu.VMEM((count, width), bf16),
            pltpu.VMEM((n * count, width), bf16),
            pltpu.VMEM((count, down_rows), f32),
            dma((4,)),
            dma((2, n, pieces)),
            dma((n, pieces)),
            dma((n, pieces)),
            dma((n, pieces)),
            dma((n, 2, pieces)),
            dma((n, 2, pieces)),
            dma((3,)),
            dma((n + 1,)),
            dma((n + 1, n)),
            dma((n, n)),
            dma((n, parts)),
            dma((n, parts)),
            dma((n, parts + 1)),
            dma((2, parts + 1)),
            dma((n, n)),
            dma((2 * n,)),
            dma((3, n)),
            dma((3, n)),
        ],
        compiler_params=pltpu.CompilerParams(
            collective_id=0, has_side_effects=True, vmem_limit_bytes=60 * 2**20
        ),
    )(tokens, w_down, gain, w_up, head_counts, cotangent)


def move_weights_body(tokens, w_down, gain, w_up, head_counts, cotangent):
    return project(tokens, w_down, gain, w_up, head_counts, cotangent)


def solution(mesh):
    in_specs = (
        P(("groups", "dp"), None),
        P("dp", "mp"),
        P("mp"),
        P("dp", "mp"),
        P(),
        P(("groups", "dp"), "mp"),
    )
    out_specs = (P(("groups", "dp"), "mp"), P(("groups", "dp"), "mp"))
    square = mesh.shape["dp"] == mesh.shape["mp"] == 4 and mesh.shape["groups"] == 2
    body = move_weights_body if square else gather_weights_body
    return jax.shard_map(body, mesh=mesh, in_specs=in_specs, out_specs=out_specs, check_vma=False)
```

```python
import functools

import jax
import jax.numpy as jnp
from jax import lax
from jax.experimental import pallas as pl
from jax.experimental.pallas import tpu as pltpu
from jax.sharding import PartitionSpec as P

HD = 192
MESH = pl.DeviceIdType.MESH


def contract_last(left, right):
    return lax.dot_general(
        left, right, (((1,), (1,)), ((), ())), preferred_element_type=jnp.float32
    )


def keep_mask_of(head_counts, block_cols):
    position = lax.axis_index("mp")
    held_heads = lax.dynamic_slice_in_dim(head_counts, position, 1, 0)
    slot_index = jnp.arange(block_cols, dtype=jnp.int32) // HD
    return (slot_index < held_heads).astype(jnp.float32)


def gather_weights_body(tokens, w_down, gain, w_up, head_counts, cotangent):
    latent_width = w_down.shape[1] * lax.axis_size("mp")
    keep_mask = keep_mask_of(head_counts, w_up.shape[1])
    down_whole = lax.all_gather(w_down, "dp", axis=0, tiled=True)
    latent_raw = jnp.dot(tokens, down_whole, preferred_element_type=jnp.float32)
    squares = lax.psum(jnp.sum(latent_raw * latent_raw, axis=1, keepdims=True), "mp")
    root_mean = jnp.sqrt(squares / latent_width + 1e-06)
    latent_local = (latent_raw / root_mean * gain).astype(jnp.bfloat16)
    latent = lax.all_gather(latent_local, "mp", axis=1, tiled=True)
    masked = cotangent * keep_mask.astype(jnp.bfloat16)
    up_whole = lax.all_gather(w_up, "dp", axis=0, tiled=True)
    query_total = jnp.dot(latent, up_whole, preferred_element_type=jnp.float32)
    grad_partial = contract_last(masked, up_whole)
    queries = (query_total * keep_mask).astype(jnp.bfloat16)
    grad_latent = lax.psum_scatter(
        grad_partial.astype(jnp.bfloat16), "mp", scatter_dimension=1, tiled=True
    ).astype(jnp.float32)
    inner_dot = lax.psum(jnp.sum(gain * grad_latent * latent_raw, axis=1, keepdims=True), "mp")
    grad_raw = (
        gain * grad_latent / root_mean - latent_raw * inner_dot / (latent_width * root_mean**3)
    ).astype(jnp.bfloat16)
    partial_value = contract_last(grad_raw, down_whole).astype(jnp.bfloat16)
    grad_tokens = lax.psum_scatter(partial_value, "mp", scatter_dimension=1, tiled=True)
    return (queries, grad_tokens)


def project_kernel(
    n, spans, tile, pieces, tokens_hbm, down_hbm, gain_ref, w_hbm, counts_ref, cot_hbm,
    queries_ref, grad_tokens_ref, tokens_ref, cot_ref, cot_pass, down_all, down_feat, w_all,
    cots, query_out, latents, latent_out, grad_out, grad_in, total, last_total, raw_ref,
    root_ref, square_out, square_in, dot_total, dot_out, dot_in, grad_raw, grad_all,
    token_total, token_out, local_sem, down_send, down_recv, across_send, across_recv,
    feat_send, feat_recv, cot_send, cot_recv, latent_send, latent_recv, w_send, w_recv,
    query_sem, grad_send, grad_recv, small_send, small_recv,
):
    g, d, m = lax.axis_index("groups"), lax.axis_index("dp"), lax.axis_index("mp")
    other = 1 - g
    upper = (d >= 2).astype(jnp.int32)
    mid, edge = 1 + upper, 3 * upper
    far_mid, far_edge = 2 - upper, 3 - 3 * upper
    inner = d == mid
    outer = jnp.logical_not(inner)
    role = 1 - inner.astype(jnp.int32)
    count, cols = cot_ref.shape
    depth = w_hbm.shape[0]
    down_rows, width = down_hbm.shape
    half = cots.shape[1]
    step = cols - half
    extra = half - step
    half_rows = down_rows // 2
    piece_rows = half_rows // pieces
    chunks = len(spans)

    def at_rows(k, size):
        return pl.ds(pl.multiple_of(k * size, size), size)

    down_load = pltpu.make_async_copy(
        down_hbm, down_all.at[at_rows(d, down_rows)], local_sem.at[0]
    )
    cot_load = pltpu.make_async_copy(cot_hbm, cot_ref, local_sem.at[1])
    w_load = pltpu.make_async_copy(
        w_hbm.at[:, pl.ds(pl.multiple_of(g * step, 128), half)],
        w_all.at[at_rows(d, depth)], local_sem.at[2],
    )
    tokens_load = pltpu.make_async_copy(tokens_hbm, tokens_ref, local_sem.at[3])
    down_load.start()
    cot_load.start()
    w_load.start()
    tokens_load.start()

    barrier = pltpu.get_barrier_semaphore()

    def greet(**where):
        pl.semaphore_signal(barrier, inc=1, device_id=where, device_id_type=MESH)

    for plane in range(2):
        for place in (0, 1):
            for who in range(n):
                there = mid if place == 0 else edge
                itself = jnp.logical_and(
                    g == plane, jnp.logical_and(role == place, m == who)
                )
                pl.when(jnp.logical_not(itself))(
                    lambda plane=plane, there=there, who=who: greet(
                        groups=plane, dp=there, mp=who
                    )
                )
    pl.when(inner)(lambda: greet(dp=far_mid))
    down_load.wait()
    pl.when(inner)(lambda: pl.semaphore_wait(barrier, 4 * n))
    pl.when(outer)(lambda: pl.semaphore_wait(barrier, 4 * n - 1))

    def remote(source, target, send, recv, **where):
        return pltpu.make_async_remote_copy(
            src_ref=source, dst_ref=target, send_sem=send, recv_sem=recv,
            device_id=where, device_id_type=MESH,
        )

    def down_piece(shard, plane, k):
        start = shard * down_rows + plane * half_rows + k * piece_rows
        return down_all.at[pl.ds(pl.multiple_of(start, piece_rows), piece_rows)]

    def down_copy(way, kind, shard, k, to):
        held = down_piece(shard, g, k)
        return remote(held, held, down_send.at[way], down_recv.at[kind, k], dp=to)

    def down_half(shard, plane):
        start = shard * down_rows + plane * half_rows
        return down_all.at[pl.ds(pl.multiple_of(start, piece_rows), half_rows)]

    def down_sent(way):
        held = down_half(d, g)
        remote(held, held, down_send.at[way], down_recv.at[0, 0], dp=far_mid).wait_send()

    def down_across(kind, shard, k):
        held = down_piece(shard, g, k)
        return remote(held, held, across_send.at[kind], across_recv.at[kind], groups=other)

    def down_crossed(kind, shard, plane):
        held = down_half(shard, plane)
        return remote(held, held, across_send.at[kind], across_recv.at[kind], groups=other)

    def cot_half(plane):
        return cot_ref.at[:, pl.ds(pl.multiple_of(plane * step, 128), half)]

    def cot_copy(way, source, slot, plane, to):
        return remote(
            source, cots.at[at_rows(slot, count)], cot_send.at[way], cot_recv.at[slot],
            groups=plane, dp=to,
        )

    def cot_across():
        return remote(
            cot_half(other), cot_pass, cot_send.at[2], cot_recv.at[n], groups=other
        )

    def cot_arrival(slot):
        held = cots.at[at_rows(slot, count)]
        return remote(held, held, cot_send.at[0], cot_recv.at[slot], dp=far_mid)

    def w_rows(shard, row, rows):
        return pl.ds(pl.multiple_of(shard * depth + row, 128), rows)

    def w_piece(shard, j):
        row, rows, first, size = spans[j]
        return w_all.at[w_rows(shard, row, rows), pl.ds(first, size)]

    def w_copy(way, kind, shard, j, to):
        held = w_piece(shard, j)
        sem = w_recv.at[2 * chunks] if kind == 1 else w_recv.at[kind // 2 * chunks + j]
        return remote(held, held, w_send.at[way], sem, dp=to)

    def w_whole(way, shard):
        held = w_all.at[at_rows(shard, depth), :]
        return remote(held, held, w_send.at[way], w_recv.at[2 * chunks], dp=far_mid)

    def keep_cot():
        cots[at_rows(2 * g, count), :] = cot_ref[
            :, pl.ds(pl.multiple_of(g * step, 128), half)
        ]

    def feat_copy(shard, plane, k):
        start = plane * half_rows + k * piece_rows
        rows = pl.ds(pl.multiple_of(start, piece_rows), piece_rows)
        return remote(
            down_piece(shard, plane, k), down_feat.at[rows, at_rows(m, width)],
            feat_send.at[shard], feat_recv.at[m], mp=shard,
        )

    def start_feat(shard, plane):
        @pl.when(shard != m)
        def _():
            for k in range(pieces):
                feat_copy(shard, plane, k).start()

    def feat_whole(sent, arrived):
        held = down_feat.at[:, at_rows(arrived, width)]
        return remote(held, held, feat_send.at[sent], feat_recv.at[arrived], groups=other)

    def keep_feat():
        @pl.loop(0, pieces * 2)
        def _(k):
            source = m * down_rows + k * piece_rows
            down_feat[at_rows(k, piece_rows), at_rows(m, width)] = down_all[
                pl.ds(pl.multiple_of(source, piece_rows), piece_rows), :
            ]

    def feat_piece(shard, plane, k):
        pl.when(shard != m)(lambda: feat_copy(shard, plane, k).start())

    early = 3

    @pl.when(inner)
    def _():
        for k in range(pieces):
            down_copy(0, 1, d, k, far_mid).start()
            down_copy(1, 0, d, k, edge).start()
        start_feat(d, 0)
        start_feat(d, 1)
        cot_load.wait()
        keep_cot()
        for k in range(pieces):
            for kind, shard, way, to in ((0, edge, 2, far_mid), (1, far_mid, 3, edge)):
                down_copy(way, kind, shard, k, to).wait_recv()
                down_copy(way, kind + (2 if kind == 0 else 0), shard, k, to).start()
                down_across(kind, shard, k).start()
                feat_piece(shard, g, k)
        w_load.wait()
        for j in range(chunks):
            w_copy(0, 1, d, j, far_mid).start()
        for k in range(pieces):
            down_copy(4, 2, far_edge, k, edge).wait_recv()
            down_copy(4, 2, far_edge, k, edge).start()
            down_across(2, far_edge, k).start()
            feat_piece(far_edge, g, k)
        cot_copy(0, cot_half(other), 2 * g, other, d).start()

    @pl.when(outer)
    def _():
        for k in range(pieces):
            down_copy(0, 0, d, k, mid).start()
        cot_load.wait()
        cot_across().start()
        cot_copy(0, cot_half(g), 2 * g + 1, g, mid).start()
        start_feat(d, 0)
        start_feat(d, 1)
        w_load.wait()
        for kind, shard in enumerate((mid, far_mid, far_edge)):
            for k in range(pieces):
                down_copy(0, kind, shard, k, mid).wait_recv()
                down_across(kind, shard, k).start()
                feat_piece(shard, g, k)
            if kind == 0:
                cot_across().wait_recv()
                cot_copy(1, cot_pass, 2 * other + 1, g, mid).start()
                for j in range(early):
                    w_copy(0, 0, d, j, mid).start()

    neighbours = (jnp.where(inner, edge, mid), far_mid, far_edge)
    for kind, shard in enumerate(neighbours):
        down_crossed(kind, shard, other).wait_recv()
        if kind < 2:
            start_feat(shard, other)

    tokens_load.wait()
    raw_ref[...] = jnp.zeros_like(raw_ref)

    @pl.loop(0, 2 * n)
    def _(c):
        at = at_rows(c, half_rows)
        raw_ref[...] += jnp.dot(
            tokens_ref[:, at], down_all[at, :], preferred_element_type=jnp.float32
        )

    def to_peer(sent, arrived, source, target, mp):
        return remote(source, target, small_send.at[sent], small_recv.at[arrived], mp=mp)

    raw = raw_ref[...]
    square_out[...] = jnp.broadcast_to(
        jnp.sum(raw * raw, axis=1, keepdims=True), (count, 128)
    ).T[:8]
    for o in range(1, n):
        to_peer(0, 0, square_out, square_in.at[o - 1], lax.rem(m + o, n)).start()
    to_peer(0, 0, square_in, square_in, far_mid).wait_recv()
    value = square_out[...]
    for o in range(1, n):
        value += square_in[o - 1]
    squares = jnp.broadcast_to(value[:1], (128, count)).T[:, :1]
    root = jnp.sqrt(squares / (width * n) + 1e-06)
    root_ref[...] = jnp.broadcast_to(root, root_ref.shape)
    gain = gain_ref[...].reshape(1, width)
    latent_out[...] = (raw / root * gain).astype(latent_out.dtype)

    def latent_at(slot, who):
        return latents.at[at_rows(slot, count), at_rows(who, width)]

    def latent_inward(to):
        return remote(
            latent_out, latent_at(2 * g + role, m), latent_send.at[to],
            latent_recv.at[2 * g + role], groups=to, dp=mid,
        )

    def latent_arrival(slot):
        held = latent_at(slot, m)
        return remote(held, held, latent_send.at[0], latent_recv.at[slot], dp=far_mid)

    def latent_spread(slot, o):
        held = latent_at(slot, m)
        return remote(
            held, held, latent_send.at[2], latent_recv.at[n], mp=lax.rem(m + o, n)
        )

    def latents_spread():
        held = latents.at[:, pl.ds(0, (n - 1) * width)]
        return remote(held, held, latent_send.at[2], latent_recv.at[n], dp=far_mid)

    slots = (2 * g, 2 * other, 2 * g + 1, 2 * other + 1)

    cut = depth - 128
    grad_parts = ((0, cut), (cut, 128))

    def add_grad(sum_ref, shard, row, rows, t):
        at = at_rows(t, tile)
        sum_ref[:, row:row + rows] += contract_last(
            cots[:, at], w_all[w_rows(shard, row, rows), at]
        )

    def grad_copy(shard, slot, part):
        row, rows = grad_parts[part]
        return remote(
            grad_out.at[at_rows(slot, count), w_rows(shard, row, rows)],
            grad_in.at[g * n + m, :, pl.ds(row, rows)],
            grad_send.at[0], grad_recv.at[0],
            groups=slot // 2, dp=mid if slot % 2 == 0 else edge, mp=shard,
        )

    def is_self(shard, slot):
        return jnp.logical_and(g == slot // 2, m == shard)

    def each_grad(shard, part, act):
        for slot in range(n):
            if slot % 2 == 1:
                act(grad_copy(shard, slot, part))
                continue
            pl.when(jnp.logical_not(is_self(shard, slot)))(
                lambda slot=slot: act(grad_copy(shard, slot, part))
            )

    def send_grad(sum_ref, shard, part):
        row, rows = grad_parts[part]
        grad_out[:, w_rows(shard, row, rows)] = sum_ref[:, row:row + rows].astype(
            grad_out.dtype
        )
        each_grad(shard, part, lambda c: c.start())

        @pl.when(m == shard)
        def _():
            grad_in[g * n + m, :, row:row + rows] = grad_out[
                at_rows(2 * g, count), w_rows(shard, row, rows)
            ]

    def whole_grad(shard):
        total[...] = jnp.zeros_like(total)

        @pl.loop(0, half // tile)
        def _(t):
            add_grad(total, shard, 0, depth, t)

        for part in range(2):
            send_grad(total, shard, part)

    def query_parts(j):
        row, rows, first, size = spans[j]
        if row + rows < depth:
            return ()
        if j == 0:
            return ((extra, size - extra, False), (0, extra, True))
        return ((first, size, False),)

    def query_copy(slot, first, size):
        return remote(
            query_out.at[at_rows(slot, count), pl.ds(first, size)],
            queries_ref.at[:, pl.ds(pl.multiple_of(g * step + first, 128), size)],
            query_sem.at[2], query_sem.at[g],
            groups=slot // 2, dp=mid if slot % 2 == 0 else edge,
        )

    def query_keep(first, size):
        return pltpu.make_async_copy(
            query_out.at[at_rows(2 * g, count), pl.ds(first, size)],
            queries_ref.at[:, pl.ds(pl.multiple_of(g * step + first, 128), size)],
            query_sem.at[3],
        )

    def send_queries(j):
        for first, size, once in query_parts(j):

            def act():
                for slot in range(n):
                    if slot % 2 == 1:
                        query_copy(slot, first, size).start()
                        continue
                    mine = g == slot // 2
                    pl.when(jnp.logical_not(mine))(
                        lambda slot=slot: query_copy(slot, first, size).start()
                    )
                query_keep(first, size).start()

            if once:
                pl.when(g == 0)(act)
            else:
                act()

    def keep_row(t):
        column = lax.broadcasted_iota(jnp.int32, (1, tile), 1) + (g * step + t * tile)
        return (column < counts_ref[m] * HD).astype(jnp.float32)

    def query_tile(t):
        at = at_rows(t, tile)
        product = jnp.dot(latents[...], w_all[:, at], preferred_element_type=jnp.float32)
        query_out[:, at] = (product * keep_row(t)).astype(query_out.dtype)
        dots = product * cots[:, at].astype(jnp.float32)
        for part in range(tile // 128):
            dot_total[...] += dots[:, part * 128:(part + 1) * 128]

    def dot_copy(slot, to):
        return remote(
            dot_out.at[slot], dot_in.at[g * n + m], grad_send.at[1], grad_recv.at[1],
            groups=slot // 2,
            dp=mid if slot % 2 == 0 else edge, mp=to,
        )

    def each_dot(act):
        for slot in range(n):
            for to in range(n):
                if slot % 2 == 1:
                    act(dot_copy(slot, to))
                    continue
                pl.when(jnp.logical_not(is_self(to, slot)))(
                    lambda slot=slot, to=to: act(dot_copy(slot, to))
                )

    def send_dots():
        for slot in range(n):
            column = jnp.sum(dot_total[at_rows(slot, count), :], axis=1, keepdims=True)
            dot_out[slot] = jnp.broadcast_to(column, (count, 128)).T[:8]
        each_dot(lambda c: c.start())
        dot_in[g * n + m] = dot_out[2 * g]

    def finish_chunk(j):
        row, rows, first, size = spans[j]
        w_copy(0, 2, far_edge, j, far_mid).wait_recv()

        @pl.loop(first // tile, (first + size) // tile)
        def _(t):
            add_grad(last_total, far_edge, row, rows, t)

        if j == chunks - 2:
            send_grad(last_total, far_edge, 0)
        if j == chunks - 1:
            send_grad(last_total, far_edge, 1)
        if row + rows == depth:
            pl.loop(first // tile, (first + size) // tile)(query_tile)
        if j == chunks - 1:
            send_dots()
        send_queries(j)

    @pl.when(outer)
    def _():
        latent_inward(0).start()
        latent_inward(1).start()
        for j in range(early, chunks):
            w_copy(0, 0, d, j, mid).start()
        start_feat(far_edge, other)
        keep_feat()

    def pass_on(j):
        w_copy(0, 0, edge, j, far_mid).wait_recv()
        w_copy(1, 2, edge, j, far_mid).start()

    @pl.when(inner)
    def _():
        latents[at_rows(2 * g, count), at_rows(m, width)] = latent_out[...]
        latent_inward(other).start()
        for o in range(1, n):
            latent_spread(slots[0], o).start()
        start_feat(far_edge, other)
        keep_feat()
        for j in range(early):
            pass_on(j)
        for slot in slots[1:]:
            latent_arrival(slot).wait_recv()
            for o in range(1, n):
                latent_spread(slot, o).start()

        for slot in slots[1:]:
            cot_arrival(slot).wait_recv()

        @pl.loop(0, half // tile)
        def _(t):
            at = at_rows(t, tile)
            cots[:, at] = cots[:, at] * keep_row(t).astype(cots.dtype)

        @pl.when(g == 1)
        def _():
            cots[:, :extra] = jnp.zeros((n * count, extra), cots.dtype)

        whole_grad(d)
        w_whole(0, far_mid).wait_recv()
        whole_grad(far_mid)
        latents_spread().wait_recv()
        last_total[...] = jnp.zeros_like(last_total)
        dot_total[...] = jnp.zeros_like(dot_total)
        passed = early
        for j in range(chunks):
            for _ in range(min(1 if j == 0 else 2, chunks - passed)):
                pass_on(passed)
                passed += 1
            finish_chunk(j)
            if j == 2:
                whole_grad(edge)

    to_peer(0, 0, square_in, square_in, far_mid).wait_send()
    for o in range(1, n):
        feat_whole(lax.rem(m + o, n), m).wait_send()
        feat_whole(m, lax.rem(m + o, n)).wait_recv()
    for kind, shard in enumerate(neighbours):
        down_crossed(kind, shard, g).wait_send()
    down_sent(0)
    cot_copy(0, cot_half(g), 2 * g, g, mid).wait_send()
    w_whole(0, d).wait_send()
    latent_inward(other).wait_send()

    @pl.when(outer)
    def _():
        cot_copy(1, cot_half(g), 2 * g, g, mid).wait_send()
        cot_across().wait_send()
        latent_inward(g).wait_send()

    @pl.when(inner)
    def _():
        for way in range(1, 5):
            down_sent(way)
        latents_spread().wait_send()

    def gathered(sem, held):
        return remote(held, held, grad_send.at[sem], grad_recv.at[sem], groups=other)

    def all_sources(sem, buffer):
        pl.when(inner)(lambda: gathered(sem, buffer.at[pl.ds(0, 2 * n - 1)]).wait_recv())
        pl.when(outer)(lambda: gathered(sem, buffer).wait_recv())

    all_sources(0, grad_in)
    grad_latent = grad_in[0].astype(jnp.float32)
    for source in range(1, 2 * n):
        grad_latent += grad_in[source].astype(jnp.float32)
    all_sources(1, dot_in)
    dots = dot_in[0]
    for source in range(1, 2 * n):
        dots += dot_in[source]
    inner_dot = jnp.broadcast_to(dots[:1], (128, count)).T[:, :1]
    scaled = gain_ref[...].reshape(1, width) * grad_latent
    root = root_ref[:, :1]
    slope = inner_dot / (width * n * (root * root))
    grad_raw[...] = (scaled / root - raw_ref[...] * slope).astype(grad_raw.dtype)

    far, near = lax.rem(m + 2, n), m + 1 - 2 * lax.rem(m, 2)
    far_near = lax.rem(near + 2, n)

    def block_copy(sem, source, who, to):
        return remote(
            source, grad_all.at[at_rows(who, count)], small_send.at[1 + sem],
            small_recv.at[1 + who], mp=to,
        )

    def block_arrival(who):
        held = grad_all.at[at_rows(who, count)]
        return remote(held, held, small_send.at[1], small_recv.at[1 + who], groups=other)

    block_copy(0, grad_raw, m, far).start()
    block_copy(1, grad_raw, m, near).start()

    def add_block(read, who, first, last):
        @pl.loop(0, down_rows // row_tile)
        def _(c):
            rows = at_rows(c, row_tile)
            value = contract_last(read(), down_feat[rows, at_rows(who, width)])
            if not first:
                value += token_total[:, rows]
            if last:
                token_out[:, rows] = value.astype(token_out.dtype)
            else:
                token_total[:, rows] = value

    row_tile = down_rows // 2 if down_rows % 256 == 0 else down_rows
    add_block(lambda: grad_raw[...], m, True, False)
    block_arrival(near).wait_recv()
    add_block(lambda: grad_all[at_rows(near, count), :], near, False, False)
    block_arrival(far).wait_recv()
    held = grad_all.at[at_rows(far, count)]
    block_copy(2, held, far, near).start()
    add_block(lambda: grad_all[at_rows(far, count), :], far, False, False)

    def query_arrival(plane):
        first = plane * cols - plane * (half - extra)
        part = queries_ref.at[:, pl.ds(first, half - plane * extra)]
        return remote(part, part, query_sem.at[2], query_sem.at[plane], groups=other)

    for plane in range(2):
        away = jnp.logical_not(jnp.logical_and(inner, g == plane))
        pl.when(away)(lambda plane=plane: query_arrival(plane).wait_recv())

    @pl.when(inner)
    def _():
        w_whole(1, edge).wait_send()
        for plane in range(2):

            @pl.when(g == plane)
            def _():
                size = half - plane * extra
                part = query_out.at[pl.ds(0, (n - 1) * count), pl.ds(0, size)]
                remote(
                    part, part, query_sem.at[2], query_sem.at[plane], groups=other
                ).wait_send()
                query_keep(half - size, size).wait()

        blocks = down_all.at[pl.ds(0, (n * n - 1) * count), pl.ds(0, depth)]
        gathered(0, blocks).wait_send()
        gathered(1, raw_ref.at[pl.ds(0, (n * n - 1) * 8), pl.ds(0, 128)]).wait_send()

    block_copy(0, grad_raw, m, far).wait_send()
    block_copy(1, grad_raw, m, near).wait_send()
    block_copy(2, held, far, near).wait_send()
    block_arrival(far_near).wait_recv()
    add_block(lambda: grad_all[at_rows(far_near, count), :], far_near, False, True)
    token_keep = pltpu.make_async_copy(token_out, grad_tokens_ref, local_sem.at[0])
    token_keep.start()
    token_keep.wait()


def project(tokens, w_down, gain, w_up, head_counts, cotangent):
    n = lax.axis_size("dp")
    count, cols = cotangent.shape
    depth = w_up.shape[0]
    down_rows, width = w_down.shape
    half = (cols // 128 + 1) // 2 * 128
    tile = 256 if half % 256 == 0 else 128
    tiles = half // tile
    ends = min(2, tiles - 1)
    body = tiles - ends
    sizes = []
    while sum(sizes) < body:
        left = body - sum(sizes)
        sizes.append(min(2, left))
    parts = len(sizes)
    cut = depth - 128
    spans = [(0, depth, sum(sizes[:i]) * tile, sizes[i] * tile) for i in range(parts)]
    for row, rows in ((0, cut), (cut, 128)):
        spans.append((row, rows, body * tile, ends * tile))
    spans = tuple(spans)
    parts = len(spans)
    pieces = 2
    vmem = pl.BlockSpec(memory_space=pltpu.VMEM)
    hbm = pl.BlockSpec(memory_space=pl.ANY)
    bf16, f32 = jnp.bfloat16, jnp.float32
    dma = pltpu.SemaphoreType.DMA
    return pl.pallas_call(
        functools.partial(project_kernel, n, spans, tile, pieces),
        out_shape=(
            jax.ShapeDtypeStruct((count, cols), bf16),
            jax.ShapeDtypeStruct((count, down_rows), bf16),
        ),
        in_specs=[hbm, hbm, vmem, hbm, pl.BlockSpec(memory_space=pltpu.SMEM), hbm],
        out_specs=(hbm, hbm),
        scratch_shapes=[
            pltpu.VMEM(tokens.shape, bf16),
            pltpu.VMEM((count, cols), bf16),
            pltpu.VMEM((count, half), bf16),
            pltpu.VMEM((n * down_rows, width), bf16),
            pltpu.VMEM((down_rows, n * width), bf16),
            pltpu.VMEM((n * depth, half), bf16),
            pltpu.VMEM((n * count, half), bf16),
            pltpu.VMEM((n * count, half), bf16),
            pltpu.VMEM((n * count, n * width), bf16),
            pltpu.VMEM((count, width), bf16),
            pltpu.VMEM((n * count, n * depth), bf16),
            pltpu.VMEM((2 * n, count, depth), bf16),
            pltpu.VMEM((n * count, depth), f32),
            pltpu.VMEM((n * count, depth), f32),
            pltpu.VMEM((count, width), f32),
            pltpu.VMEM((count, 128), f32),
            pltpu.VMEM((8, count), f32),
            pltpu.VMEM((n - 1, 8, count), f32),
            pltpu.VMEM((n * count, 128), f32),
            pltpu.VMEM((n, 8, count), f32),
            pltpu.VMEM((2 * n, 8, count), f32),
            pltpu.VMEM((count, width), bf16),
            pltpu.VMEM((n * count, width), bf16),
            pltpu.VMEM((count, down_rows), f32),
            pltpu.VMEM((count, down_rows), bf16),
            dma((4,)),
            dma((5,)),
            dma((3, pieces)),
            dma((3,)),
            dma((3,)),
            dma((n,)),
            dma((n,)),
            dma((3,)),
            dma((n + 1,)),
            dma((3,)),
            dma((n + 1,)),
            dma((2,)),
            dma((2 * parts + 1,)),
            dma((4,)),
            dma((2,)),
            dma((2,)),
            dma((4,)),
            dma((n + 1,)),
        ],
        compiler_params=pltpu.CompilerParams(
            collective_id=0, has_side_effects=True, vmem_limit_bytes=60 * 2**20
        ),
    )(tokens, w_down, gain, w_up, head_counts, cotangent)


def move_weights_body(tokens, w_down, gain, w_up, head_counts, cotangent):
    return project(tokens, w_down, gain, w_up, head_counts, cotangent)


def solution(mesh):
    in_specs = (
        P(("groups", "dp"), None),
        P("dp", "mp"),
        P("mp"),
        P("dp", "mp"),
        P(),
        P(("groups", "dp"), "mp"),
    )
    out_specs = (P(("groups", "dp"), "mp"), P(("groups", "dp"), "mp"))
    square = mesh.shape["dp"] == mesh.shape["mp"] == 4 and mesh.shape["groups"] == 2
    body = move_weights_body if square else gather_weights_body
    return jax.shard_map(body, mesh=mesh, in_specs=in_specs, out_specs=out_specs, check_vma=False)
```

```python
import functools

import jax
import jax.numpy as jnp
from jax import lax
from jax.experimental import pallas as pl
from jax.experimental.pallas import tpu as pltpu
from jax.sharding import PartitionSpec as P

HD = 192
MESH = pl.DeviceIdType.MESH


def contract_last(left, right):
    return lax.dot_general(
        left, right, (((1,), (1,)), ((), ())), preferred_element_type=jnp.float32
    )


def keep_mask_of(head_counts, block_cols):
    position = lax.axis_index("mp")
    held_heads = lax.dynamic_slice_in_dim(head_counts, position, 1, 0)
    slot_index = jnp.arange(block_cols, dtype=jnp.int32) // HD
    return (slot_index < held_heads).astype(jnp.float32)


def gather_weights_body(tokens, w_down, gain, w_up, head_counts, cotangent):
    latent_width = w_down.shape[1] * lax.axis_size("mp")
    keep_mask = keep_mask_of(head_counts, w_up.shape[1])
    down_whole = lax.all_gather(w_down, "dp", axis=0, tiled=True)
    latent_raw = jnp.dot(tokens, down_whole, preferred_element_type=jnp.float32)
    squares = lax.psum(jnp.sum(latent_raw * latent_raw, axis=1, keepdims=True), "mp")
    root_mean = jnp.sqrt(squares / latent_width + 1e-06)
    latent_local = (latent_raw / root_mean * gain).astype(jnp.bfloat16)
    latent = lax.all_gather(latent_local, "mp", axis=1, tiled=True)
    masked = cotangent * keep_mask.astype(jnp.bfloat16)
    up_whole = lax.all_gather(w_up, "dp", axis=0, tiled=True)
    query_total = jnp.dot(latent, up_whole, preferred_element_type=jnp.float32)
    grad_partial = contract_last(masked, up_whole)
    queries = (query_total * keep_mask).astype(jnp.bfloat16)
    grad_latent = lax.psum_scatter(
        grad_partial.astype(jnp.bfloat16), "mp", scatter_dimension=1, tiled=True
    ).astype(jnp.float32)
    inner_dot = lax.psum(jnp.sum(gain * grad_latent * latent_raw, axis=1, keepdims=True), "mp")
    grad_raw = (
        gain * grad_latent / root_mean - latent_raw * inner_dot / (latent_width * root_mean**3)
    ).astype(jnp.bfloat16)
    partial_value = contract_last(grad_raw, down_whole).astype(jnp.bfloat16)
    grad_tokens = lax.psum_scatter(partial_value, "mp", scatter_dimension=1, tiled=True)
    return (queries, grad_tokens)


def project_kernel(
    n, spans, tile, pieces, tokens_hbm, down_hbm, gain_hbm, w_hbm, counts_hbm, cot_hbm,
    queries_ref, grad_tokens_ref, gain_ref, counts_ref, tokens_ref, cot_ref, cot_pass, down_all, down_feat, w_all,
    cots, query_out, latents, latent_out, grad_out, grad_in, total, last_total, raw_ref,
    root_ref, square_out, square_in, dot_total, dot_out, dot_in, grad_raw, grad_all,
    token_total, token_out, local_sem, down_send, down_recv, across_send, across_recv,
    feat_send, feat_recv, cot_send, cot_recv, latent_send, latent_recv, w_send, w_recv,
    query_sem, grad_send, grad_recv, small_send, small_recv,
):
    g, d, m = lax.axis_index("groups"), lax.axis_index("dp"), lax.axis_index("mp")
    other = 1 - g
    upper = (d >= 2).astype(jnp.int32)
    mid, edge = 1 + upper, 3 * upper
    far_mid, far_edge = 2 - upper, 3 - 3 * upper
    inner = d == mid
    outer = jnp.logical_not(inner)
    role = 1 - inner.astype(jnp.int32)
    count, cols = cot_ref.shape
    depth = w_hbm.shape[0]
    down_rows, width = down_hbm.shape
    half = cots.shape[1]
    step = cols - half
    extra = half - step
    half_rows = down_rows // 2
    piece_rows = half_rows // pieces
    chunks = len(spans)

    def at_rows(k, size):
        return pl.ds(pl.multiple_of(k * size, size), size)

    down_load = pltpu.make_async_copy(
        down_hbm, down_all.at[at_rows(d, down_rows)], local_sem.at[0]
    )
    cot_load = pltpu.make_async_copy(cot_hbm, cot_ref, local_sem.at[1])
    w_load = pltpu.make_async_copy(
        w_hbm.at[:, pl.ds(pl.multiple_of(g * step, 128), half)],
        w_all.at[at_rows(d, depth)], local_sem.at[2],
    )
    tokens_load = pltpu.make_async_copy(tokens_hbm, tokens_ref, local_sem.at[3])
    down_load.start()
    cot_load.start()
    w_load.start()
    tokens_load.start()
    gain_load = pltpu.make_async_copy(gain_hbm, gain_ref, local_sem.at[4])
    counts_load = pltpu.make_async_copy(counts_hbm, counts_ref, local_sem.at[5])
    gain_load.start()
    counts_load.start()

    barrier = pltpu.get_barrier_semaphore()

    def greet(**where):
        pl.semaphore_signal(barrier, inc=1, device_id=where, device_id_type=MESH)

    for plane in range(2):
        for place in (0, 1):
            for who in range(n):
                there = mid if place == 0 else edge
                itself = jnp.logical_and(
                    g == plane, jnp.logical_and(role == place, m == who)
                )
                pl.when(jnp.logical_not(itself))(
                    lambda plane=plane, there=there, who=who: greet(
                        groups=plane, dp=there, mp=who
                    )
                )
    pl.when(inner)(lambda: greet(dp=far_mid))
    down_load.wait()
    pl.when(inner)(lambda: pl.semaphore_wait(barrier, 4 * n))
    pl.when(outer)(lambda: pl.semaphore_wait(barrier, 4 * n - 1))

    def remote(source, target, send, recv, **where):
        return pltpu.make_async_remote_copy(
            src_ref=source, dst_ref=target, send_sem=send, recv_sem=recv,
            device_id=where, device_id_type=MESH,
        )

    def down_piece(shard, plane, k):
        start = shard * down_rows + plane * half_rows + k * piece_rows
        return down_all.at[pl.ds(pl.multiple_of(start, piece_rows), piece_rows)]

    def down_copy(way, kind, shard, k, to):
        held = down_piece(shard, g, k)
        return remote(held, held, down_send.at[way], down_recv.at[kind, k], dp=to)

    def down_half(shard, plane):
        start = shard * down_rows + plane * half_rows
        return down_all.at[pl.ds(pl.multiple_of(start, piece_rows), half_rows)]

    def down_sent(way):
        held = down_half(d, g)
        remote(held, held, down_send.at[way], down_recv.at[0, 0], dp=far_mid).wait_send()

    def down_across(kind, shard, k):
        held = down_piece(shard, g, k)
        return remote(held, held, across_send.at[kind], across_recv.at[kind], groups=other)

    def down_crossed(kind, shard, plane):
        held = down_half(shard, plane)
        return remote(held, held, across_send.at[kind], across_recv.at[kind], groups=other)

    def cot_half(plane):
        return cot_ref.at[:, pl.ds(pl.multiple_of(plane * step, 128), half)]

    def cot_copy(way, source, slot, plane, to):
        return remote(
            source, cots.at[at_rows(slot, count)], cot_send.at[way], cot_recv.at[slot],
            groups=plane, dp=to,
        )

    def cot_across():
        return remote(
            cot_half(other), cot_pass, cot_send.at[2], cot_recv.at[n], groups=other
        )

    def cot_arrival(slot):
        held = cots.at[at_rows(slot, count)]
        return remote(held, held, cot_send.at[0], cot_recv.at[slot], dp=far_mid)

    def w_rows(shard, row, rows):
        return pl.ds(pl.multiple_of(shard * depth + row, 128), rows)

    def w_piece(shard, j):
        row, rows, first, size = spans[j]
        return w_all.at[w_rows(shard, row, rows), pl.ds(first, size)]

    def w_copy(way, kind, shard, j, to):
        held = w_piece(shard, j)
        sem = w_recv.at[2 * chunks] if kind == 1 else w_recv.at[kind // 2 * chunks + j]
        return remote(held, held, w_send.at[way], sem, dp=to)

    def w_whole(way, shard):
        held = w_all.at[at_rows(shard, depth), :]
        return remote(held, held, w_send.at[way], w_recv.at[2 * chunks], dp=far_mid)

    def keep_cot():
        cots[at_rows(2 * g, count), :] = cot_ref[
            :, pl.ds(pl.multiple_of(g * step, 128), half)
        ]

    def feat_copy(shard, plane, k):
        start = plane * half_rows + k * piece_rows
        rows = pl.ds(pl.multiple_of(start, piece_rows), piece_rows)
        return remote(
            down_piece(shard, plane, k), down_feat.at[rows, at_rows(m, width)],
            feat_send.at[shard], feat_recv.at[m], mp=shard,
        )

    def start_feat(shard, plane):
        @pl.when(shard != m)
        def _():
            for k in range(pieces):
                feat_copy(shard, plane, k).start()

    def feat_whole(sent, arrived):
        held = down_feat.at[:, at_rows(arrived, width)]
        return remote(held, held, feat_send.at[sent], feat_recv.at[arrived], groups=other)

    def keep_feat():
        @pl.loop(0, pieces * 2)
        def _(k):
            source = m * down_rows + k * piece_rows
            down_feat[at_rows(k, piece_rows), at_rows(m, width)] = down_all[
                pl.ds(pl.multiple_of(source, piece_rows), piece_rows), :
            ]

    def feat_piece(shard, plane, k):
        pl.when(shard != m)(lambda: feat_copy(shard, plane, k).start())

    early = 3

    @pl.when(inner)
    def _():
        for k in range(pieces):
            down_copy(0, 1, d, k, far_mid).start()
            down_copy(1, 0, d, k, edge).start()
        start_feat(d, 0)
        start_feat(d, 1)
        cot_load.wait()
        keep_cot()
        for k in range(pieces):
            for kind, shard, way, to in ((0, edge, 2, far_mid), (1, far_mid, 3, edge)):
                down_copy(way, kind, shard, k, to).wait_recv()
                down_copy(way, kind + (2 if kind == 0 else 0), shard, k, to).start()
                down_across(kind, shard, k).start()
                feat_piece(shard, g, k)
        w_load.wait()
        for j in range(chunks):
            w_copy(0, 1, d, j, far_mid).start()
        for k in range(pieces):
            down_copy(4, 2, far_edge, k, edge).wait_recv()
            down_copy(4, 2, far_edge, k, edge).start()
            down_across(2, far_edge, k).start()
            feat_piece(far_edge, g, k)
        cot_copy(0, cot_half(other), 2 * g, other, d).start()

    @pl.when(outer)
    def _():
        for k in range(pieces):
            down_copy(0, 0, d, k, mid).start()
        cot_load.wait()
        cot_across().start()
        cot_copy(0, cot_half(g), 2 * g + 1, g, mid).start()
        start_feat(d, 0)
        start_feat(d, 1)
        w_load.wait()
        for kind, shard in enumerate((mid, far_mid, far_edge)):
            for k in range(pieces):
                down_copy(0, kind, shard, k, mid).wait_recv()
                down_across(kind, shard, k).start()
                feat_piece(shard, g, k)
            if kind == 0:
                cot_across().wait_recv()
                cot_copy(1, cot_pass, 2 * other + 1, g, mid).start()
                for j in range(early):
                    w_copy(0, 0, d, j, mid).start()

    neighbours = (jnp.where(inner, edge, mid), far_mid, far_edge)
    for kind, shard in enumerate(neighbours):
        down_crossed(kind, shard, other).wait_recv()
        if kind < 2:
            start_feat(shard, other)

    tokens_load.wait()
    gain_load.wait()
    counts_load.wait()
    raw_ref[...] = jnp.zeros_like(raw_ref)

    @pl.loop(0, 2 * n)
    def _(c):
        at = at_rows(c, half_rows)
        raw_ref[...] += jnp.dot(
            tokens_ref[:, at], down_all[at, :], preferred_element_type=jnp.float32
        )

    def to_peer(sent, arrived, source, target, mp):
        return remote(source, target, small_send.at[sent], small_recv.at[arrived], mp=mp)

    raw = raw_ref[...]
    square_out[...] = jnp.broadcast_to(
        jnp.sum(raw * raw, axis=1, keepdims=True), (count, 128)
    ).T[:8]
    for o in range(1, n):
        to_peer(0, 0, square_out, square_in.at[o - 1], lax.rem(m + o, n)).start()
    to_peer(0, 0, square_in, square_in, far_mid).wait_recv()
    value = square_out[...]
    for o in range(1, n):
        value += square_in[o - 1]
    squares = jnp.broadcast_to(value[:1], (128, count)).T[:, :1]
    root = jnp.sqrt(squares / (width * n) + 1e-06)
    root_ref[...] = jnp.broadcast_to(root, root_ref.shape)
    gain = gain_ref[...].reshape(1, width)
    latent_out[...] = (raw / root * gain).astype(latent_out.dtype)

    def latent_at(slot, who):
        return latents.at[at_rows(slot, count), at_rows(who, width)]

    def latent_inward(to):
        return remote(
            latent_out, latent_at(2 * g + role, m), latent_send.at[to],
            latent_recv.at[2 * g + role], groups=to, dp=mid,
        )

    def latent_arrival(slot):
        held = latent_at(slot, m)
        return remote(held, held, latent_send.at[0], latent_recv.at[slot], dp=far_mid)

    def latent_spread(slot, o):
        held = latent_at(slot, m)
        return remote(
            held, held, latent_send.at[2], latent_recv.at[n], mp=lax.rem(m + o, n)
        )

    def latents_spread():
        held = latents.at[:, pl.ds(0, (n - 1) * width)]
        return remote(held, held, latent_send.at[2], latent_recv.at[n], dp=far_mid)

    slots = (2 * g, 2 * other, 2 * g + 1, 2 * other + 1)

    cut = depth - 128
    grad_parts = ((0, cut), (cut, 128))

    def add_grad(sum_ref, shard, row, rows, t):
        at = at_rows(t, tile)
        sum_ref[:, row:row + rows] += contract_last(
            cots[:, at], w_all[w_rows(shard, row, rows), at]
        )

    def grad_copy(shard, slot, part):
        row, rows = grad_parts[part]
        return remote(
            grad_out.at[at_rows(slot, count), w_rows(shard, row, rows)],
            grad_in.at[g * n + m, :, pl.ds(row, rows)],
            grad_send.at[0], grad_recv.at[0],
            groups=slot // 2, dp=mid if slot % 2 == 0 else edge, mp=shard,
        )

    def is_self(shard, slot):
        return jnp.logical_and(g == slot // 2, m == shard)

    def each_grad(shard, part, act):
        for slot in range(n):
            if slot % 2 == 1:
                act(grad_copy(shard, slot, part))
                continue
            pl.when(jnp.logical_not(is_self(shard, slot)))(
                lambda slot=slot: act(grad_copy(shard, slot, part))
            )

    def send_grad(sum_ref, shard, part):
        row, rows = grad_parts[part]
        grad_out[:, w_rows(shard, row, rows)] = sum_ref[:, row:row + rows].astype(
            grad_out.dtype
        )
        each_grad(shard, part, lambda c: c.start())

        @pl.when(m == shard)
        def _():
            grad_in[g * n + m, :, row:row + rows] = grad_out[
                at_rows(2 * g, count), w_rows(shard, row, rows)
            ]

    def whole_grad(shard):
        total[...] = jnp.zeros_like(total)

        @pl.loop(0, half // tile)
        def _(t):
            add_grad(total, shard, 0, depth, t)

        for part in range(2):
            send_grad(total, shard, part)

    def query_parts(j):
        row, rows, first, size = spans[j]
        if row + rows < depth:
            return ()
        if j == 0:
            return ((extra, size - extra, False), (0, extra, True))
        return ((first, size, False),)

    def query_copy(slot, first, size):
        return remote(
            query_out.at[at_rows(slot, count), pl.ds(first, size)],
            queries_ref.at[:, pl.ds(pl.multiple_of(g * step + first, 128), size)],
            query_sem.at[2], query_sem.at[g],
            groups=slot // 2, dp=mid if slot % 2 == 0 else edge,
        )

    def query_keep(first, size):
        return pltpu.make_async_copy(
            query_out.at[at_rows(2 * g, count), pl.ds(first, size)],
            queries_ref.at[:, pl.ds(pl.multiple_of(g * step + first, 128), size)],
            query_sem.at[3],
        )

    def send_queries(j):
        for first, size, once in query_parts(j):

            def act():
                for slot in range(n):
                    if slot % 2 == 1:
                        query_copy(slot, first, size).start()
                        continue
                    mine = g == slot // 2
                    pl.when(jnp.logical_not(mine))(
                        lambda slot=slot: query_copy(slot, first, size).start()
                    )
                query_keep(first, size).start()

            if once:
                pl.when(g == 0)(act)
            else:
                act()

    def keep_row(t):
        column = lax.broadcasted_iota(jnp.int32, (1, tile), 1) + (g * step + t * tile)
        return (column < counts_ref[m] * HD).astype(jnp.float32)

    def query_tile(t):
        at = at_rows(t, tile)
        product = jnp.dot(latents[...], w_all[:, at], preferred_element_type=jnp.float32)
        query_out[:, at] = (product * keep_row(t)).astype(query_out.dtype)
        dots = product * cots[:, at].astype(jnp.float32)
        for part in range(tile // 128):
            dot_total[...] += dots[:, part * 128:(part + 1) * 128]

    def dot_copy(slot, to):
        return remote(
            dot_out.at[slot], dot_in.at[g * n + m], grad_send.at[1], grad_recv.at[1],
            groups=slot // 2,
            dp=mid if slot % 2 == 0 else edge, mp=to,
        )

    def each_dot(act):
        for slot in range(n):
            for to in range(n):
                if slot % 2 == 1:
                    act(dot_copy(slot, to))
                    continue
                pl.when(jnp.logical_not(is_self(to, slot)))(
                    lambda slot=slot, to=to: act(dot_copy(slot, to))
                )

    def send_dots():
        for slot in range(n):
            column = jnp.sum(dot_total[at_rows(slot, count), :], axis=1, keepdims=True)
            dot_out[slot] = jnp.broadcast_to(column, (count, 128)).T[:8]
        each_dot(lambda c: c.start())
        dot_in[g * n + m] = dot_out[2 * g]

    def finish_chunk(j):
        row, rows, first, size = spans[j]
        w_copy(0, 2, far_edge, j, far_mid).wait_recv()

        @pl.loop(first // tile, (first + size) // tile)
        def _(t):
            add_grad(last_total, far_edge, row, rows, t)

        if j == chunks - 2:
            send_grad(last_total, far_edge, 0)
        if j == chunks - 1:
            send_grad(last_total, far_edge, 1)
        if row + rows == depth:
            pl.loop(first // tile, (first + size) // tile)(query_tile)
        if j == chunks - 1:
            send_dots()
        send_queries(j)

    @pl.when(outer)
    def _():
        latent_inward(0).start()
        latent_inward(1).start()
        for j in range(early, chunks):
            w_copy(0, 0, d, j, mid).start()
        start_feat(far_edge, other)
        keep_feat()

    def pass_on(j):
        w_copy(0, 0, edge, j, far_mid).wait_recv()
        w_copy(1, 2, edge, j, far_mid).start()

    @pl.when(inner)
    def _():
        latents[at_rows(2 * g, count), at_rows(m, width)] = latent_out[...]
        latent_inward(other).start()
        for o in range(1, n):
            latent_spread(slots[0], o).start()
        start_feat(far_edge, other)
        keep_feat()
        for j in range(early):
            pass_on(j)
        for slot in slots[1:]:
            latent_arrival(slot).wait_recv()
            for o in range(1, n):
                latent_spread(slot, o).start()

        for slot in slots[1:]:
            cot_arrival(slot).wait_recv()

        @pl.loop(0, half // tile)
        def _(t):
            at = at_rows(t, tile)
            cots[:, at] = cots[:, at] * keep_row(t).astype(cots.dtype)

        @pl.when(g == 1)
        def _():
            cots[:, :extra] = jnp.zeros((n * count, extra), cots.dtype)

        whole_grad(d)
        w_whole(0, far_mid).wait_recv()
        whole_grad(far_mid)
        latents_spread().wait_recv()
        last_total[...] = jnp.zeros_like(last_total)
        dot_total[...] = jnp.zeros_like(dot_total)
        passed = early
        for j in range(chunks):
            for _ in range(min(1 if j == 0 else 2, chunks - passed)):
                pass_on(passed)
                passed += 1
            finish_chunk(j)
            if j == 2:
                whole_grad(edge)

    to_peer(0, 0, square_in, square_in, far_mid).wait_send()
    for o in range(1, n):
        feat_whole(lax.rem(m + o, n), m).wait_send()
        feat_whole(m, lax.rem(m + o, n)).wait_recv()
    for kind, shard in enumerate(neighbours):
        down_crossed(kind, shard, g).wait_send()
    down_sent(0)
    cot_copy(0, cot_half(g), 2 * g, g, mid).wait_send()
    w_whole(0, d).wait_send()
    latent_inward(other).wait_send()

    @pl.when(outer)
    def _():
        cot_copy(1, cot_half(g), 2 * g, g, mid).wait_send()
        cot_across().wait_send()
        latent_inward(g).wait_send()

    @pl.when(inner)
    def _():
        for way in range(1, 5):
            down_sent(way)
        latents_spread().wait_send()

    def gathered(sem, held):
        return remote(held, held, grad_send.at[sem], grad_recv.at[sem], groups=other)

    def all_sources(sem, buffer):
        pl.when(inner)(lambda: gathered(sem, buffer.at[pl.ds(0, 2 * n - 1)]).wait_recv())
        pl.when(outer)(lambda: gathered(sem, buffer).wait_recv())

    all_sources(0, grad_in)
    grad_latent = grad_in[0].astype(jnp.float32)
    for source in range(1, 2 * n):
        grad_latent += grad_in[source].astype(jnp.float32)
    all_sources(1, dot_in)
    dots = dot_in[0]
    for source in range(1, 2 * n):
        dots += dot_in[source]
    inner_dot = jnp.broadcast_to(dots[:1], (128, count)).T[:, :1]
    scaled = gain_ref[...].reshape(1, width) * grad_latent
    root = root_ref[:, :1]
    slope = inner_dot / (width * n * (root * root))
    grad_raw[...] = (scaled / root - raw_ref[...] * slope).astype(grad_raw.dtype)

    far, near = lax.rem(m + 2, n), m + 1 - 2 * lax.rem(m, 2)
    far_near = lax.rem(near + 2, n)

    def block_copy(sem, source, who, to):
        return remote(
            source, grad_all.at[at_rows(who, count)], small_send.at[1 + sem],
            small_recv.at[1 + who], mp=to,
        )

    def block_arrival(who):
        held = grad_all.at[at_rows(who, count)]
        return remote(held, held, small_send.at[1], small_recv.at[1 + who], groups=other)

    block_copy(0, grad_raw, m, far).start()
    block_copy(1, grad_raw, m, near).start()

    def add_block(read, who, first, last):
        @pl.loop(0, down_rows // row_tile)
        def _(c):
            rows = at_rows(c, row_tile)
            value = contract_last(read(), down_feat[rows, at_rows(who, width)])
            if not first:
                value += token_total[:, rows]
            if last:
                token_out[:, rows] = value.astype(token_out.dtype)
            else:
                token_total[:, rows] = value

    row_tile = down_rows // 2 if down_rows % 256 == 0 else down_rows
    add_block(lambda: grad_raw[...], m, True, False)
    block_arrival(near).wait_recv()
    add_block(lambda: grad_all[at_rows(near, count), :], near, False, False)
    block_arrival(far).wait_recv()
    held = grad_all.at[at_rows(far, count)]
    block_copy(2, held, far, near).start()
    add_block(lambda: grad_all[at_rows(far, count), :], far, False, False)

    def query_arrival(plane):
        first = plane * cols - plane * (half - extra)
        part = queries_ref.at[:, pl.ds(first, half - plane * extra)]
        return remote(part, part, query_sem.at[2], query_sem.at[plane], groups=other)

    for plane in range(2):
        away = jnp.logical_not(jnp.logical_and(inner, g == plane))
        pl.when(away)(lambda plane=plane: query_arrival(plane).wait_recv())

    @pl.when(inner)
    def _():
        w_whole(1, edge).wait_send()
        for plane in range(2):

            @pl.when(g == plane)
            def _():
                size = half - plane * extra
                part = query_out.at[pl.ds(0, (n - 1) * count), pl.ds(0, size)]
                remote(
                    part, part, query_sem.at[2], query_sem.at[plane], groups=other
                ).wait_send()
                query_keep(half - size, size).wait()

        blocks = down_all.at[pl.ds(0, (n * n - 1) * count), pl.ds(0, depth)]
        gathered(0, blocks).wait_send()
        gathered(1, raw_ref.at[pl.ds(0, (n * n - 1) * 8), pl.ds(0, 128)]).wait_send()

    block_copy(0, grad_raw, m, far).wait_send()
    block_copy(1, grad_raw, m, near).wait_send()
    block_copy(2, held, far, near).wait_send()
    block_arrival(far_near).wait_recv()
    add_block(lambda: grad_all[at_rows(far_near, count), :], far_near, False, True)
    token_keep = pltpu.make_async_copy(token_out, grad_tokens_ref, local_sem.at[0])
    token_keep.start()
    token_keep.wait()


def project(tokens, w_down, gain, w_up, head_counts, cotangent):
    n = lax.axis_size("dp")
    count, cols = cotangent.shape
    depth = w_up.shape[0]
    down_rows, width = w_down.shape
    half = (cols // 128 + 1) // 2 * 128
    tile = 256 if half % 256 == 0 else 128
    tiles = half // tile
    ends = min(2, tiles - 1)
    body = tiles - ends
    sizes = []
    while sum(sizes) < body:
        left = body - sum(sizes)
        sizes.append(min(2, left))
    parts = len(sizes)
    cut = depth - 128
    spans = [(0, depth, sum(sizes[:i]) * tile, sizes[i] * tile) for i in range(parts)]
    for row, rows in ((0, cut), (cut, 128)):
        spans.append((row, rows, body * tile, ends * tile))
    spans = tuple(spans)
    parts = len(spans)
    pieces = 2
    hbm = pl.BlockSpec(memory_space=pl.ANY)
    bf16, f32 = jnp.bfloat16, jnp.float32
    dma = pltpu.SemaphoreType.DMA
    return pl.pallas_call(
        functools.partial(project_kernel, n, spans, tile, pieces),
        out_shape=(
            jax.ShapeDtypeStruct((count, cols), bf16),
            jax.ShapeDtypeStruct((count, down_rows), bf16),
        ),
        in_specs=[hbm] * 6,
        out_specs=(hbm, hbm),
        scratch_shapes=[
            pltpu.VMEM(gain.shape, f32),
            pltpu.SMEM(head_counts.shape, jnp.int32),
            pltpu.VMEM(tokens.shape, bf16),
            pltpu.VMEM((count, cols), bf16),
            pltpu.VMEM((count, half), bf16),
            pltpu.VMEM((n * down_rows, width), bf16),
            pltpu.VMEM((down_rows, n * width), bf16),
            pltpu.VMEM((n * depth, half), bf16),
            pltpu.VMEM((n * count, half), bf16),
            pltpu.VMEM((n * count, half), bf16),
            pltpu.VMEM((n * count, n * width), bf16),
            pltpu.VMEM((count, width), bf16),
            pltpu.VMEM((n * count, n * depth), bf16),
            pltpu.VMEM((2 * n, count, depth), bf16),
            pltpu.VMEM((n * count, depth), f32),
            pltpu.VMEM((n * count, depth), f32),
            pltpu.VMEM((count, width), f32),
            pltpu.VMEM((count, 128), f32),
            pltpu.VMEM((8, count), f32),
            pltpu.VMEM((n - 1, 8, count), f32),
            pltpu.VMEM((n * count, 128), f32),
            pltpu.VMEM((n, 8, count), f32),
            pltpu.VMEM((2 * n, 8, count), f32),
            pltpu.VMEM((count, width), bf16),
            pltpu.VMEM((n * count, width), bf16),
            pltpu.VMEM((count, down_rows), f32),
            pltpu.VMEM((count, down_rows), bf16),
            dma((6,)),
            dma((5,)),
            dma((3, pieces)),
            dma((3,)),
            dma((3,)),
            dma((n,)),
            dma((n,)),
            dma((3,)),
            dma((n + 1,)),
            dma((3,)),
            dma((n + 1,)),
            dma((2,)),
            dma((2 * parts + 1,)),
            dma((4,)),
            dma((2,)),
            dma((2,)),
            dma((4,)),
            dma((n + 1,)),
        ],
        compiler_params=pltpu.CompilerParams(
            collective_id=0, has_side_effects=True, vmem_limit_bytes=60 * 2**20
        ),
    )(tokens, w_down, gain, w_up, head_counts, cotangent)


def store_kernel(parts, queries_in, grad_in, queries_out, grad_out, held, grad, sem):
    rows = held.shape[0] // parts

    def span(k):
        return pl.ds(k * rows, rows)

    reads = [
        pltpu.make_async_copy(queries_in.at[span(k)], held.at[span(k)], sem.at[0, k])
        for k in range(parts)
    ] + [pltpu.make_async_copy(grad_in, grad, sem.at[0, parts])]
    writes = [
        pltpu.make_async_copy(held.at[span(k)], queries_out.at[span(k)], sem.at[1, k])
        for k in range(parts)
    ] + [pltpu.make_async_copy(grad, grad_out, sem.at[1, parts])]
    for read in reads:
        read.start()
    for read, write in zip(reads, writes):
        read.wait()
        write.start()
    for write in writes:
        write.wait()


def store(queries, grad_tokens):
    parts = 4
    hbm = pl.BlockSpec(memory_space=pl.ANY)
    return pl.pallas_call(
        functools.partial(store_kernel, parts),
        out_shape=(
            jax.ShapeDtypeStruct(queries.shape, queries.dtype),
            jax.ShapeDtypeStruct(grad_tokens.shape, grad_tokens.dtype),
        ),
        in_specs=[hbm] * 2,
        out_specs=(hbm,) * 2,
        scratch_shapes=[
            pltpu.VMEM(queries.shape, queries.dtype),
            pltpu.VMEM(grad_tokens.shape, grad_tokens.dtype),
            pltpu.SemaphoreType.DMA((2, parts + 1)),
        ],
    )(queries, grad_tokens)


def move_weights_body(tokens, w_down, gain, w_up, head_counts, cotangent):
    return store(*project(tokens, w_down, gain, w_up, head_counts, cotangent))


def solution(mesh):
    in_specs = (
        P(("groups", "dp"), None),
        P("dp", "mp"),
        P("mp"),
        P("dp", "mp"),
        P(),
        P(("groups", "dp"), "mp"),
    )
    out_specs = (P(("groups", "dp"), "mp"), P(("groups", "dp"), "mp"))
    square = mesh.shape["dp"] == mesh.shape["mp"] == 4 and mesh.shape["groups"] == 2
    body = move_weights_body if square else gather_weights_body
    return jax.shard_map(body, mesh=mesh, in_specs=in_specs, out_specs=out_specs, check_vma=False)
```

```python
import functools

import jax
import jax.numpy as jnp
from jax import lax
from jax.experimental import pallas as pl
from jax.experimental.pallas import tpu as pltpu
from jax.sharding import PartitionSpec as P

HD = 192
MESH = pl.DeviceIdType.MESH


def contract_last(left, right):
    return lax.dot_general(
        left, right, (((1,), (1,)), ((), ())), preferred_element_type=jnp.float32
    )


def keep_mask_of(head_counts, block_cols):
    position = lax.axis_index("mp")
    held_heads = lax.dynamic_slice_in_dim(head_counts, position, 1, 0)
    slot_index = jnp.arange(block_cols, dtype=jnp.int32) // HD
    return (slot_index < held_heads).astype(jnp.float32)


def gather_weights_body(tokens, w_down, gain, w_up, head_counts, cotangent):
    latent_width = w_down.shape[1] * lax.axis_size("mp")
    keep_mask = keep_mask_of(head_counts, w_up.shape[1])
    down_whole = lax.all_gather(w_down, "dp", axis=0, tiled=True)
    latent_raw = jnp.dot(tokens, down_whole, preferred_element_type=jnp.float32)
    squares = lax.psum(jnp.sum(latent_raw * latent_raw, axis=1, keepdims=True), "mp")
    root_mean = jnp.sqrt(squares / latent_width + 1e-06)
    latent_local = (latent_raw / root_mean * gain).astype(jnp.bfloat16)
    latent = lax.all_gather(latent_local, "mp", axis=1, tiled=True)
    masked = cotangent * keep_mask.astype(jnp.bfloat16)
    up_whole = lax.all_gather(w_up, "dp", axis=0, tiled=True)
    query_total = jnp.dot(latent, up_whole, preferred_element_type=jnp.float32)
    grad_partial = contract_last(masked, up_whole)
    queries = (query_total * keep_mask).astype(jnp.bfloat16)
    grad_latent = lax.psum_scatter(
        grad_partial.astype(jnp.bfloat16), "mp", scatter_dimension=1, tiled=True
    ).astype(jnp.float32)
    inner_dot = lax.psum(jnp.sum(gain * grad_latent * latent_raw, axis=1, keepdims=True), "mp")
    grad_raw = (
        gain * grad_latent / root_mean - latent_raw * inner_dot / (latent_width * root_mean**3)
    ).astype(jnp.bfloat16)
    partial_value = contract_last(grad_raw, down_whole).astype(jnp.bfloat16)
    grad_tokens = lax.psum_scatter(partial_value, "mp", scatter_dimension=1, tiled=True)
    return (queries, grad_tokens)


def project_kernel(
    n, spans, tile, pieces, tokens_hbm, down_hbm, gain_hbm, w_hbm, counts_hbm, cot_hbm,
    queries_ref, grad_tokens_ref, gain_ref, counts_ref, tokens_ref, cot_ref, cot_pass, down_all, down_feat, w_all,
    cots, query_out, latents, latent_out, grad_out, grad_in, total, last_total, raw_ref,
    root_ref, square_out, square_in, dot_total, dot_out, dot_in, grad_raw, grad_all,
    token_total, token_out, local_sem, down_send, down_recv, across_send, across_recv,
    feat_send, feat_recv, cot_send, cot_recv, latent_send, latent_recv, w_send, w_recv,
    query_sem, grad_send, grad_recv, small_send, small_recv,
):
    g, d, m = lax.axis_index("groups"), lax.axis_index("dp"), lax.axis_index("mp")
    other = 1 - g
    upper = (d >= 2).astype(jnp.int32)
    mid, edge = 1 + upper, 3 * upper
    far_mid, far_edge = 2 - upper, 3 - 3 * upper
    inner = d == mid
    outer = jnp.logical_not(inner)
    role = 1 - inner.astype(jnp.int32)
    count, cols = cot_ref.shape
    depth = w_hbm.shape[0]
    down_rows, width = down_hbm.shape
    half = cots.shape[1]
    step = cols - half
    extra = half - step
    spare_rows = extra * depth // width
    plane_rows = (down_rows - spare_rows) // 2
    piece_rows = plane_rows // pieces
    chunks = len(spans)

    def at_rows(k, size):
        return pl.ds(pl.multiple_of(k * size, size), size)

    down_load = pltpu.make_async_copy(
        down_hbm, down_all.at[at_rows(d, down_rows)], local_sem.at[0]
    )
    cot_load = pltpu.make_async_copy(cot_hbm, cot_ref, local_sem.at[1])
    w_load = pltpu.make_async_copy(
        w_hbm.at[:, pl.ds(pl.multiple_of(g * step, 128), half)],
        w_all.at[at_rows(d, depth)], local_sem.at[2],
    )
    tokens_load = pltpu.make_async_copy(tokens_hbm, tokens_ref, local_sem.at[3])
    down_load.start()
    cot_load.start()
    w_load.start()
    tokens_load.start()
    gain_load = pltpu.make_async_copy(gain_hbm, gain_ref, local_sem.at[4])
    counts_load = pltpu.make_async_copy(counts_hbm, counts_ref, local_sem.at[5])
    gain_load.start()
    counts_load.start()

    barrier = pltpu.get_barrier_semaphore()

    def greet(**where):
        pl.semaphore_signal(barrier, inc=1, device_id=where, device_id_type=MESH)

    for plane in range(2):
        for place in (0, 1):
            for who in range(n):
                there = mid if place == 0 else edge
                itself = jnp.logical_and(
                    g == plane, jnp.logical_and(role == place, m == who)
                )
                pl.when(jnp.logical_not(itself))(
                    lambda plane=plane, there=there, who=who: greet(
                        groups=plane, dp=there, mp=who
                    )
                )
    pl.when(inner)(lambda: greet(dp=far_mid))
    down_load.wait()
    pl.when(inner)(lambda: pl.semaphore_wait(barrier, 4 * n))
    pl.when(outer)(lambda: pl.semaphore_wait(barrier, 4 * n - 1))

    def remote(source, target, send, recv, **where):
        return pltpu.make_async_remote_copy(
            src_ref=source, dst_ref=target, send_sem=send, recv_sem=recv,
            device_id=where, device_id_type=MESH,
        )

    def down_span(plane, k):
        if k == pieces:
            return plane_rows, spare_rows
        return plane * (plane_rows + spare_rows) + k * piece_rows, piece_rows

    def down_piece(shard, plane, k):
        start, rows = down_span(plane, k)
        return down_all.at[pl.ds(pl.multiple_of(shard * down_rows + start, 16), rows)]

    def down_copy(way, kind, shard, k, to):
        held = down_piece(shard, g, k)
        return remote(held, held, down_send.at[way], down_recv.at[kind, k], dp=to)

    def down_across(kind, shard, k):
        held = down_piece(shard, g, k)
        return remote(held, held, across_send.at[kind], across_recv.at[kind], groups=other)

    def for_each_plane(body):
        for plane in range(2):
            pl.when(g == plane)(lambda plane=plane: body(plane))

    def moved_rows(shard, plane):
        rows = plane_rows + plane * spare_rows
        start = shard * down_rows + plane * plane_rows
        return down_all.at[pl.ds(pl.multiple_of(start, 16), rows)]

    def down_sent(way):
        def wait(plane):
            held = moved_rows(d, plane)
            remote(
                held, held, down_send.at[way], down_recv.at[0, 0], dp=far_mid
            ).wait_send()

        for_each_plane(wait)

    def crossed(kind, shard, plane):
        held = moved_rows(shard, plane)
        return remote(held, held, across_send.at[kind], across_recv.at[kind], groups=other)

    def each_piece(act):
        for k in range(pieces):
            act(k)
        pl.when(g == 1)(lambda: act(pieces))

    def cot_half(plane):
        return cot_ref.at[:, pl.ds(pl.multiple_of(plane * step, 128), half)]

    def cot_copy(way, source, slot, plane, to):
        return remote(
            source, cots.at[at_rows(slot, count)], cot_send.at[way], cot_recv.at[slot],
            groups=plane, dp=to,
        )

    def cot_across():
        return remote(
            cot_half(other), cot_pass, cot_send.at[2], cot_recv.at[n], groups=other
        )

    def cot_arrival(slot):
        held = cots.at[at_rows(slot, count)]
        return remote(held, held, cot_send.at[0], cot_recv.at[slot], dp=far_mid)

    def w_rows(shard, row, rows):
        return pl.ds(pl.multiple_of(shard * depth + row, 128), rows)

    def w_piece(shard, j):
        row, rows, first, size = spans[j]
        return w_all.at[w_rows(shard, row, rows), pl.ds(first, size)]

    def w_copy(way, kind, shard, j, to):
        held = w_piece(shard, j)
        sem = w_recv.at[2 * chunks] if kind == 1 else w_recv.at[kind // 2 * chunks + j]
        return remote(held, held, w_send.at[way], sem, dp=to)

    def w_moved(way, shard, plane):
        first = plane * extra
        held = w_all.at[at_rows(shard, depth), pl.ds(first, half - first)]
        return remote(held, held, w_send.at[way], w_recv.at[2 * chunks], dp=far_mid)

    def for_chunk(j, act):
        if j == 0:
            pl.when(g == 0)(act)
        else:
            act()

    def keep_cot():
        cots[at_rows(2 * g, count), :] = cot_ref[
            :, pl.ds(pl.multiple_of(g * step, 128), half)
        ]

    def feat_copy(shard, plane, k):
        start, rows = down_span(plane, k)
        return remote(
            down_piece(shard, plane, k),
            down_feat.at[pl.ds(pl.multiple_of(start, 16), rows), at_rows(m, width)],
            feat_send.at[shard], feat_recv.at[m], mp=shard,
        )

    def feat_piece(shard, plane, k):
        pl.when(shard != m)(lambda: feat_copy(shard, plane, k).start())

    def crossed_feat(shard):
        for k in range(pieces):
            feat_piece(shard, other, k)
        pl.when(g == 0)(lambda: feat_piece(shard, other, pieces))

    def feat_whole(sent, arrived):
        held = down_feat.at[:, at_rows(arrived, width)]
        return remote(held, held, feat_send.at[sent], feat_recv.at[arrived], groups=other)

    def keep_feat():
        @pl.loop(0, down_rows // 128)
        def _(k):
            source = m * down_rows + k * 128
            down_feat[at_rows(k, 128), at_rows(m, width)] = down_all[
                pl.ds(pl.multiple_of(source, 128), 128), :
            ]

    early = 4

    @pl.when(inner)
    def _():
        def start_own(k):
            down_copy(0, 1, d, k, far_mid).start()
            down_copy(1, 0, d, k, edge).start()

        each_piece(start_own)
        for k in range(pieces + 1):
            feat_piece(d, 0, k)
        for k in range(pieces):
            feat_piece(d, 1, k)
        cot_load.wait()
        keep_cot()

        @pl.when(g == 1)
        def _():
            for shard in (edge, far_mid, far_edge):
                w_all[at_rows(shard, depth), :extra] = jnp.zeros((depth, extra), w_all.dtype)

        def pass_near(k):
            for kind, sent, shard, way, to in (
                (0, 2, edge, 2, far_mid), (1, 1, far_mid, 3, edge)
            ):
                down_copy(way, kind, shard, k, to).wait_recv()
                down_copy(way, sent, shard, k, to).start()
                down_across(kind, shard, k).start()
                feat_piece(shard, g, k)

        each_piece(pass_near)
        w_load.wait()
        for j in range(chunks):
            for_chunk(j, lambda j=j: w_copy(0, 1, d, j, far_mid).start())

        def pass_far(k):
            down_copy(4, 2, far_edge, k, edge).wait_recv()
            down_copy(4, 2, far_edge, k, edge).start()
            down_across(2, far_edge, k).start()
            feat_piece(far_edge, g, k)

        each_piece(pass_far)
        cot_copy(0, cot_half(other), 2 * g, other, d).start()

    @pl.when(outer)
    def _():
        each_piece(lambda k: down_copy(0, 0, d, k, mid).start())
        cot_load.wait()
        cot_across().start()
        cot_copy(0, cot_half(g), 2 * g + 1, g, mid).start()
        for k in range(pieces + 1):
            feat_piece(d, 0, k)
        for k in range(pieces):
            feat_piece(d, 1, k)
        w_load.wait()
        for kind, shard in enumerate((mid, far_mid, far_edge)):

            def take(k):
                down_copy(0, kind, shard, k, mid).wait_recv()
                down_across(kind, shard, k).start()
                feat_piece(shard, g, k)

            each_piece(take)
            if kind == 0:
                cot_across().wait_recv()
                cot_copy(1, cot_pass, 2 * other + 1, g, mid).start()
                for j in range(early):
                    for_chunk(j, lambda j=j: w_copy(0, 0, d, j, mid).start())

    neighbours = (jnp.where(inner, edge, mid), far_mid, far_edge)
    for kind, shard in enumerate(neighbours):
        for_each_plane(lambda plane: crossed(kind, shard, 1 - plane).wait_recv())
        if kind < 2:
            crossed_feat(shard)

    tokens_load.wait()
    gain_load.wait()
    counts_load.wait()
    raw_ref[...] = jnp.zeros_like(raw_ref)

    @pl.loop(0, 2 * n)
    def _(c):
        at = at_rows(c, down_rows // 2)
        raw_ref[...] += jnp.dot(
            tokens_ref[:, at], down_all[at, :], preferred_element_type=jnp.float32
        )

    def to_peer(sent, arrived, source, target, mp):
        return remote(source, target, small_send.at[sent], small_recv.at[arrived], mp=mp)

    raw = raw_ref[...]
    square_out[...] = jnp.broadcast_to(
        jnp.sum(raw * raw, axis=1, keepdims=True), (count, 128)
    ).T[:8]
    for o in range(1, n):
        to_peer(0, 0, square_out, square_in.at[o - 1], lax.rem(m + o, n)).start()
    to_peer(0, 0, square_in, square_in, far_mid).wait_recv()
    value = square_out[...]
    for o in range(1, n):
        value += square_in[o - 1]
    squares = jnp.broadcast_to(value[:1], (128, count)).T[:, :1]
    root = jnp.sqrt(squares / (width * n) + 1e-06)
    root_ref[...] = jnp.broadcast_to(root, root_ref.shape)
    gain = gain_ref[...].reshape(1, width)
    latent_out[...] = (raw / root * gain).astype(latent_out.dtype)

    def latent_at(slot, who):
        return latents.at[at_rows(slot, count), at_rows(who, width)]

    def latent_inward(to):
        return remote(
            latent_out, latent_at(2 * g + role, m), latent_send.at[to],
            latent_recv.at[2 * g + role], groups=to, dp=mid,
        )

    def latent_arrival(slot):
        held = latent_at(slot, m)
        return remote(held, held, latent_send.at[0], latent_recv.at[slot], dp=far_mid)

    def latent_spread(slot, o):
        held = latent_at(slot, m)
        return remote(
            held, held, latent_send.at[2], latent_recv.at[n], mp=lax.rem(m + o, n)
        )

    def latents_spread():
        held = latents.at[:, pl.ds(0, (n - 1) * width)]
        return remote(held, held, latent_send.at[2], latent_recv.at[n], dp=far_mid)

    slots = (2 * g, 2 * other, 2 * g + 1, 2 * other + 1)

    cut = depth - 128
    grad_parts = ((0, cut), (cut, 128))

    def add_grad(sum_ref, shard, row, rows, t):
        at = at_rows(t, tile)
        sum_ref[:, row:row + rows] += contract_last(
            cots[:, at], w_all[w_rows(shard, row, rows), at]
        )

    def grad_copy(shard, slot, part):
        row, rows = grad_parts[part]
        return remote(
            grad_out.at[at_rows(slot, count), w_rows(shard, row, rows)],
            grad_in.at[g * n + m, :, pl.ds(row, rows)],
            grad_send.at[0], grad_recv.at[0],
            groups=slot // 2, dp=mid if slot % 2 == 0 else edge, mp=shard,
        )

    def is_self(shard, slot):
        return jnp.logical_and(g == slot // 2, m == shard)

    def each_grad(shard, part, act):
        for slot in range(n):
            if slot % 2 == 1:
                act(grad_copy(shard, slot, part))
                continue
            pl.when(jnp.logical_not(is_self(shard, slot)))(
                lambda slot=slot: act(grad_copy(shard, slot, part))
            )

    def send_grad(sum_ref, shard, part):
        row, rows = grad_parts[part]
        grad_out[:, w_rows(shard, row, rows)] = sum_ref[:, row:row + rows].astype(
            grad_out.dtype
        )
        each_grad(shard, part, lambda c: c.start())

        @pl.when(m == shard)
        def _():
            grad_in[g * n + m, :, row:row + rows] = grad_out[
                at_rows(2 * g, count), w_rows(shard, row, rows)
            ]

    def whole_grad(shard):
        total[...] = jnp.zeros_like(total)

        @pl.loop(0, half // tile)
        def _(t):
            add_grad(total, shard, 0, depth, t)

        for part in range(2):
            send_grad(total, shard, part)

    def query_parts(j):
        row, rows, first, size = spans[j]
        if row + rows < depth:
            return ()
        return ((first, size, j == 0),)

    def query_copy(slot, first, size):
        return remote(
            query_out.at[at_rows(slot, count), pl.ds(first, size)],
            queries_ref.at[:, pl.ds(pl.multiple_of(g * step + first, 128), size)],
            query_sem.at[2], query_sem.at[g],
            groups=slot // 2, dp=mid if slot % 2 == 0 else edge,
        )

    def query_keep(first, size):
        return pltpu.make_async_copy(
            query_out.at[at_rows(2 * g, count), pl.ds(first, size)],
            queries_ref.at[:, pl.ds(pl.multiple_of(g * step + first, 128), size)],
            query_sem.at[3],
        )

    def send_queries(j):
        for first, size, once in query_parts(j):

            def act():
                for slot in range(n):
                    if slot % 2 == 1:
                        query_copy(slot, first, size).start()
                        continue
                    mine = g == slot // 2
                    pl.when(jnp.logical_not(mine))(
                        lambda slot=slot: query_copy(slot, first, size).start()
                    )
                query_keep(first, size).start()

            if once:
                pl.when(g == 0)(act)
            else:
                act()

    def keep_row(t):
        column = lax.broadcasted_iota(jnp.int32, (1, tile), 1) + (g * step + t * tile)
        return (column < counts_ref[m] * HD).astype(jnp.float32)

    def query_tile(t):
        at = at_rows(t, tile)
        product = jnp.dot(latents[...], w_all[:, at], preferred_element_type=jnp.float32)
        query_out[:, at] = (product * keep_row(t)).astype(query_out.dtype)
        dots = product * cots[:, at].astype(jnp.float32)
        for part in range(tile // 128):
            dot_total[...] += dots[:, part * 128:(part + 1) * 128]

    def dot_copy(slot, to):
        return remote(
            dot_out.at[slot], dot_in.at[g * n + m], grad_send.at[1], grad_recv.at[1],
            groups=slot // 2,
            dp=mid if slot % 2 == 0 else edge, mp=to,
        )

    def each_dot(act):
        for slot in range(n):
            for to in range(n):
                if slot % 2 == 1:
                    act(dot_copy(slot, to))
                    continue
                pl.when(jnp.logical_not(is_self(to, slot)))(
                    lambda slot=slot, to=to: act(dot_copy(slot, to))
                )

    def send_dots():
        for slot in range(n):
            column = jnp.sum(dot_total[at_rows(slot, count), :], axis=1, keepdims=True)
            dot_out[slot] = jnp.broadcast_to(column, (count, 128)).T[:8]
        each_dot(lambda c: c.start())
        dot_in[g * n + m] = dot_out[2 * g]

    def finish_chunk(j):
        row, rows, first, size = spans[j]
        for_chunk(j, w_copy(0, 2, far_edge, j, far_mid).wait_recv)
        if j == 0:
            return
        if j == 1:
            first, size = 0, first + size

        @pl.loop(first // tile, (first + size) // tile)
        def _(t):
            add_grad(last_total, far_edge, row, rows, t)

        if j == chunks - 2:
            send_grad(last_total, far_edge, 0)
        if j == chunks - 1:
            send_grad(last_total, far_edge, 1)
        if row + rows == depth:
            pl.loop(first // tile, (first + size) // tile)(query_tile)
        if j == chunks - 1:
            send_dots()
        if j == 1:
            send_queries(0)
        send_queries(j)

    @pl.when(outer)
    def _():
        latent_inward(0).start()
        latent_inward(1).start()
        for j in range(early, chunks):
            for_chunk(j, lambda j=j: w_copy(0, 0, d, j, mid).start())
        crossed_feat(far_edge)
        keep_feat()

    def pass_on(j):
        def act():
            w_copy(0, 0, edge, j, far_mid).wait_recv()
            w_copy(1, 2, edge, j, far_mid).start()

        for_chunk(j, act)

    @pl.when(inner)
    def _():
        latents[at_rows(2 * g, count), at_rows(m, width)] = latent_out[...]
        latent_inward(other).start()
        for o in range(1, n):
            latent_spread(slots[0], o).start()
        crossed_feat(far_edge)
        keep_feat()
        for j in range(early):
            pass_on(j)
        for slot in slots[1:]:
            latent_arrival(slot).wait_recv()
            for o in range(1, n):
                latent_spread(slot, o).start()

        for slot in slots[1:]:
            cot_arrival(slot).wait_recv()

        @pl.loop(0, half // tile)
        def _(t):
            at = at_rows(t, tile)
            cots[:, at] = cots[:, at] * keep_row(t).astype(cots.dtype)

        @pl.when(g == 1)
        def _():
            cots[:, :extra] = jnp.zeros((n * count, extra), cots.dtype)

        whole_grad(d)
        for_each_plane(lambda plane: w_moved(0, far_mid, plane).wait_recv())
        whole_grad(far_mid)
        latents_spread().wait_recv()
        last_total[...] = jnp.zeros_like(last_total)
        dot_total[...] = jnp.zeros_like(dot_total)
        passed = early
        for j in range(chunks):
            for _ in range(min((0, 1)[j] if j < 2 else 2, chunks - passed)):
                pass_on(passed)
                passed += 1
            finish_chunk(j)
            if j == 3:
                whole_grad(edge)

    to_peer(0, 0, square_in, square_in, far_mid).wait_send()
    for o in range(1, n):
        feat_whole(lax.rem(m + o, n), m).wait_send()
        feat_whole(m, lax.rem(m + o, n)).wait_recv()
    for kind, shard in enumerate(neighbours):
        for_each_plane(lambda plane: crossed(kind, shard, plane).wait_send())
    down_sent(0)
    cot_copy(0, cot_half(g), 2 * g, g, mid).wait_send()

    def w_own_sent(plane):
        w_moved(0, d, plane).wait_send()

    for_each_plane(w_own_sent)
    latent_inward(other).wait_send()

    @pl.when(outer)
    def _():
        cot_copy(1, cot_half(g), 2 * g, g, mid).wait_send()
        cot_across().wait_send()
        latent_inward(g).wait_send()

    @pl.when(inner)
    def _():
        for way in range(1, 5):
            down_sent(way)
        latents_spread().wait_send()

    def gathered(sem, held):
        return remote(held, held, grad_send.at[sem], grad_recv.at[sem], groups=other)

    def all_sources(sem, buffer):
        pl.when(inner)(lambda: gathered(sem, buffer.at[pl.ds(0, 2 * n - 1)]).wait_recv())
        pl.when(outer)(lambda: gathered(sem, buffer).wait_recv())

    all_sources(0, grad_in)
    grad_latent = grad_in[0].astype(jnp.float32)
    for source in range(1, 2 * n):
        grad_latent += grad_in[source].astype(jnp.float32)
    all_sources(1, dot_in)
    dots = dot_in[0]
    for source in range(1, 2 * n):
        dots += dot_in[source]
    inner_dot = jnp.broadcast_to(dots[:1], (128, count)).T[:, :1]
    scaled = gain_ref[...].reshape(1, width) * grad_latent
    root = root_ref[:, :1]
    slope = inner_dot / (width * n * (root * root))
    grad_raw[...] = (scaled / root - raw_ref[...] * slope).astype(grad_raw.dtype)

    far, near = lax.rem(m + 2, n), m + 1 - 2 * lax.rem(m, 2)
    far_near = lax.rem(near + 2, n)

    def block_copy(sem, source, who, to):
        return remote(
            source, grad_all.at[at_rows(who, count)], small_send.at[1 + sem],
            small_recv.at[1 + who], mp=to,
        )

    def block_arrival(who):
        held = grad_all.at[at_rows(who, count)]
        return remote(held, held, small_send.at[1], small_recv.at[1 + who], groups=other)

    block_copy(0, grad_raw, m, far).start()
    block_copy(1, grad_raw, m, near).start()

    def add_block(read, who, first, last):
        @pl.loop(0, down_rows // row_tile)
        def _(c):
            rows = at_rows(c, row_tile)
            value = contract_last(read(), down_feat[rows, at_rows(who, width)])
            if not first:
                value += token_total[:, rows]
            if last:
                token_out[:, rows] = value.astype(token_out.dtype)
            else:
                token_total[:, rows] = value

    row_tile = down_rows // 2 if down_rows % 256 == 0 else down_rows
    add_block(lambda: grad_raw[...], m, True, False)
    block_arrival(near).wait_recv()
    add_block(lambda: grad_all[at_rows(near, count), :], near, False, False)
    block_arrival(far).wait_recv()
    held = grad_all.at[at_rows(far, count)]
    block_copy(2, held, far, near).start()
    add_block(lambda: grad_all[at_rows(far, count), :], far, False, False)

    def query_arrival(plane):
        first = plane * cols - plane * (half - extra)
        part = queries_ref.at[:, pl.ds(first, half - plane * extra)]
        return remote(part, part, query_sem.at[2], query_sem.at[plane], groups=other)

    for plane in range(2):
        away = jnp.logical_not(jnp.logical_and(inner, g == plane))
        pl.when(away)(lambda plane=plane: query_arrival(plane).wait_recv())

    @pl.when(inner)
    def _():
        for_each_plane(lambda plane: w_moved(1, edge, plane).wait_send())
        for plane in range(2):

            @pl.when(g == plane)
            def _():
                size = half - plane * extra
                part = query_out.at[pl.ds(0, (n - 1) * count), pl.ds(0, size)]
                remote(
                    part, part, query_sem.at[2], query_sem.at[plane], groups=other
                ).wait_send()
                query_keep(half - size, size).wait()

        blocks = down_all.at[pl.ds(0, (n * n - 1) * count), pl.ds(0, depth)]
        gathered(0, blocks).wait_send()
        gathered(1, raw_ref.at[pl.ds(0, (n * n - 1) * 8), pl.ds(0, 128)]).wait_send()

    block_copy(0, grad_raw, m, far).wait_send()
    block_copy(1, grad_raw, m, near).wait_send()
    block_copy(2, held, far, near).wait_send()
    block_arrival(far_near).wait_recv()
    add_block(lambda: grad_all[at_rows(far_near, count), :], far_near, False, True)
    token_keep = pltpu.make_async_copy(token_out, grad_tokens_ref, local_sem.at[0])
    token_keep.start()
    token_keep.wait()


def project(tokens, w_down, gain, w_up, head_counts, cotangent):
    n = lax.axis_size("dp")
    count, cols = cotangent.shape
    depth = w_up.shape[0]
    down_rows, width = w_down.shape
    half = (cols // 128 + 1) // 2 * 128
    tile = 256 if half % 256 == 0 else 128
    tiles = half // tile
    ends = min(2, tiles - 1)
    body = tiles - ends
    sizes = []
    while sum(sizes) < body:
        left = body - sum(sizes)
        sizes.append(min(2, left))
    parts = len(sizes)
    cut = depth - 128
    spans = [(0, depth, sum(sizes[:i]) * tile, sizes[i] * tile) for i in range(parts)]
    extra = 2 * half - cols
    spans[0] = (0, depth, extra, sizes[0] * tile - extra)
    spans.insert(0, (0, depth, 0, extra))
    for row, rows in ((0, cut), (cut, 128)):
        spans.append((row, rows, body * tile, ends * tile))
    spans = tuple(spans)
    parts = len(spans)
    pieces = 2
    hbm = pl.BlockSpec(memory_space=pl.ANY)
    bf16, f32 = jnp.bfloat16, jnp.float32
    dma = pltpu.SemaphoreType.DMA
    return pl.pallas_call(
        functools.partial(project_kernel, n, spans, tile, pieces),
        out_shape=(
            jax.ShapeDtypeStruct((count, cols), bf16),
            jax.ShapeDtypeStruct((count, down_rows), bf16),
        ),
        in_specs=[hbm] * 6,
        out_specs=(hbm, hbm),
        scratch_shapes=[
            pltpu.VMEM(gain.shape, f32),
            pltpu.SMEM(head_counts.shape, jnp.int32),
            pltpu.VMEM(tokens.shape, bf16),
            pltpu.VMEM((count, cols), bf16),
            pltpu.VMEM((count, half), bf16),
            pltpu.VMEM((n * down_rows, width), bf16),
            pltpu.VMEM((down_rows, n * width), bf16),
            pltpu.VMEM((n * depth, half), bf16),
            pltpu.VMEM((n * count, half), bf16),
            pltpu.VMEM((n * count, half), bf16),
            pltpu.VMEM((n * count, n * width), bf16),
            pltpu.VMEM((count, width), bf16),
            pltpu.VMEM((n * count, n * depth), bf16),
            pltpu.VMEM((2 * n, count, depth), bf16),
            pltpu.VMEM((n * count, depth), f32),
            pltpu.VMEM((n * count, depth), f32),
            pltpu.VMEM((count, width), f32),
            pltpu.VMEM((count, 128), f32),
            pltpu.VMEM((8, count), f32),
            pltpu.VMEM((n - 1, 8, count), f32),
            pltpu.VMEM((n * count, 128), f32),
            pltpu.VMEM((n, 8, count), f32),
            pltpu.VMEM((2 * n, 8, count), f32),
            pltpu.VMEM((count, width), bf16),
            pltpu.VMEM((n * count, width), bf16),
            pltpu.VMEM((count, down_rows), f32),
            pltpu.VMEM((count, down_rows), bf16),
            dma((6,)),
            dma((5,)),
            dma((3, pieces + 1)),
            dma((3,)),
            dma((3,)),
            dma((n,)),
            dma((n,)),
            dma((3,)),
            dma((n + 1,)),
            dma((3,)),
            dma((n + 1,)),
            dma((2,)),
            dma((2 * parts + 1,)),
            dma((4,)),
            dma((2,)),
            dma((2,)),
            dma((4,)),
            dma((n + 1,)),
        ],
        compiler_params=pltpu.CompilerParams(
            collective_id=0, has_side_effects=True, vmem_limit_bytes=60 * 2**20
        ),
    )(tokens, w_down, gain, w_up, head_counts, cotangent)


def store_kernel(parts, queries_in, grad_in, queries_out, grad_out, held, grad, sem):
    rows = held.shape[0] // parts

    def span(k):
        return pl.ds(k * rows, rows)

    reads = [
        pltpu.make_async_copy(queries_in.at[span(k)], held.at[span(k)], sem.at[0, k])
        for k in range(parts)
    ] + [pltpu.make_async_copy(grad_in, grad, sem.at[0, parts])]
    writes = [
        pltpu.make_async_copy(held.at[span(k)], queries_out.at[span(k)], sem.at[1, k])
        for k in range(parts)
    ] + [pltpu.make_async_copy(grad, grad_out, sem.at[1, parts])]
    for read in reads:
        read.start()
    for read, write in zip(reads, writes):
        read.wait()
        write.start()
    for write in writes:
        write.wait()


def store(queries, grad_tokens):
    parts = 4
    hbm = pl.BlockSpec(memory_space=pl.ANY)
    return pl.pallas_call(
        functools.partial(store_kernel, parts),
        out_shape=(
            jax.ShapeDtypeStruct(queries.shape, queries.dtype),
            jax.ShapeDtypeStruct(grad_tokens.shape, grad_tokens.dtype),
        ),
        in_specs=[hbm] * 2,
        out_specs=(hbm,) * 2,
        scratch_shapes=[
            pltpu.VMEM(queries.shape, queries.dtype),
            pltpu.VMEM(grad_tokens.shape, grad_tokens.dtype),
            pltpu.SemaphoreType.DMA((2, parts + 1)),
        ],
    )(queries, grad_tokens)


def move_weights_body(tokens, w_down, gain, w_up, head_counts, cotangent):
    return store(*project(tokens, w_down, gain, w_up, head_counts, cotangent))


def solution(mesh):
    in_specs = (
        P(("groups", "dp"), None),
        P("dp", "mp"),
        P("mp"),
        P("dp", "mp"),
        P(),
        P(("groups", "dp"), "mp"),
    )
    out_specs = (P(("groups", "dp"), "mp"), P(("groups", "dp"), "mp"))
    square = mesh.shape["dp"] == mesh.shape["mp"] == 4 and mesh.shape["groups"] == 2
    body = move_weights_body if square else gather_weights_body
    return jax.shard_map(body, mesh=mesh, in_specs=in_specs, out_specs=out_specs, check_vma=False)
```

```python
import functools

import jax
import jax.numpy as jnp
from jax import lax
from jax.experimental import pallas as pl
from jax.experimental.pallas import tpu as pltpu
from jax.sharding import PartitionSpec as P

HD = 192
MESH = pl.DeviceIdType.MESH


def contract_last(left, right):
    return lax.dot_general(
        left, right, (((1,), (1,)), ((), ())), preferred_element_type=jnp.float32
    )


def keep_mask_of(head_counts, block_cols):
    position = lax.axis_index("mp")
    held_heads = lax.dynamic_slice_in_dim(head_counts, position, 1, 0)
    slot_index = jnp.arange(block_cols, dtype=jnp.int32) // HD
    return (slot_index < held_heads).astype(jnp.float32)


def gather_weights_body(tokens, w_down, gain, w_up, head_counts, cotangent):
    latent_width = w_down.shape[1] * lax.axis_size("mp")
    keep_mask = keep_mask_of(head_counts, w_up.shape[1])
    down_whole = lax.all_gather(w_down, "dp", axis=0, tiled=True)
    latent_raw = jnp.dot(tokens, down_whole, preferred_element_type=jnp.float32)
    squares = lax.psum(jnp.sum(latent_raw * latent_raw, axis=1, keepdims=True), "mp")
    root_mean = jnp.sqrt(squares / latent_width + 1e-06)
    latent_local = (latent_raw / root_mean * gain).astype(jnp.bfloat16)
    latent = lax.all_gather(latent_local, "mp", axis=1, tiled=True)
    masked = cotangent * keep_mask.astype(jnp.bfloat16)
    up_whole = lax.all_gather(w_up, "dp", axis=0, tiled=True)
    query_total = jnp.dot(latent, up_whole, preferred_element_type=jnp.float32)
    grad_partial = contract_last(masked, up_whole)
    queries = (query_total * keep_mask).astype(jnp.bfloat16)
    grad_latent = lax.psum_scatter(
        grad_partial.astype(jnp.bfloat16), "mp", scatter_dimension=1, tiled=True
    ).astype(jnp.float32)
    inner_dot = lax.psum(jnp.sum(gain * grad_latent * latent_raw, axis=1, keepdims=True), "mp")
    grad_raw = (
        gain * grad_latent / root_mean - latent_raw * inner_dot / (latent_width * root_mean**3)
    ).astype(jnp.bfloat16)
    partial_value = contract_last(grad_raw, down_whole).astype(jnp.bfloat16)
    grad_tokens = lax.psum_scatter(partial_value, "mp", scatter_dimension=1, tiled=True)
    return (queries, grad_tokens)


def project_kernel(
    n, spans, tile, pieces, tokens_hbm, down_hbm, gain_hbm, w_hbm, counts_hbm, cot_hbm,
    queries_ref, grad_tokens_ref, gain_ref, counts_ref, tokens_ref, cot_ref, cot_pass, down_all, down_feat, w_all,
    cots, query_out, latents, latent_out, grad_out, grad_in, total, last_total, raw_ref,
    root_ref, square_out, square_in, dot_total, dot_out, dot_in, raw_all, block_all, grad_all, query_part,
    token_total, token_out, local_sem, down_send, down_recv, across_send, across_recv,
    feat_send, feat_recv, cot_send, cot_recv, latent_send, latent_recv, w_send, w_recv,
    query_sem, grad_send, grad_recv, small_send, small_recv, peer_send, peer_recv,
):
    g, d, m = lax.axis_index("groups"), lax.axis_index("dp"), lax.axis_index("mp")
    other = 1 - g
    upper = (d >= 2).astype(jnp.int32)
    mid, edge = 1 + upper, 3 * upper
    far_mid, far_edge = 2 - upper, 3 - 3 * upper
    inner = d == mid
    outer = jnp.logical_not(inner)
    role = 1 - inner.astype(jnp.int32)
    count, cols = cot_ref.shape
    depth = w_hbm.shape[0]
    down_rows, width = down_hbm.shape
    half = cots.shape[1]
    step = cols - half
    extra = half - step
    spare_rows = extra * depth // width
    plane_rows = (down_rows - spare_rows) // 2
    piece_rows = plane_rows // pieces
    chunks = len(spans)

    def at_rows(k, size):
        return pl.ds(pl.multiple_of(k * size, size), size)

    down_load = pltpu.make_async_copy(
        down_hbm, down_all.at[at_rows(d, down_rows)], local_sem.at[0]
    )
    cot_load = pltpu.make_async_copy(cot_hbm, cot_ref, local_sem.at[1])
    w_load = pltpu.make_async_copy(
        w_hbm.at[:, pl.ds(pl.multiple_of(g * step, 128), half)],
        w_all.at[at_rows(d, depth)], local_sem.at[2],
    )
    tokens_load = pltpu.make_async_copy(tokens_hbm, tokens_ref, local_sem.at[3])
    down_load.start()
    cot_load.start()
    w_load.start()
    tokens_load.start()
    gain_load = pltpu.make_async_copy(gain_hbm, gain_ref, local_sem.at[4])
    counts_load = pltpu.make_async_copy(counts_hbm, counts_ref, local_sem.at[5])
    gain_load.start()
    counts_load.start()

    barrier = pltpu.get_barrier_semaphore()

    def greet(**where):
        pl.semaphore_signal(barrier, inc=1, device_id=where, device_id_type=MESH)

    for plane in range(2):
        for place in (0, 1):
            for who in range(n):
                there = mid if place == 0 else edge
                itself = jnp.logical_and(
                    g == plane, jnp.logical_and(role == place, m == who)
                )
                pl.when(jnp.logical_not(itself))(
                    lambda plane=plane, there=there, who=who: greet(
                        groups=plane, dp=there, mp=who
                    )
                )
    pl.when(inner)(lambda: greet(dp=far_mid))
    down_load.wait()
    pl.when(inner)(lambda: pl.semaphore_wait(barrier, 4 * n))
    pl.when(outer)(lambda: pl.semaphore_wait(barrier, 4 * n - 1))

    def remote(source, target, send, recv, **where):
        return pltpu.make_async_remote_copy(
            src_ref=source, dst_ref=target, send_sem=send, recv_sem=recv,
            device_id=where, device_id_type=MESH,
        )

    def down_span(plane, k):
        if k == pieces:
            return plane_rows, spare_rows
        return plane * (plane_rows + spare_rows) + k * piece_rows, piece_rows

    def down_piece(shard, plane, k):
        start, rows = down_span(plane, k)
        return down_all.at[pl.ds(pl.multiple_of(shard * down_rows + start, 16), rows)]

    def down_copy(way, kind, shard, k, to):
        held = down_piece(shard, g, k)
        return remote(held, held, down_send.at[way], down_recv.at[kind, k], dp=to)

    def down_across(kind, shard, k):
        held = down_piece(shard, g, k)
        return remote(held, held, across_send.at[kind], across_recv.at[kind], groups=other)

    def for_each_plane(body):
        for plane in range(2):
            pl.when(g == plane)(lambda plane=plane: body(plane))

    def moved_rows(shard, plane):
        rows = plane_rows + plane * spare_rows
        start = shard * down_rows + plane * plane_rows
        return down_all.at[pl.ds(pl.multiple_of(start, 16), rows)]

    def down_sent(way):
        def wait(plane):
            held = moved_rows(d, plane)
            remote(
                held, held, down_send.at[way], down_recv.at[0, 0], dp=far_mid
            ).wait_send()

        for_each_plane(wait)

    def crossed(kind, shard, plane):
        held = moved_rows(shard, plane)
        return remote(held, held, across_send.at[kind], across_recv.at[kind], groups=other)

    def each_piece(act):
        for k in range(pieces):
            act(k)
        pl.when(g == 1)(lambda: act(pieces))

    def cot_half(plane):
        return cot_ref.at[:, pl.ds(pl.multiple_of(plane * step, 128), half)]

    def cot_copy(way, source, slot, plane, to):
        return remote(
            source, cots.at[at_rows(slot, count)], cot_send.at[way], cot_recv.at[slot],
            groups=plane, dp=to,
        )

    def cot_across():
        return remote(
            cot_half(other), cot_pass, cot_send.at[2], cot_recv.at[n], groups=other
        )

    def cot_arrival(slot):
        held = cots.at[at_rows(slot, count)]
        return remote(held, held, cot_send.at[0], cot_recv.at[slot], dp=far_mid)

    def w_rows(shard, row, rows):
        return pl.ds(pl.multiple_of(shard * depth + row, 128), rows)

    def w_piece(shard, j):
        row, rows, first, size = spans[j]
        return w_all.at[w_rows(shard, row, rows), pl.ds(first, size)]

    def w_copy(way, kind, shard, j, to):
        held = w_piece(shard, j)
        sem = w_recv.at[2 * chunks] if kind == 1 else w_recv.at[kind // 2 * chunks + j]
        return remote(held, held, w_send.at[way], sem, dp=to)

    def w_moved(way, shard, plane):
        first = plane * extra
        held = w_all.at[at_rows(shard, depth), pl.ds(first, half - first)]
        return remote(held, held, w_send.at[way], w_recv.at[2 * chunks], dp=far_mid)

    def for_chunk(j, act):
        if j == 0:
            pl.when(g == 0)(act)
        else:
            act()

    def keep_cot():
        cots[at_rows(2 * g, count), :] = cot_ref[
            :, pl.ds(pl.multiple_of(g * step, 128), half)
        ]

    def feat_copy(shard, plane, k):
        start, rows = down_span(plane, k)
        return remote(
            down_piece(shard, plane, k),
            down_feat.at[pl.ds(pl.multiple_of(start, 16), rows), at_rows(m, width)],
            feat_send.at[shard], feat_recv.at[m], mp=shard,
        )

    def feat_piece(shard, plane, k):
        pl.when(shard != m)(lambda: feat_copy(shard, plane, k).start())

    def crossed_feat(shard):
        for k in range(pieces):
            feat_piece(shard, other, k)
        pl.when(g == 0)(lambda: feat_piece(shard, other, pieces))

    def feat_whole(sent, arrived):
        held = down_feat.at[:, at_rows(arrived, width)]
        return remote(held, held, feat_send.at[sent], feat_recv.at[arrived], groups=other)

    def keep_feat():
        @pl.loop(0, down_rows // 128)
        def _(k):
            source = m * down_rows + k * 128
            down_feat[at_rows(k, 128), at_rows(m, width)] = down_all[
                pl.ds(pl.multiple_of(source, 128), 128), :
            ]

    early = 4

    @pl.when(inner)
    def _():
        def start_own(k):
            down_copy(0, 1, d, k, far_mid).start()
            down_copy(1, 0, d, k, edge).start()

        each_piece(start_own)
        for k in range(pieces + 1):
            feat_piece(d, 0, k)
        for k in range(pieces):
            feat_piece(d, 1, k)
        cot_load.wait()
        keep_cot()

        @pl.when(g == 1)
        def _():
            for shard in (edge, far_mid, far_edge):
                w_all[at_rows(shard, depth), :extra] = jnp.zeros((depth, extra), w_all.dtype)

        def pass_near(k):
            for kind, sent, shard, way, to in (
                (0, 2, edge, 2, far_mid), (1, 1, far_mid, 3, edge)
            ):
                down_copy(way, kind, shard, k, to).wait_recv()
                down_copy(way, sent, shard, k, to).start()
                down_across(kind, shard, k).start()
                feat_piece(shard, g, k)

        each_piece(pass_near)
        w_load.wait()
        for j in range(chunks):
            for_chunk(j, lambda j=j: w_copy(0, 1, d, j, far_mid).start())

        def pass_far(k):
            down_copy(4, 2, far_edge, k, edge).wait_recv()
            down_copy(4, 2, far_edge, k, edge).start()
            down_across(2, far_edge, k).start()
            feat_piece(far_edge, g, k)

        each_piece(pass_far)
        cot_copy(0, cot_half(other), 2 * g, other, d).start()

    @pl.when(outer)
    def _():
        each_piece(lambda k: down_copy(0, 0, d, k, mid).start())
        cot_load.wait()
        cot_across().start()
        cot_copy(0, cot_half(g), 2 * g + 1, g, mid).start()
        for k in range(pieces + 1):
            feat_piece(d, 0, k)
        for k in range(pieces):
            feat_piece(d, 1, k)
        w_load.wait()
        for kind, shard in enumerate((mid, far_mid, far_edge)):

            def take(k):
                down_copy(0, kind, shard, k, mid).wait_recv()
                down_across(kind, shard, k).start()
                feat_piece(shard, g, k)

            each_piece(take)
            if kind == 0:
                cot_across().wait_recv()
                cot_copy(1, cot_pass, 2 * other + 1, g, mid).start()
                for j in range(early):
                    for_chunk(j, lambda j=j: w_copy(0, 0, d, j, mid).start())

    neighbours = (jnp.where(inner, edge, mid), far_mid, far_edge)
    for kind, shard in enumerate(neighbours):
        for_each_plane(lambda plane: crossed(kind, shard, 1 - plane).wait_recv())
        if kind < 2:
            crossed_feat(shard)

    tokens_load.wait()
    gain_load.wait()
    counts_load.wait()
    raw_ref[...] = jnp.zeros_like(raw_ref)

    @pl.loop(0, 2 * n)
    def _(c):
        at = at_rows(c, down_rows // 2)
        raw_ref[...] += jnp.dot(
            tokens_ref[:, at], down_all[at, :], preferred_element_type=jnp.float32
        )

    def to_peer(sent, arrived, source, target, mp):
        return remote(source, target, small_send.at[sent], small_recv.at[arrived], mp=mp)

    raw = raw_ref[...]
    square_out[...] = jnp.broadcast_to(
        jnp.sum(raw * raw, axis=1, keepdims=True), (count, 128)
    ).T[:8]
    for o in range(1, n):
        to_peer(0, 0, square_out, square_in.at[o - 1], lax.rem(m + o, n)).start()
    to_peer(0, 0, square_in, square_in, far_mid).wait_recv()
    value = square_out[...]
    for o in range(1, n):
        value += square_in[o - 1]
    squares = jnp.broadcast_to(value[:1], (128, count)).T[:, :1]
    root = jnp.sqrt(squares / (width * n) + 1e-06)
    root_ref[...] = jnp.broadcast_to(root, root_ref.shape)
    gain = gain_ref[...].reshape(1, width)
    latent_out[...] = (raw / root * gain).astype(latent_out.dtype)

    def latent_at(slot, who):
        return latents.at[at_rows(slot, count), at_rows(who, width)]

    def latent_inward(to):
        return remote(
            latent_out, latent_at(2 * g + role, m), latent_send.at[to],
            latent_recv.at[2 * g + role], groups=to, dp=mid,
        )

    def latent_arrival(slot):
        held = latent_at(slot, m)
        return remote(held, held, latent_send.at[0], latent_recv.at[slot], dp=far_mid)

    def latent_spread(slot, o):
        held = latent_at(slot, m)
        return remote(
            held, held, latent_send.at[2], latent_recv.at[n], mp=lax.rem(m + o, n)
        )

    def latents_spread():
        held = latents.at[:, pl.ds(0, (n - 1) * width)]
        return remote(held, held, latent_send.at[2], latent_recv.at[n], dp=far_mid)

    slots = (2 * g, 2 * other, 2 * g + 1, 2 * other + 1)

    cut = depth - 128
    grad_parts = ((0, cut), (cut, 128))

    def add_grad(sum_ref, shard, row, rows, t):
        at = at_rows(t, tile)
        sum_ref[:, row:row + rows] += contract_last(
            cots[:, at], w_all[w_rows(shard, row, rows), at]
        )

    def grad_copy(shard, slot, part):
        row, rows = grad_parts[part]
        return remote(
            grad_out.at[at_rows(slot, count), w_rows(shard, row, rows)],
            grad_in.at[g * n + m, :, pl.ds(row, rows)],
            grad_send.at[0], grad_recv.at[0],
            groups=slot // 2, dp=mid if slot % 2 == 0 else edge, mp=shard,
        )

    def is_self(shard, slot):
        return jnp.logical_and(g == slot // 2, m == shard)

    def each_grad(shard, part, act):
        for slot in range(n):
            if slot % 2 == 1:
                act(grad_copy(shard, slot, part))
                continue
            pl.when(jnp.logical_not(is_self(shard, slot)))(
                lambda slot=slot: act(grad_copy(shard, slot, part))
            )

    def send_grad(sum_ref, shard, part):
        row, rows = grad_parts[part]
        grad_out[:, w_rows(shard, row, rows)] = sum_ref[:, row:row + rows].astype(
            grad_out.dtype
        )
        each_grad(shard, part, lambda c: c.start())

        @pl.when(m == shard)
        def _():
            grad_in[g * n + m, :, row:row + rows] = grad_out[
                at_rows(2 * g, count), w_rows(shard, row, rows)
            ]

    def whole_grad(shard):
        total[...] = jnp.zeros_like(total)

        @pl.loop(0, half // tile)
        def _(t):
            add_grad(total, shard, 0, depth, t)

        for part in range(2):
            send_grad(total, shard, part)

    def query_parts(j):
        row, rows, first, size = spans[j]
        if row + rows < depth:
            return ()
        return ((first, size, j == 0),)

    def query_copy(slot, first, size):
        return remote(
            query_out.at[at_rows(slot, count), pl.ds(first, size)],
            queries_ref.at[:, pl.ds(pl.multiple_of(g * step + first, 128), size)],
            query_sem.at[2], query_sem.at[g],
            groups=slot // 2, dp=mid if slot % 2 == 0 else edge,
        )

    def query_keep(first, size):
        return pltpu.make_async_copy(
            query_out.at[at_rows(2 * g, count), pl.ds(first, size)],
            queries_ref.at[:, pl.ds(pl.multiple_of(g * step + first, 128), size)],
            query_sem.at[3],
        )

    def send_queries(j):
        for first, size, once in query_parts(j):

            def act():
                for slot in range(n):
                    if slot % 2 == 1:
                        query_copy(slot, first, size).start()
                        continue
                    mine = g == slot // 2
                    pl.when(jnp.logical_not(mine))(
                        lambda slot=slot: query_copy(slot, first, size).start()
                    )
                query_keep(first, size).start()

            if once:
                pl.when(g == 0)(act)
            else:
                act()

    def keep_row(t):
        column = lax.broadcasted_iota(jnp.int32, (1, tile), 1) + (g * step + t * tile)
        return (column < counts_ref[m] * HD).astype(jnp.float32)

    first_late = spans[chunks - 1][2]

    def late_at(t):
        return pl.ds(pl.multiple_of(t * tile - first_late, tile), tile)

    def query_sum(shard, row, rows, at):
        return jnp.dot(
            latents[:, w_rows(shard, row, rows)], w_all[w_rows(shard, row, rows), at],
            preferred_element_type=jnp.float32,
        )

    def query_start(t):
        at = at_rows(t, tile)
        product = query_sum(far_edge, 0, cut, at)
        for shard in (d, edge, far_mid):
            product += query_sum(shard, 0, depth, at)
        query_part[:, late_at(t)] = product

    def query_end(t):
        at = at_rows(t, tile)
        finish_query(t, query_part[:, late_at(t)] + query_sum(far_edge, cut, depth - cut, at))

    def query_tile(t):
        at = at_rows(t, tile)
        finish_query(
            t, jnp.dot(latents[...], w_all[:, at], preferred_element_type=jnp.float32)
        )

    def finish_query(t, product):
        at = at_rows(t, tile)
        query_out[:, at] = (product * keep_row(t)).astype(query_out.dtype)
        dots = product * cots[:, at].astype(jnp.float32)
        for part in range(tile // 128):
            dot_total[...] += dots[:, part * 128:(part + 1) * 128]

    def dot_copy(slot, to):
        return remote(
            dot_out.at[slot], dot_in.at[g * n + m], grad_send.at[1], grad_recv.at[1],
            groups=slot // 2,
            dp=mid if slot % 2 == 0 else edge, mp=to,
        )

    def each_dot(act):
        for slot in range(n):
            for to in range(n):
                if slot % 2 == 1:
                    act(dot_copy(slot, to))
                    continue
                pl.when(jnp.logical_not(is_self(to, slot)))(
                    lambda slot=slot, to=to: act(dot_copy(slot, to))
                )

    def send_dots():
        for slot in range(n):
            column = jnp.sum(dot_total[at_rows(slot, count), :], axis=1, keepdims=True)
            dot_out[slot] = jnp.broadcast_to(column, (count, 128)).T[:8]
        each_dot(lambda c: c.start())
        dot_in[g * n + m] = dot_out[2 * g]

    def finish_chunk(j):
        row, rows, first, size = spans[j]
        for_chunk(j, w_copy(0, 2, far_edge, j, far_mid).wait_recv)
        if j == 0:
            return
        if j == 1:
            first, size = 0, first + size

        @pl.loop(first // tile, (first + size) // tile)
        def _(t):
            add_grad(last_total, far_edge, row, rows, t)

        if j == chunks - 2:
            send_grad(last_total, far_edge, 0)
        if j == chunks - 1:
            send_grad(last_total, far_edge, 1)
        body = query_tile if rows == depth else query_end if row > 0 else query_start
        pl.loop(first // tile, (first + size) // tile)(body)
        if j == chunks - 1:
            send_dots()
        if j == 1:
            send_queries(0)
        send_queries(j)

    def gathered(sem, held):
        return remote(held, held, grad_send.at[sem], grad_recv.at[sem], groups=other)

    def all_sources(sem, buffer):
        pl.when(inner)(lambda: gathered(sem, buffer.at[pl.ds(0, 2 * n - 1)]).wait_recv())
        pl.when(outer)(lambda: gathered(sem, buffer).wait_recv())

    late = m == far_edge

    def own_block():
        all_sources(0, grad_in)
        grad_latent = grad_in[0].astype(jnp.float32)
        for source in range(1, 2 * n):
            grad_latent += grad_in[source].astype(jnp.float32)
        return gain_ref[...].reshape(1, width) * grad_latent / root_ref[:, :1]

    def to_others(sem, held):
        return [
            remote(held, held, peer_send.at[sem], peer_recv.at[sem], mp=lax.rem(m + o, n))
            for o in (2, 1, 3)
        ]

    def from_others(sem, buffer, blocks):
        held = buffer.at[pl.ds(0, blocks)]
        return remote(held, held, peer_send.at[sem], peer_recv.at[sem], groups=other)

    def early_block(ready):
        @pl.when(jnp.logical_and(jnp.logical_not(late), ready))
        def _():
            block_all[m] = own_block()
            for c in to_others(1, block_all.at[m]):
                c.start()

    def start_raw():
        raw_all[m] = raw_ref[...]
        for c in to_others(0, raw_all.at[m]):
            c.start()

    @pl.when(outer)
    def _():
        latent_inward(0).start()
        latent_inward(1).start()
        for j in range(early, chunks):
            for_chunk(j, lambda j=j: w_copy(0, 0, d, j, mid).start())
        crossed_feat(far_edge)
        start_raw()
        keep_feat()

    def pass_on(j):
        def act():
            w_copy(0, 0, edge, j, far_mid).wait_recv()
            w_copy(1, 2, edge, j, far_mid).start()

        for_chunk(j, act)

    @pl.when(inner)
    def _():
        latents[at_rows(2 * g, count), at_rows(m, width)] = latent_out[...]
        latent_inward(other).start()
        for o in range(1, n):
            latent_spread(slots[0], o).start()
        crossed_feat(far_edge)
        keep_feat()
        for j in range(early):
            pass_on(j)
        for slot in slots[1:]:
            latent_arrival(slot).wait_recv()
            for o in range(1, n):
                latent_spread(slot, o).start()

        for slot in slots[1:]:
            cot_arrival(slot).wait_recv()

        @pl.loop(0, half // tile)
        def _(t):
            at = at_rows(t, tile)
            cots[:, at] = cots[:, at] * keep_row(t).astype(cots.dtype)

        @pl.when(g == 1)
        def _():
            cots[:, :extra] = jnp.zeros((n * count, extra), cots.dtype)

        whole_grad(d)
        for_each_plane(lambda plane: w_moved(0, far_mid, plane).wait_recv())
        whole_grad(far_mid)
        latents_spread().wait_recv()
        start_raw()
        last_total[...] = jnp.zeros_like(last_total)
        dot_total[...] = jnp.zeros_like(dot_total)
        passed = early
        for j in range(chunks):
            for _ in range(min((0, 1)[j] if j < 2 else 2, chunks - passed)):
                pass_on(passed)
                passed += 1
            finish_chunk(j)
            if j == 3:
                whole_grad(edge)
            if j == 2:
                early_block(m != edge)
            if j == 5:
                early_block(m == edge)

    to_peer(0, 0, square_in, square_in, far_mid).wait_send()
    for o in range(1, n):
        feat_whole(lax.rem(m + o, n), m).wait_send()
        feat_whole(m, lax.rem(m + o, n)).wait_recv()
    for kind, shard in enumerate(neighbours):
        for_each_plane(lambda plane: crossed(kind, shard, plane).wait_send())
    down_sent(0)
    cot_copy(0, cot_half(g), 2 * g, g, mid).wait_send()

    def w_own_sent(plane):
        w_moved(0, d, plane).wait_send()

    for_each_plane(w_own_sent)
    latent_inward(other).wait_send()

    @pl.when(outer)
    def _():
        cot_copy(1, cot_half(g), 2 * g, g, mid).wait_send()
        cot_across().wait_send()
        latent_inward(g).wait_send()

    @pl.when(inner)
    def _():
        for way in range(1, 5):
            down_sent(way)
        latents_spread().wait_send()

    early_block(outer)
    all_sources(1, dot_in)
    dots = dot_in[0]
    for source in range(1, 2 * n):
        dots += dot_in[source]
    inner_dot = jnp.broadcast_to(dots[:1], (128, count)).T[:, :1]
    root = root_ref[:, :1]
    slope = inner_dot / (width * n * (root * root))

    @pl.when(late)
    def _():
        grad_all[far_edge] = (own_block() - raw_ref[...] * slope).astype(grad_all.dtype)
        for c in to_others(2, grad_all.at[far_edge]):
            c.start()

    row_tile = down_rows // 2 if down_rows % 256 == 0 else down_rows

    def add_block(who, first, last):
        @pl.loop(0, down_rows // row_tile)
        def _(c):
            rows = at_rows(c, row_tile)
            value = contract_last(grad_all[who], down_feat[rows, at_rows(who, width)])
            if not first:
                value += token_total[:, rows]
            if last:
                token_out[:, rows] = value.astype(token_out.dtype)
            else:
                token_total[:, rows] = value

    from_others(0, raw_all, n - 1).wait_recv()
    pl.when(late)(lambda: from_others(1, block_all, n - 1).wait_recv())
    pl.when(jnp.logical_not(late))(lambda: from_others(1, block_all, n - 2).wait_recv())
    for who in (1, 2, edge):
        grad_all[who] = (block_all[who] - raw_all[who] * slope).astype(grad_all.dtype)
        add_block(who, isinstance(who, int) and who == 1, False)

    def query_arrival(plane):
        first = plane * cols - plane * (half - extra)
        part = queries_ref.at[:, pl.ds(first, half - plane * extra)]
        return remote(part, part, query_sem.at[2], query_sem.at[plane], groups=other)

    for plane in range(2):
        away = jnp.logical_not(jnp.logical_and(inner, g == plane))
        pl.when(away)(lambda plane=plane: query_arrival(plane).wait_recv())

    @pl.when(inner)
    def _():
        for_each_plane(lambda plane: w_moved(1, edge, plane).wait_send())
        for plane in range(2):

            @pl.when(g == plane)
            def _():
                size = half - plane * extra
                part = query_out.at[pl.ds(0, (n - 1) * count), pl.ds(0, size)]
                remote(
                    part, part, query_sem.at[2], query_sem.at[plane], groups=other
                ).wait_send()
                query_keep(half - size, size).wait()

        blocks = down_all.at[pl.ds(0, (n * n - 1) * count), pl.ds(0, depth)]
        gathered(0, blocks).wait_send()
        gathered(1, raw_ref.at[pl.ds(0, (n * n - 1) * 8), pl.ds(0, 128)]).wait_send()

    from_others(0, raw_all, n - 1).wait_send()
    pl.when(jnp.logical_not(late))(lambda: from_others(1, block_all, n - 1).wait_send())
    pl.when(late)(lambda: from_others(2, grad_all, n - 1).wait_send())
    pl.when(jnp.logical_not(late))(lambda: from_others(2, grad_all, 1).wait_recv())
    add_block(far_edge, False, True)
    token_keep = pltpu.make_async_copy(token_out, grad_tokens_ref, local_sem.at[0])
    token_keep.start()
    token_keep.wait()


def project(tokens, w_down, gain, w_up, head_counts, cotangent):
    n = lax.axis_size("dp")
    count, cols = cotangent.shape
    depth = w_up.shape[0]
    down_rows, width = w_down.shape
    half = (cols // 128 + 1) // 2 * 128
    tile = 256 if half % 256 == 0 else 128
    tiles = half // tile
    ends = min(2, tiles - 1)
    body = tiles - ends
    sizes = []
    while sum(sizes) < body:
        left = body - sum(sizes)
        sizes.append(min(2, left))
    parts = len(sizes)
    cut = depth - 128
    spans = [(0, depth, sum(sizes[:i]) * tile, sizes[i] * tile) for i in range(parts)]
    extra = 2 * half - cols
    spans[0] = (0, depth, extra, sizes[0] * tile - extra)
    spans.insert(0, (0, depth, 0, extra))
    for row, rows in ((0, cut), (cut, 128)):
        spans.append((row, rows, body * tile, ends * tile))
    spans = tuple(spans)
    parts = len(spans)
    pieces = 2
    hbm = pl.BlockSpec(memory_space=pl.ANY)
    bf16, f32 = jnp.bfloat16, jnp.float32
    dma = pltpu.SemaphoreType.DMA
    return pl.pallas_call(
        functools.partial(project_kernel, n, spans, tile, pieces),
        out_shape=(
            jax.ShapeDtypeStruct((count, cols), bf16),
            jax.ShapeDtypeStruct((count, down_rows), bf16),
        ),
        in_specs=[hbm] * 6,
        out_specs=(hbm, hbm),
        scratch_shapes=[
            pltpu.VMEM(gain.shape, f32),
            pltpu.SMEM(head_counts.shape, jnp.int32),
            pltpu.VMEM(tokens.shape, bf16),
            pltpu.VMEM((count, cols), bf16),
            pltpu.VMEM((count, half), bf16),
            pltpu.VMEM((n * down_rows, width), bf16),
            pltpu.VMEM((down_rows, n * width), bf16),
            pltpu.VMEM((n * depth, half), bf16),
            pltpu.VMEM((n * count, half), bf16),
            pltpu.VMEM((n * count, half), bf16),
            pltpu.VMEM((n * count, n * width), bf16),
            pltpu.VMEM((count, width), bf16),
            pltpu.VMEM((n * count, n * depth), bf16),
            pltpu.VMEM((2 * n, count, depth), bf16),
            pltpu.VMEM((n * count, depth), f32),
            pltpu.VMEM((n * count, depth), f32),
            pltpu.VMEM((count, width), f32),
            pltpu.VMEM((count, 128), f32),
            pltpu.VMEM((8, count), f32),
            pltpu.VMEM((n - 1, 8, count), f32),
            pltpu.VMEM((n * count, 128), f32),
            pltpu.VMEM((n, 8, count), f32),
            pltpu.VMEM((2 * n, 8, count), f32),
            pltpu.VMEM((n, count, width), f32),
            pltpu.VMEM((n, count, width), f32),
            pltpu.VMEM((n, count, width), bf16),
            pltpu.VMEM((n * count, spans[-1][3]), f32),
            pltpu.VMEM((count, down_rows), f32),
            pltpu.VMEM((count, down_rows), bf16),
            dma((6,)),
            dma((5,)),
            dma((3, pieces + 1)),
            dma((3,)),
            dma((3,)),
            dma((n,)),
            dma((n,)),
            dma((3,)),
            dma((n + 1,)),
            dma((3,)),
            dma((n + 1,)),
            dma((2,)),
            dma((2 * parts + 1,)),
            dma((4,)),
            dma((2,)),
            dma((2,)),
            dma((1,)),
            dma((1,)),
            dma((3,)),
            dma((3,)),
        ],
        compiler_params=pltpu.CompilerParams(
            collective_id=0, has_side_effects=True, vmem_limit_bytes=60 * 2**20
        ),
    )(tokens, w_down, gain, w_up, head_counts, cotangent)


def store_kernel(parts, queries_in, grad_in, queries_out, grad_out, held, grad, sem):
    rows = held.shape[0] // parts

    def span(k):
        return pl.ds(k * rows, rows)

    reads = [
        pltpu.make_async_copy(queries_in.at[span(k)], held.at[span(k)], sem.at[0, k])
        for k in range(parts)
    ] + [pltpu.make_async_copy(grad_in, grad, sem.at[0, parts])]
    writes = [
        pltpu.make_async_copy(held.at[span(k)], queries_out.at[span(k)], sem.at[1, k])
        for k in range(parts)
    ] + [pltpu.make_async_copy(grad, grad_out, sem.at[1, parts])]
    for read in reads:
        read.start()
    for read, write in zip(reads, writes):
        read.wait()
        write.start()
    for write in writes:
        write.wait()


def store(queries, grad_tokens):
    parts = 4
    hbm = pl.BlockSpec(memory_space=pl.ANY)
    return pl.pallas_call(
        functools.partial(store_kernel, parts),
        out_shape=(
            jax.ShapeDtypeStruct(queries.shape, queries.dtype),
            jax.ShapeDtypeStruct(grad_tokens.shape, grad_tokens.dtype),
        ),
        in_specs=[hbm] * 2,
        out_specs=(hbm,) * 2,
        scratch_shapes=[
            pltpu.VMEM(queries.shape, queries.dtype),
            pltpu.VMEM(grad_tokens.shape, grad_tokens.dtype),
            pltpu.SemaphoreType.DMA((2, parts + 1)),
        ],
    )(queries, grad_tokens)


def move_weights_body(tokens, w_down, gain, w_up, head_counts, cotangent):
    return store(*project(tokens, w_down, gain, w_up, head_counts, cotangent))


def solution(mesh):
    in_specs = (
        P(("groups", "dp"), None),
        P("dp", "mp"),
        P("mp"),
        P("dp", "mp"),
        P(),
        P(("groups", "dp"), "mp"),
    )
    out_specs = (P(("groups", "dp"), "mp"), P(("groups", "dp"), "mp"))
    square = mesh.shape["dp"] == mesh.shape["mp"] == 4 and mesh.shape["groups"] == 2
    body = move_weights_body if square else gather_weights_body
    return jax.shard_map(body, mesh=mesh, in_specs=in_specs, out_specs=out_specs, check_vma=False)
```

```python
import functools

import jax
import jax.numpy as jnp
from jax import lax
from jax.experimental import pallas as pl
from jax.experimental.pallas import tpu as pltpu
from jax.sharding import PartitionSpec as P

HD = 192
MESH = pl.DeviceIdType.MESH


def contract_last(left, right):
    return lax.dot_general(
        left, right, (((1,), (1,)), ((), ())), preferred_element_type=jnp.float32
    )


def keep_mask_of(head_counts, block_cols):
    position = lax.axis_index("mp")
    held_heads = lax.dynamic_slice_in_dim(head_counts, position, 1, 0)
    slot_index = jnp.arange(block_cols, dtype=jnp.int32) // HD
    return (slot_index < held_heads).astype(jnp.float32)


def gather_weights_body(tokens, w_down, gain, w_up, head_counts, cotangent):
    latent_width = w_down.shape[1] * lax.axis_size("mp")
    keep_mask = keep_mask_of(head_counts, w_up.shape[1])
    down_whole = lax.all_gather(w_down, "dp", axis=0, tiled=True)
    latent_raw = jnp.dot(tokens, down_whole, preferred_element_type=jnp.float32)
    squares = lax.psum(jnp.sum(latent_raw * latent_raw, axis=1, keepdims=True), "mp")
    root_mean = jnp.sqrt(squares / latent_width + 1e-06)
    latent_local = (latent_raw / root_mean * gain).astype(jnp.bfloat16)
    latent = lax.all_gather(latent_local, "mp", axis=1, tiled=True)
    masked = cotangent * keep_mask.astype(jnp.bfloat16)
    up_whole = lax.all_gather(w_up, "dp", axis=0, tiled=True)
    query_total = jnp.dot(latent, up_whole, preferred_element_type=jnp.float32)
    grad_partial = contract_last(masked, up_whole)
    queries = (query_total * keep_mask).astype(jnp.bfloat16)
    grad_latent = lax.psum_scatter(
        grad_partial.astype(jnp.bfloat16), "mp", scatter_dimension=1, tiled=True
    ).astype(jnp.float32)
    inner_dot = lax.psum(jnp.sum(gain * grad_latent * latent_raw, axis=1, keepdims=True), "mp")
    grad_raw = (
        gain * grad_latent / root_mean - latent_raw * inner_dot / (latent_width * root_mean**3)
    ).astype(jnp.bfloat16)
    partial_value = contract_last(grad_raw, down_whole).astype(jnp.bfloat16)
    grad_tokens = lax.psum_scatter(partial_value, "mp", scatter_dimension=1, tiled=True)
    return (queries, grad_tokens)


def project_kernel(
    n, spans, tile, pieces, tokens_hbm, down_hbm, gain_hbm, w_hbm, counts_hbm, cot_hbm,
    queries_ref, grad_tokens_ref, gain_ref, counts_ref, tokens_ref, cot_ref, cot_pass, down_all, down_feat, w_all,
    cots, query_out, latents, latent_out, grad_out, grad_in, late_in, gain_far, slope_ref, total, last_total, raw_ref,
    root_ref, square_out, square_in, dot_total, dot_out, dot_in, raw_all, block_all, grad_all, query_part,
    token_total, token_out, local_sem, down_send, down_recv, across_send, across_recv,
    feat_send, feat_recv, cot_send, cot_recv, latent_send, latent_recv, w_send, w_recv,
    query_sem, grad_send, grad_recv, small_send, small_recv, peer_send, peer_recv,
):
    g, d, m = lax.axis_index("groups"), lax.axis_index("dp"), lax.axis_index("mp")
    other = 1 - g
    upper = (d >= 2).astype(jnp.int32)
    mid, edge = 1 + upper, 3 * upper
    far_mid, far_edge = 2 - upper, 3 - 3 * upper
    inner = d == mid
    outer = jnp.logical_not(inner)
    role = 1 - inner.astype(jnp.int32)
    count, cols = cot_ref.shape
    depth = w_hbm.shape[0]
    down_rows, width = down_hbm.shape
    half = cots.shape[1]
    step = cols - half
    extra = half - step
    spare_rows = extra * depth // width
    plane_rows = (down_rows - spare_rows) // 2
    piece_rows = plane_rows // pieces
    chunks = len(spans)

    def at_rows(k, size):
        return pl.ds(pl.multiple_of(k * size, size), size)

    down_load = pltpu.make_async_copy(
        down_hbm, down_all.at[at_rows(d, down_rows)], local_sem.at[0]
    )
    cot_load = pltpu.make_async_copy(cot_hbm, cot_ref, local_sem.at[1])
    w_load = pltpu.make_async_copy(
        w_hbm.at[:, pl.ds(pl.multiple_of(g * step, 128), half)],
        w_all.at[at_rows(d, depth)], local_sem.at[2],
    )
    tokens_load = pltpu.make_async_copy(tokens_hbm, tokens_ref, local_sem.at[3])
    down_load.start()
    cot_load.start()
    w_load.start()
    tokens_load.start()
    gain_load = pltpu.make_async_copy(gain_hbm, gain_ref, local_sem.at[4])
    counts_load = pltpu.make_async_copy(counts_hbm, counts_ref, local_sem.at[5])
    gain_load.start()
    counts_load.start()

    barrier = pltpu.get_barrier_semaphore()

    def greet(**where):
        pl.semaphore_signal(barrier, inc=1, device_id=where, device_id_type=MESH)

    for plane in range(2):
        for place in (0, 1):
            for who in range(n):
                there = mid if place == 0 else edge
                itself = jnp.logical_and(
                    g == plane, jnp.logical_and(role == place, m == who)
                )
                pl.when(jnp.logical_not(itself))(
                    lambda plane=plane, there=there, who=who: greet(
                        groups=plane, dp=there, mp=who
                    )
                )
    pl.when(inner)(lambda: greet(dp=far_mid))
    down_load.wait()
    pl.when(inner)(lambda: pl.semaphore_wait(barrier, 4 * n))
    pl.when(outer)(lambda: pl.semaphore_wait(barrier, 4 * n - 1))

    def remote(source, target, send, recv, **where):
        return pltpu.make_async_remote_copy(
            src_ref=source, dst_ref=target, send_sem=send, recv_sem=recv,
            device_id=where, device_id_type=MESH,
        )

    def down_span(plane, k):
        if k == pieces:
            return plane_rows, spare_rows
        return plane * (plane_rows + spare_rows) + k * piece_rows, piece_rows

    def down_piece(shard, plane, k):
        start, rows = down_span(plane, k)
        return down_all.at[pl.ds(pl.multiple_of(shard * down_rows + start, 16), rows)]

    def down_copy(way, kind, shard, k, to):
        held = down_piece(shard, g, k)
        return remote(held, held, down_send.at[way], down_recv.at[kind, k], dp=to)

    def down_across(kind, shard, k):
        held = down_piece(shard, g, k)
        return remote(held, held, across_send.at[kind], across_recv.at[kind], groups=other)

    def for_each_plane(body):
        for plane in range(2):
            pl.when(g == plane)(lambda plane=plane: body(plane))

    def moved_rows(shard, plane):
        rows = plane_rows + plane * spare_rows
        start = shard * down_rows + plane * plane_rows
        return down_all.at[pl.ds(pl.multiple_of(start, 16), rows)]

    def down_sent(way):
        def wait(plane):
            held = moved_rows(d, plane)
            remote(
                held, held, down_send.at[way], down_recv.at[0, 0], dp=far_mid
            ).wait_send()

        for_each_plane(wait)

    def crossed(kind, shard, plane):
        held = moved_rows(shard, plane)
        return remote(held, held, across_send.at[kind], across_recv.at[kind], groups=other)

    def each_piece(act):
        for k in range(pieces):
            act(k)
        pl.when(g == 1)(lambda: act(pieces))

    def cot_half(plane):
        return cot_ref.at[:, pl.ds(pl.multiple_of(plane * step, 128), half)]

    def cot_copy(way, source, slot, plane, to):
        return remote(
            source, cots.at[at_rows(slot, count)], cot_send.at[way], cot_recv.at[slot],
            groups=plane, dp=to,
        )

    def cot_across():
        return remote(
            cot_half(other), cot_pass, cot_send.at[2], cot_recv.at[n], groups=other
        )

    def cot_arrival(slot):
        held = cots.at[at_rows(slot, count)]
        return remote(held, held, cot_send.at[0], cot_recv.at[slot], dp=far_mid)

    def w_rows(shard, row, rows):
        return pl.ds(pl.multiple_of(shard * depth + row, 128), rows)

    def w_piece(shard, j):
        row, rows, first, size = spans[j]
        return w_all.at[w_rows(shard, row, rows), pl.ds(first, size)]

    def w_copy(way, kind, shard, j, to):
        held = w_piece(shard, j)
        sem = w_recv.at[2 * chunks] if kind == 1 else w_recv.at[kind // 2 * chunks + j]
        return remote(held, held, w_send.at[way], sem, dp=to)

    def w_moved(way, shard, plane):
        first = plane * extra
        held = w_all.at[at_rows(shard, depth), pl.ds(first, half - first)]
        return remote(held, held, w_send.at[way], w_recv.at[2 * chunks], dp=far_mid)

    def for_chunk(j, act):
        if j == 0:
            pl.when(g == 0)(act)
        else:
            act()

    def keep_cot():
        cots[at_rows(2 * g, count), :] = cot_ref[
            :, pl.ds(pl.multiple_of(g * step, 128), half)
        ]

    def feat_copy(shard, plane, k):
        start, rows = down_span(plane, k)
        return remote(
            down_piece(shard, plane, k),
            down_feat.at[pl.ds(pl.multiple_of(start, 16), rows), at_rows(m, width)],
            feat_send.at[shard], feat_recv.at[m], mp=shard,
        )

    def feat_piece(shard, plane, k):
        pl.when(shard != m)(lambda: feat_copy(shard, plane, k).start())

    def crossed_feat(shard):
        for k in range(pieces):
            feat_piece(shard, other, k)
        pl.when(g == 0)(lambda: feat_piece(shard, other, pieces))

    def feat_whole(sent, arrived):
        held = down_feat.at[:, at_rows(arrived, width)]
        return remote(held, held, feat_send.at[sent], feat_recv.at[arrived], groups=other)

    def keep_feat():
        @pl.loop(0, down_rows // 128)
        def _(k):
            source = m * down_rows + k * 128
            down_feat[at_rows(k, 128), at_rows(m, width)] = down_all[
                pl.ds(pl.multiple_of(source, 128), 128), :
            ]

    early = 4

    @pl.when(inner)
    def _():
        def start_own(k):
            down_copy(0, 1, d, k, far_mid).start()
            down_copy(1, 0, d, k, edge).start()

        each_piece(start_own)
        for k in range(pieces + 1):
            feat_piece(d, 0, k)
        for k in range(pieces):
            feat_piece(d, 1, k)
        cot_load.wait()
        keep_cot()

        @pl.when(g == 1)
        def _():
            for shard in (edge, far_mid, far_edge):
                w_all[at_rows(shard, depth), :extra] = jnp.zeros((depth, extra), w_all.dtype)

        def pass_near(k):
            for kind, sent, shard, way, to in (
                (0, 2, edge, 2, far_mid), (1, 1, far_mid, 3, edge)
            ):
                down_copy(way, kind, shard, k, to).wait_recv()
                down_copy(way, sent, shard, k, to).start()
                down_across(kind, shard, k).start()
                feat_piece(shard, g, k)

        each_piece(pass_near)
        w_load.wait()
        for j in range(chunks):
            for_chunk(j, lambda j=j: w_copy(0, 1, d, j, far_mid).start())

        def pass_far(k):
            down_copy(4, 2, far_edge, k, edge).wait_recv()
            down_copy(4, 2, far_edge, k, edge).start()
            down_across(2, far_edge, k).start()
            feat_piece(far_edge, g, k)

        each_piece(pass_far)
        cot_copy(0, cot_half(other), 2 * g, other, d).start()

    @pl.when(outer)
    def _():
        each_piece(lambda k: down_copy(0, 0, d, k, mid).start())
        cot_load.wait()
        cot_across().start()
        cot_copy(0, cot_half(g), 2 * g + 1, g, mid).start()
        for k in range(pieces + 1):
            feat_piece(d, 0, k)
        for k in range(pieces):
            feat_piece(d, 1, k)
        w_load.wait()
        for kind, shard in enumerate((mid, far_mid, far_edge)):

            def take(k):
                down_copy(0, kind, shard, k, mid).wait_recv()
                down_across(kind, shard, k).start()
                feat_piece(shard, g, k)

            each_piece(take)
            if kind == 0:
                cot_across().wait_recv()
                cot_copy(1, cot_pass, 2 * other + 1, g, mid).start()
                for j in range(early):
                    for_chunk(j, lambda j=j: w_copy(0, 0, d, j, mid).start())

    neighbours = (jnp.where(inner, edge, mid), far_mid, far_edge)
    for kind, shard in enumerate(neighbours):
        for_each_plane(lambda plane: crossed(kind, shard, 1 - plane).wait_recv())
        if kind < 2:
            crossed_feat(shard)

    tokens_load.wait()
    gain_load.wait()
    counts_load.wait()
    raw_ref[...] = jnp.zeros_like(raw_ref)

    @pl.loop(0, 2 * n)
    def _(c):
        at = at_rows(c, down_rows // 2)
        raw_ref[...] += jnp.dot(
            tokens_ref[:, at], down_all[at, :], preferred_element_type=jnp.float32
        )

    def to_peer(sent, arrived, source, target, mp):
        return remote(source, target, small_send.at[sent], small_recv.at[arrived], mp=mp)

    raw = raw_ref[...]
    square_out[...] = jnp.broadcast_to(
        jnp.sum(raw * raw, axis=1, keepdims=True), (count, 128)
    ).T[:8]
    for o in range(1, n):
        to_peer(0, 0, square_out, square_in.at[o - 1], lax.rem(m + o, n)).start()
    to_peer(0, 0, square_in, square_in, far_mid).wait_recv()
    value = square_out[...]
    for o in range(1, n):
        value += square_in[o - 1]
    squares = jnp.broadcast_to(value[:1], (128, count)).T[:, :1]
    root = jnp.sqrt(squares / (width * n) + 1e-06)
    root_ref[...] = jnp.broadcast_to(root, root_ref.shape)
    gain = gain_ref[...].reshape(1, width)
    latent_out[...] = (raw / root * gain).astype(latent_out.dtype)

    def latent_at(slot, who):
        return latents.at[at_rows(slot, count), at_rows(who, width)]

    def latent_inward(to):
        return remote(
            latent_out, latent_at(2 * g + role, m), latent_send.at[to],
            latent_recv.at[2 * g + role], groups=to, dp=mid,
        )

    def latent_arrival(slot):
        held = latent_at(slot, m)
        return remote(held, held, latent_send.at[0], latent_recv.at[slot], dp=far_mid)

    def latent_spread(slot, o):
        held = latent_at(slot, m)
        return remote(
            held, held, latent_send.at[2], latent_recv.at[n], mp=lax.rem(m + o, n)
        )

    def latents_spread():
        held = latents.at[:, pl.ds(0, (n - 1) * width)]
        return remote(held, held, latent_send.at[2], latent_recv.at[n], dp=far_mid)

    slots = (2 * g, 2 * other, 2 * g + 1, 2 * other + 1)

    cut = depth - 128
    grad_parts = ((0, cut), (cut, 128))

    def add_grad(sum_ref, shard, row, rows, t):
        at = at_rows(t, tile)
        sum_ref[:, row:row + rows] += contract_last(
            cots[:, at], w_all[w_rows(shard, row, rows), at]
        )

    def grad_copy(shard, slot, part):
        row, rows = grad_parts[part]
        return remote(
            grad_out.at[at_rows(slot, count), w_rows(shard, row, rows)],
            grad_in.at[g * n + m, :, pl.ds(row, rows)],
            grad_send.at[0], grad_recv.at[0],
            groups=slot // 2, dp=mid if slot % 2 == 0 else edge, mp=shard,
        )

    def is_self(shard, slot):
        return jnp.logical_and(g == slot // 2, m == shard)

    def each_grad(shard, part, act):
        for slot in range(n):
            if slot % 2 == 1:
                act(grad_copy(shard, slot, part))
                continue
            pl.when(jnp.logical_not(is_self(shard, slot)))(
                lambda slot=slot: act(grad_copy(shard, slot, part))
            )

    half_count = count // 2
    late_owners = (far_edge, lax.rem(far_edge + 2, n))

    def late_copy(slot, side, part):
        row, rows = grad_parts[part]
        source = pl.ds(pl.multiple_of(slot * count + side * half_count, 16), half_count)
        return remote(
            grad_out.at[source, w_rows(far_edge, row, rows)],
            late_in.at[g * n + m, :, pl.ds(row, rows)],
            grad_send.at[2], grad_recv.at[2], groups=slot // 2,
            dp=mid if slot % 2 == 0 else edge, mp=late_owners[side],
        )

    def send_late(sum_ref, part):
        row, rows = grad_parts[part]
        grad_out[:, w_rows(far_edge, row, rows)] = sum_ref[:, row:row + rows].astype(
            grad_out.dtype
        )
        for slot in range(n):
            for side in range(2):
                if slot % 2 == 1:
                    late_copy(slot, side, part).start()
                    continue
                itself = is_self(late_owners[side], slot)
                pl.when(jnp.logical_not(itself))(
                    lambda slot=slot, side=side: late_copy(slot, side, part).start()
                )
        for side in range(2):

            @pl.when(m == late_owners[side])
            def _():
                source = pl.ds(
                    pl.multiple_of(2 * g * count + side * half_count, 16), half_count
                )
                late_in[g * n + m, :, row:row + rows] = grad_out[
                    source, w_rows(far_edge, row, rows)
                ]

    def send_grad(sum_ref, shard, part):
        row, rows = grad_parts[part]
        grad_out[:, w_rows(shard, row, rows)] = sum_ref[:, row:row + rows].astype(
            grad_out.dtype
        )
        each_grad(shard, part, lambda c: c.start())

        @pl.when(m == shard)
        def _():
            grad_in[g * n + m, :, row:row + rows] = grad_out[
                at_rows(2 * g, count), w_rows(shard, row, rows)
            ]

    def whole_grad(shard):
        total[...] = jnp.zeros_like(total)

        @pl.loop(0, half // tile)
        def _(t):
            add_grad(total, shard, 0, depth, t)

        for part in range(2):
            send_grad(total, shard, part)

    def query_parts(j):
        row, rows, first, size = spans[j]
        if row + rows < depth:
            return ()
        return ((first, size, j == 0),)

    def query_copy(slot, first, size):
        return remote(
            query_out.at[at_rows(slot, count), pl.ds(first, size)],
            queries_ref.at[:, pl.ds(pl.multiple_of(g * step + first, 128), size)],
            query_sem.at[2], query_sem.at[g],
            groups=slot // 2, dp=mid if slot % 2 == 0 else edge,
        )

    def query_keep(first, size):
        return pltpu.make_async_copy(
            query_out.at[at_rows(2 * g, count), pl.ds(first, size)],
            queries_ref.at[:, pl.ds(pl.multiple_of(g * step + first, 128), size)],
            query_sem.at[3],
        )

    def send_queries(j):
        for first, size, once in query_parts(j):

            def act():
                for slot in range(n):
                    if slot % 2 == 1:
                        query_copy(slot, first, size).start()
                        continue
                    mine = g == slot // 2
                    pl.when(jnp.logical_not(mine))(
                        lambda slot=slot: query_copy(slot, first, size).start()
                    )
                query_keep(first, size).start()

            if once:
                pl.when(g == 0)(act)
            else:
                act()

    def keep_row(t):
        column = lax.broadcasted_iota(jnp.int32, (1, tile), 1) + (g * step + t * tile)
        return (column < counts_ref[m] * HD).astype(jnp.float32)

    ends = sum(row > 0 for row, rows, first, size in spans)
    first_late = min(first for row, rows, first, size in spans if row > 0)

    def late_at(t):
        return pl.ds(pl.multiple_of(t * tile - first_late, tile), tile)

    def query_sum(shard, row, rows, at):
        return jnp.dot(
            latents[:, w_rows(shard, row, rows)], w_all[w_rows(shard, row, rows), at],
            preferred_element_type=jnp.float32,
        )

    def query_start(t):
        at = at_rows(t, tile)
        product = query_sum(far_edge, 0, cut, at)
        for shard in (d, edge, far_mid):
            product += query_sum(shard, 0, depth, at)
        query_part[:, late_at(t)] = product

    def query_end(t):
        at = at_rows(t, tile)
        finish_query(t, query_part[:, late_at(t)] + query_sum(far_edge, cut, depth - cut, at))

    def query_tile(t):
        at = at_rows(t, tile)
        finish_query(
            t, jnp.dot(latents[...], w_all[:, at], preferred_element_type=jnp.float32)
        )

    def finish_query(t, product):
        at = at_rows(t, tile)
        query_out[:, at] = (product * keep_row(t)).astype(query_out.dtype)
        dots = product * cots[:, at].astype(jnp.float32)
        for part in range(tile // 128):
            dot_total[...] += dots[:, part * 128:(part + 1) * 128]

    def dot_copy(slot, to):
        return remote(
            dot_out.at[slot], dot_in.at[g * n + m], grad_send.at[1], grad_recv.at[1],
            groups=slot // 2,
            dp=mid if slot % 2 == 0 else edge, mp=to,
        )

    def each_dot(act):
        for slot in range(n):
            for to in range(n):
                if slot % 2 == 1:
                    act(dot_copy(slot, to))
                    continue
                pl.when(jnp.logical_not(is_self(to, slot)))(
                    lambda slot=slot, to=to: act(dot_copy(slot, to))
                )

    def send_dots():
        for slot in range(n):
            column = jnp.sum(dot_total[at_rows(slot, count), :], axis=1, keepdims=True)
            dot_out[slot] = jnp.broadcast_to(column, (count, 128)).T[:8]
        each_dot(lambda c: c.start())
        dot_in[g * n + m] = dot_out[2 * g]

    def finish_chunk(j):
        row, rows, first, size = spans[j]
        for_chunk(j, w_copy(0, 2, far_edge, j, far_mid).wait_recv)
        if j == 0:
            return
        if j == 1:
            first, size = 0, first + size

        @pl.loop(first // tile, (first + size) // tile)
        def _(t):
            add_grad(last_total, far_edge, row, rows, t)

        if row == 0 and rows == cut:
            send_late(last_total, 0)
        if j == chunks - 1:
            send_late(last_total, 1)
        body = query_tile if rows == depth else query_end if row > 0 else query_start
        pl.loop(first // tile, (first + size) // tile)(body)
        if j == chunks - 1:
            send_dots()
        if row > 0 and j < chunks - 1:
            return
        for i in range(j if row == 0 else chunks - ends, j + 1):
            if i == 1:
                send_queries(0)
            send_queries(i)

    def gathered(sem, held):
        return remote(held, held, grad_send.at[sem], grad_recv.at[sem], groups=other)

    def all_sources(sem, buffer):
        pl.when(inner)(lambda: gathered(sem, buffer.at[pl.ds(0, 2 * n - 1)]).wait_recv())
        pl.when(outer)(lambda: gathered(sem, buffer).wait_recv())

    late = m == far_edge

    def own_block():
        all_sources(0, grad_in)
        grad_latent = grad_in[0].astype(jnp.float32)
        for source in range(1, 2 * n):
            grad_latent += grad_in[source].astype(jnp.float32)
        return gain_ref[...].reshape(1, width) * grad_latent / root_ref[:, :1]

    def to_others(sem, held):
        return [
            remote(held, held, peer_send.at[sem], peer_recv.at[sem], mp=lax.rem(m + o, n))
            for o in (2, 1, 3)
        ]

    def from_others(sem, buffer, blocks):
        held = buffer.at[pl.ds(0, blocks)]
        return remote(held, held, peer_send.at[sem], peer_recv.at[sem], groups=other)

    def early_block(ready):
        @pl.when(jnp.logical_and(jnp.logical_not(late), ready))
        def _():
            block_all[m] = own_block()
            for c in to_others(1, block_all.at[m]):
                c.start()

    gain_copy = remote(
        gain_ref, gain_far, peer_send.at[3], peer_recv.at[3], mp=lax.rem(m + 2, n)
    )

    def start_raw():
        gain_copy.start()
        raw_all[m] = raw_ref[...]
        for c in to_others(0, raw_all.at[m]):
            c.start()

    @pl.when(outer)
    def _():
        latent_inward(0).start()
        latent_inward(1).start()
        for j in range(early, chunks):
            for_chunk(j, lambda j=j: w_copy(0, 0, d, j, mid).start())
        crossed_feat(far_edge)
        start_raw()
        keep_feat()

    def pass_on(j):
        def act():
            w_copy(0, 0, edge, j, far_mid).wait_recv()
            w_copy(1, 2, edge, j, far_mid).start()

        for_chunk(j, act)

    @pl.when(inner)
    def _():
        latents[at_rows(2 * g, count), at_rows(m, width)] = latent_out[...]
        latent_inward(other).start()
        for o in range(1, n):
            latent_spread(slots[0], o).start()
        crossed_feat(far_edge)
        keep_feat()
        for j in range(early):
            pass_on(j)
        for slot in slots[1:]:
            latent_arrival(slot).wait_recv()
            for o in range(1, n):
                latent_spread(slot, o).start()

        for slot in slots[1:]:
            cot_arrival(slot).wait_recv()

        @pl.loop(0, half // tile)
        def _(t):
            at = at_rows(t, tile)
            cots[:, at] = cots[:, at] * keep_row(t).astype(cots.dtype)

        @pl.when(g == 1)
        def _():
            cots[:, :extra] = jnp.zeros((n * count, extra), cots.dtype)

        whole_grad(d)
        for_each_plane(lambda plane: w_moved(0, far_mid, plane).wait_recv())
        whole_grad(far_mid)
        latents_spread().wait_recv()
        start_raw()
        last_total[...] = jnp.zeros_like(last_total)
        dot_total[...] = jnp.zeros_like(dot_total)
        passed = early
        for j in range(chunks):
            for _ in range(min((0, 1, 2)[j] if j < 3 else chunks, chunks - passed)):
                pass_on(passed)
                passed += 1
            finish_chunk(j)
            if j == 3:
                whole_grad(edge)
            if j == 2:
                early_block(m != edge)
            if j == 5:
                early_block(m == edge)

    to_peer(0, 0, square_in, square_in, far_mid).wait_send()
    for o in range(1, n):
        feat_whole(lax.rem(m + o, n), m).wait_send()
        feat_whole(m, lax.rem(m + o, n)).wait_recv()
    for kind, shard in enumerate(neighbours):
        for_each_plane(lambda plane: crossed(kind, shard, plane).wait_send())
    down_sent(0)
    cot_copy(0, cot_half(g), 2 * g, g, mid).wait_send()

    def w_own_sent(plane):
        w_moved(0, d, plane).wait_send()

    for_each_plane(w_own_sent)
    latent_inward(other).wait_send()

    @pl.when(outer)
    def _():
        cot_copy(1, cot_half(g), 2 * g, g, mid).wait_send()
        cot_across().wait_send()
        latent_inward(g).wait_send()

    @pl.when(inner)
    def _():
        for way in range(1, 5):
            down_sent(way)
        latents_spread().wait_send()

    early_block(outer)
    all_sources(1, dot_in)
    dots = dot_in[0]
    for source in range(1, 2 * n):
        dots += dot_in[source]
    inner_dot = jnp.broadcast_to(dots[:1], (128, count)).T[:, :1]
    root = root_ref[:, :1]
    slope = inner_dot / (width * n * (root * root))

    slope_ref[...] = jnp.broadcast_to(slope, slope_ref.shape)
    owner = jnp.logical_or(m == late_owners[0], m == late_owners[1])
    visitor = jnp.logical_not(owner)
    mine = pl.ds(
        pl.multiple_of((1 - late.astype(jnp.int32)) * half_count, half_count), half_count
    )
    gain_copy.wait_recv()
    from_others(0, raw_all, n - 1).wait_recv()

    @pl.when(owner)
    def _():
        all_sources(2, late_in)
        summed = late_in[0].astype(jnp.float32)
        for source in range(1, 2 * n):
            summed += late_in[source].astype(jnp.float32)
        gain = jnp.where(late, gain_ref[...].reshape(1, width), gain_far[...].reshape(1, width))
        value = gain * summed / root_ref[mine, :1]
        value -= raw_all[far_edge, mine, :] * slope_ref[mine, :1]
        grad_all[far_edge, mine, :] = value.astype(grad_all.dtype)
        for c in to_others(2, grad_all.at[far_edge, mine, :]):
            c.start()

    row_tile = down_rows

    def add_block(who, first, last):
        @pl.loop(0, down_rows // row_tile)
        def _(c):
            rows = at_rows(c, row_tile)
            value = contract_last(grad_all[who], down_feat[rows, at_rows(who, width)])
            if not first:
                value += token_total[:, rows]
            if last:
                token_out[:, rows] = value.astype(token_out.dtype)
            else:
                token_total[:, rows] = value

    pl.when(late)(lambda: from_others(1, block_all, n - 1).wait_recv())
    pl.when(jnp.logical_not(late))(lambda: from_others(1, block_all, n - 2).wait_recv())
    for who in (1, 2, edge):
        grad_all[who] = (block_all[who] - raw_all[who] * slope).astype(grad_all.dtype)
        add_block(who, isinstance(who, int) and who == 1, False)

    pl.when(visitor)(lambda: from_others(2, grad_all, 1).wait_recv())
    theirs = pl.ds(pl.multiple_of(late.astype(jnp.int32) * half_count, half_count), half_count)

    def other_half():
        held = grad_all.at[far_edge, theirs, :]
        return remote(held, held, peer_send.at[2], peer_recv.at[2], groups=other)

    pl.when(owner)(lambda: other_half().wait_recv())
    add_block(far_edge, False, True)
    token_keep = pltpu.make_async_copy(token_out, grad_tokens_ref, local_sem.at[0])
    token_keep.start()

    def query_arrival(plane):
        first = plane * cols - plane * (half - extra)
        part = queries_ref.at[:, pl.ds(first, half - plane * extra)]
        return remote(part, part, query_sem.at[2], query_sem.at[plane], groups=other)

    for plane in range(2):
        away = jnp.logical_not(jnp.logical_and(inner, g == plane))
        pl.when(away)(lambda plane=plane: query_arrival(plane).wait_recv())

    @pl.when(inner)
    def _():
        for_each_plane(lambda plane: w_moved(1, edge, plane).wait_send())
        for plane in range(2):

            @pl.when(g == plane)
            def _():
                size = half - plane * extra
                part = query_out.at[pl.ds(0, (n - 1) * count), pl.ds(0, size)]
                remote(
                    part, part, query_sem.at[2], query_sem.at[plane], groups=other
                ).wait_send()
                query_keep(half - size, size).wait()

        def early_sent(blocks):
            held = down_all.at[pl.ds(0, blocks * count), pl.ds(0, depth)]
            gathered(0, held).wait_send()

        pl.when(late)(lambda: early_sent(3 * n))
        pl.when(jnp.logical_not(late))(lambda: early_sent(3 * n - 1))
        pl.when(owner)(lambda: gathered(2, late_in.at[pl.ds(0, 2 * n - 1)]).wait_send())
        pl.when(visitor)(lambda: gathered(2, late_in).wait_send())
        gathered(1, raw_ref.at[pl.ds(0, (n * n - 1) * 8), pl.ds(0, 128)]).wait_send()

    from_others(0, raw_all, n - 1).wait_send()
    pl.when(jnp.logical_not(late))(lambda: from_others(1, block_all, n - 1).wait_send())
    pl.when(owner)(lambda: from_others(2, late_in, n - 1).wait_send())
    gain_copy.wait_send()
    token_keep.wait()


def project(tokens, w_down, gain, w_up, head_counts, cotangent):
    n = lax.axis_size("dp")
    count, cols = cotangent.shape
    depth = w_up.shape[0]
    down_rows, width = w_down.shape
    half = (cols // 128 + 1) // 2 * 128
    tile = 256 if half % 256 == 0 else 128
    tiles = half // tile
    ends = min(2, tiles - 1)
    body = tiles - ends
    sizes = []
    while sum(sizes) < body:
        left = body - sum(sizes)
        sizes.append(min(2, left))
    parts = len(sizes)
    cut = depth - 128
    spans = [(0, depth, sum(sizes[:i]) * tile, sizes[i] * tile) for i in range(parts)]
    extra = 2 * half - cols
    spans[0] = (0, depth, extra, sizes[0] * tile - extra)
    spans.insert(0, (0, depth, 0, extra))
    spans.append((0, cut, body * tile, ends * tile))
    for i in range(ends):
        spans.append((cut, 128, (body + i) * tile, tile))
    spans = tuple(spans)
    parts = len(spans)
    pieces = 2
    hbm = pl.BlockSpec(memory_space=pl.ANY)
    bf16, f32 = jnp.bfloat16, jnp.float32
    dma = pltpu.SemaphoreType.DMA
    return pl.pallas_call(
        functools.partial(project_kernel, n, spans, tile, pieces),
        out_shape=(
            jax.ShapeDtypeStruct((count, cols), bf16),
            jax.ShapeDtypeStruct((count, down_rows), bf16),
        ),
        in_specs=[hbm] * 6,
        out_specs=(hbm, hbm),
        scratch_shapes=[
            pltpu.VMEM(gain.shape, f32),
            pltpu.SMEM(head_counts.shape, jnp.int32),
            pltpu.VMEM(tokens.shape, bf16),
            pltpu.VMEM((count, cols), bf16),
            pltpu.VMEM((count, half), bf16),
            pltpu.VMEM((n * down_rows, width), bf16),
            pltpu.VMEM((down_rows, n * width), bf16),
            pltpu.VMEM((n * depth, half), bf16),
            pltpu.VMEM((n * count, half), bf16),
            pltpu.VMEM((n * count, half), bf16),
            pltpu.VMEM((n * count, n * width), bf16),
            pltpu.VMEM((count, width), bf16),
            pltpu.VMEM((n * count, n * depth), bf16),
            pltpu.VMEM((2 * n, count, depth), bf16),
            pltpu.VMEM((2 * n, count // 2, depth), bf16),
            pltpu.VMEM(gain.shape, f32),
            pltpu.VMEM((count, 128), f32),
            pltpu.VMEM((n * count, depth), f32),
            pltpu.VMEM((n * count, depth), f32),
            pltpu.VMEM((count, width), f32),
            pltpu.VMEM((count, 128), f32),
            pltpu.VMEM((8, count), f32),
            pltpu.VMEM((n - 1, 8, count), f32),
            pltpu.VMEM((n * count, 128), f32),
            pltpu.VMEM((n, 8, count), f32),
            pltpu.VMEM((2 * n, 8, count), f32),
            pltpu.VMEM((n, count, width), f32),
            pltpu.VMEM((n, count, width), f32),
            pltpu.VMEM((n, count, width), bf16),
            pltpu.VMEM((n * count, ends * tile), f32),
            pltpu.VMEM((count, down_rows), f32),
            pltpu.VMEM((count, down_rows), bf16),
            dma((6,)),
            dma((5,)),
            dma((3, pieces + 1)),
            dma((3,)),
            dma((3,)),
            dma((n,)),
            dma((n,)),
            dma((3,)),
            dma((n + 1,)),
            dma((3,)),
            dma((n + 1,)),
            dma((2,)),
            dma((2 * parts + 1,)),
            dma((4,)),
            dma((3,)),
            dma((3,)),
            dma((1,)),
            dma((1,)),
            dma((4,)),
            dma((4,)),
        ],
        compiler_params=pltpu.CompilerParams(
            collective_id=0, has_side_effects=True, vmem_limit_bytes=60 * 2**20
        ),
    )(tokens, w_down, gain, w_up, head_counts, cotangent)


def store_kernel(parts, queries_in, grad_in, queries_out, grad_out, held, grad, sem):
    rows = held.shape[0] // parts

    def span(k):
        return pl.ds(k * rows, rows)

    reads = [
        pltpu.make_async_copy(queries_in.at[span(k)], held.at[span(k)], sem.at[0, k])
        for k in range(parts)
    ] + [pltpu.make_async_copy(grad_in, grad, sem.at[0, parts])]
    writes = [
        pltpu.make_async_copy(held.at[span(k)], queries_out.at[span(k)], sem.at[1, k])
        for k in range(parts)
    ] + [pltpu.make_async_copy(grad, grad_out, sem.at[1, parts])]
    for read in reads:
        read.start()
    for read, write in zip(reads, writes):
        read.wait()
        write.start()
    for write in writes:
        write.wait()


def store(queries, grad_tokens):
    parts = 4
    hbm = pl.BlockSpec(memory_space=pl.ANY)
    return pl.pallas_call(
        functools.partial(store_kernel, parts),
        out_shape=(
            jax.ShapeDtypeStruct(queries.shape, queries.dtype),
            jax.ShapeDtypeStruct(grad_tokens.shape, grad_tokens.dtype),
        ),
        in_specs=[hbm] * 2,
        out_specs=(hbm,) * 2,
        scratch_shapes=[
            pltpu.VMEM(queries.shape, queries.dtype),
            pltpu.VMEM(grad_tokens.shape, grad_tokens.dtype),
            pltpu.SemaphoreType.DMA((2, parts + 1)),
        ],
    )(queries, grad_tokens)


def move_weights_body(tokens, w_down, gain, w_up, head_counts, cotangent):
    return store(*project(tokens, w_down, gain, w_up, head_counts, cotangent))


def solution(mesh):
    in_specs = (
        P(("groups", "dp"), None),
        P("dp", "mp"),
        P("mp"),
        P("dp", "mp"),
        P(),
        P(("groups", "dp"), "mp"),
    )
    out_specs = (P(("groups", "dp"), "mp"), P(("groups", "dp"), "mp"))
    square = mesh.shape["dp"] == mesh.shape["mp"] == 4 and mesh.shape["groups"] == 2
    body = move_weights_body if square else gather_weights_body
    return jax.shard_map(body, mesh=mesh, in_specs=in_specs, out_specs=out_specs, check_vma=False)
```

```python
import functools

import jax
import jax.numpy as jnp
from jax import lax
from jax.experimental import pallas as pl
from jax.experimental.pallas import tpu as pltpu
from jax.sharding import PartitionSpec as P

HD = 192
MESH = pl.DeviceIdType.MESH


def contract_last(left, right):
    return lax.dot_general(
        left, right, (((1,), (1,)), ((), ())), preferred_element_type=jnp.float32
    )


def keep_mask_of(head_counts, block_cols):
    position = lax.axis_index("mp")
    held_heads = lax.dynamic_slice_in_dim(head_counts, position, 1, 0)
    slot_index = jnp.arange(block_cols, dtype=jnp.int32) // HD
    return (slot_index < held_heads).astype(jnp.float32)


def gather_weights_body(tokens, w_down, gain, w_up, head_counts, cotangent):
    latent_width = w_down.shape[1] * lax.axis_size("mp")
    keep_mask = keep_mask_of(head_counts, w_up.shape[1])
    down_whole = lax.all_gather(w_down, "dp", axis=0, tiled=True)
    latent_raw = jnp.dot(tokens, down_whole, preferred_element_type=jnp.float32)
    squares = lax.psum(jnp.sum(latent_raw * latent_raw, axis=1, keepdims=True), "mp")
    root_mean = jnp.sqrt(squares / latent_width + 1e-06)
    latent_local = (latent_raw / root_mean * gain).astype(jnp.bfloat16)
    latent = lax.all_gather(latent_local, "mp", axis=1, tiled=True)
    masked = cotangent * keep_mask.astype(jnp.bfloat16)
    up_whole = lax.all_gather(w_up, "dp", axis=0, tiled=True)
    query_total = jnp.dot(latent, up_whole, preferred_element_type=jnp.float32)
    grad_partial = contract_last(masked, up_whole)
    queries = (query_total * keep_mask).astype(jnp.bfloat16)
    grad_latent = lax.psum_scatter(
        grad_partial.astype(jnp.bfloat16), "mp", scatter_dimension=1, tiled=True
    ).astype(jnp.float32)
    inner_dot = lax.psum(jnp.sum(gain * grad_latent * latent_raw, axis=1, keepdims=True), "mp")
    grad_raw = (
        gain * grad_latent / root_mean - latent_raw * inner_dot / (latent_width * root_mean**3)
    ).astype(jnp.bfloat16)
    partial_value = contract_last(grad_raw, down_whole).astype(jnp.bfloat16)
    grad_tokens = lax.psum_scatter(partial_value, "mp", scatter_dimension=1, tiled=True)
    return (queries, grad_tokens)


def project_kernel(
    n, spans, tile, pieces, tokens_hbm, down_hbm, gain_hbm, w_hbm, counts_hbm, cot_hbm,
    queries_ref, grad_tokens_ref, gain_ref, counts_ref, tokens_ref, cot_ref, cot_pass, down_all, down_feat, w_all,
    cots, query_out, latents, latent_out, grad_out, grad_in, late_in, gain_far, slope_ref, total, last_total, raw_ref,
    root_ref, square_out, square_in, dot_total, dot_out, dot_in, raw_all, block_all, grad_all, query_part,
    token_total, token_out, local_sem, down_send, down_recv, across_send, across_recv,
    feat_send, feat_recv, cot_send, cot_recv, latent_send, latent_recv, w_send, w_recv,
    query_sem, grad_send, grad_recv, small_send, small_recv, peer_send, peer_recv,
):
    g, d, m = lax.axis_index("groups"), lax.axis_index("dp"), lax.axis_index("mp")
    other = 1 - g
    upper = (d >= 2).astype(jnp.int32)
    mid, edge = 1 + upper, 3 * upper
    far_mid, far_edge = 2 - upper, 3 - 3 * upper
    inner = d == mid
    outer = jnp.logical_not(inner)
    role = 1 - inner.astype(jnp.int32)
    count, cols = cot_ref.shape
    depth = w_hbm.shape[0]
    down_rows, width = down_hbm.shape
    half = cots.shape[1]
    step = cols - half
    extra = half - step
    spare_rows = extra * depth // width
    plane_rows = (down_rows - spare_rows) // 2
    piece_rows = plane_rows // pieces
    chunks = len(spans)

    def at_rows(k, size):
        return pl.ds(pl.multiple_of(k * size, size), size)

    down_load = pltpu.make_async_copy(
        down_hbm, down_all.at[at_rows(d, down_rows)], local_sem.at[0]
    )
    cot_load = pltpu.make_async_copy(cot_hbm, cot_ref, local_sem.at[1])
    w_load = pltpu.make_async_copy(
        w_hbm.at[:, pl.ds(pl.multiple_of(g * step, 128), half)],
        w_all.at[at_rows(d, depth)], local_sem.at[2],
    )
    tokens_load = pltpu.make_async_copy(tokens_hbm, tokens_ref, local_sem.at[3])
    down_load.start()
    cot_load.start()
    w_load.start()
    tokens_load.start()
    gain_load = pltpu.make_async_copy(gain_hbm, gain_ref, local_sem.at[4])
    counts_load = pltpu.make_async_copy(counts_hbm, counts_ref, local_sem.at[5])
    gain_load.start()
    counts_load.start()

    barrier = pltpu.get_barrier_semaphore()

    def greet(**where):
        pl.semaphore_signal(barrier, inc=1, device_id=where, device_id_type=MESH)

    for plane in range(2):
        for place in (0, 1):
            for who in range(n):
                there = mid if place == 0 else edge
                itself = jnp.logical_and(
                    g == plane, jnp.logical_and(role == place, m == who)
                )
                distant = jnp.logical_and(
                    g != plane,
                    jnp.logical_and(role != place, (m >= 2) != (who >= 2)),
                )
                pl.when(jnp.logical_not(jnp.logical_or(itself, distant)))(
                    lambda plane=plane, there=there, who=who: greet(
                        groups=plane, dp=there, mp=who
                    )
                )
    pl.when(inner)(lambda: greet(dp=far_mid))
    down_load.wait()
    pl.when(inner)(lambda: pl.semaphore_wait(barrier, 4 * n - 2))
    pl.when(outer)(lambda: pl.semaphore_wait(barrier, 4 * n - 3))

    def remote(source, target, send, recv, **where):
        return pltpu.make_async_remote_copy(
            src_ref=source, dst_ref=target, send_sem=send, recv_sem=recv,
            device_id=where, device_id_type=MESH,
        )

    def down_span(plane, k):
        if k == pieces:
            return plane_rows, spare_rows
        return plane * (plane_rows + spare_rows) + k * piece_rows, piece_rows

    def down_piece(shard, plane, k):
        start, rows = down_span(plane, k)
        return down_all.at[pl.ds(pl.multiple_of(shard * down_rows + start, 16), rows)]

    def down_copy(way, kind, shard, k, to):
        held = down_piece(shard, g, k)
        return remote(held, held, down_send.at[way], down_recv.at[kind, k], dp=to)

    def down_across(kind, shard, k):
        held = down_piece(shard, g, k)
        return remote(held, held, across_send.at[kind], across_recv.at[kind], groups=other)

    def for_each_plane(body):
        for plane in range(2):
            pl.when(g == plane)(lambda plane=plane: body(plane))

    def moved_rows(shard, plane):
        rows = plane_rows + plane * spare_rows
        start = shard * down_rows + plane * plane_rows
        return down_all.at[pl.ds(pl.multiple_of(start, 16), rows)]

    def down_sent(way):
        def wait(plane):
            held = moved_rows(d, plane)
            remote(
                held, held, down_send.at[way], down_recv.at[0, 0], dp=far_mid
            ).wait_send()

        for_each_plane(wait)

    def crossed(kind, shard, plane):
        held = moved_rows(shard, plane)
        return remote(held, held, across_send.at[kind], across_recv.at[kind], groups=other)

    def each_piece(act):
        for k in range(pieces):
            act(k)
        pl.when(g == 1)(lambda: act(pieces))

    def cot_half(plane):
        return cot_ref.at[:, pl.ds(pl.multiple_of(plane * step, 128), half)]

    def cot_copy(way, source, slot, plane, to):
        return remote(
            source, cots.at[at_rows(slot, count)], cot_send.at[way], cot_recv.at[slot],
            groups=plane, dp=to,
        )

    def cot_across():
        return remote(
            cot_half(other), cot_pass, cot_send.at[2], cot_recv.at[n], groups=other
        )

    def cot_arrival(slot):
        held = cots.at[at_rows(slot, count)]
        return remote(held, held, cot_send.at[0], cot_recv.at[slot], dp=far_mid)

    def w_rows(shard, row, rows):
        return pl.ds(pl.multiple_of(shard * depth + row, 128), rows)

    def w_piece(shard, j):
        row, rows, first, size = spans[j]
        return w_all.at[w_rows(shard, row, rows), pl.ds(first, size)]

    def w_copy(way, kind, shard, j, to):
        held = w_piece(shard, j)
        sem = w_recv.at[2 * chunks] if kind == 1 else w_recv.at[kind // 2 * chunks + j]
        return remote(held, held, w_send.at[way], sem, dp=to)

    def w_moved(way, shard, plane):
        first = plane * extra
        held = w_all.at[at_rows(shard, depth), pl.ds(first, half - first)]
        return remote(held, held, w_send.at[way], w_recv.at[2 * chunks], dp=far_mid)

    def for_chunk(j, act):
        if j == 0:
            pl.when(g == 0)(act)
        else:
            act()

    def keep_cot():
        cots[at_rows(2 * g, count), :] = cot_ref[
            :, pl.ds(pl.multiple_of(g * step, 128), half)
        ]

    def feat_copy(shard, plane, k):
        start, rows = down_span(plane, k)
        return remote(
            down_piece(shard, plane, k),
            down_feat.at[pl.ds(pl.multiple_of(start, 16), rows), at_rows(m, width)],
            feat_send.at[shard], feat_recv.at[m], mp=shard,
        )

    def feat_piece(shard, plane, k):
        pl.when(shard != m)(lambda: feat_copy(shard, plane, k).start())

    def crossed_feat(shard):
        for k in range(pieces):
            feat_piece(shard, other, k)
        pl.when(g == 0)(lambda: feat_piece(shard, other, pieces))

    def feat_whole(sent, arrived):
        held = down_feat.at[:, at_rows(arrived, width)]
        return remote(held, held, feat_send.at[sent], feat_recv.at[arrived], groups=other)

    def keep_feat():
        @pl.loop(0, down_rows // 128)
        def _(k):
            source = m * down_rows + k * 128
            down_feat[at_rows(k, 128), at_rows(m, width)] = down_all[
                pl.ds(pl.multiple_of(source, 128), 128), :
            ]

    early = 4

    @pl.when(inner)
    def _():
        def start_own(k):
            down_copy(0, 1, d, k, far_mid).start()
            down_copy(1, 0, d, k, edge).start()

        each_piece(start_own)
        for k in range(pieces + 1):
            feat_piece(d, 0, k)
        for k in range(pieces):
            feat_piece(d, 1, k)
        cot_load.wait()
        keep_cot()

        @pl.when(g == 1)
        def _():
            for shard in (edge, far_mid, far_edge):
                w_all[at_rows(shard, depth), :extra] = jnp.zeros((depth, extra), w_all.dtype)

        def pass_near(k):
            for kind, sent, shard, way, to in (
                (0, 2, edge, 2, far_mid), (1, 1, far_mid, 3, edge)
            ):
                down_copy(way, kind, shard, k, to).wait_recv()
                down_copy(way, sent, shard, k, to).start()
                down_across(kind, shard, k).start()
                feat_piece(shard, g, k)

        each_piece(pass_near)
        w_load.wait()
        for j in range(chunks):
            for_chunk(j, lambda j=j: w_copy(0, 1, d, j, far_mid).start())

        def pass_far(k):
            down_copy(4, 2, far_edge, k, edge).wait_recv()
            down_copy(4, 2, far_edge, k, edge).start()
            down_across(2, far_edge, k).start()
            feat_piece(far_edge, g, k)

        each_piece(pass_far)
        cot_copy(0, cot_half(other), 2 * g, other, d).start()

    @pl.when(outer)
    def _():
        each_piece(lambda k: down_copy(0, 0, d, k, mid).start())
        cot_load.wait()
        cot_across().start()
        cot_copy(0, cot_half(g), 2 * g + 1, g, mid).start()
        for k in range(pieces + 1):
            feat_piece(d, 0, k)
        for k in range(pieces):
            feat_piece(d, 1, k)
        w_load.wait()
        for kind, shard in enumerate((mid, far_mid, far_edge)):

            def take(k):
                down_copy(0, kind, shard, k, mid).wait_recv()
                down_across(kind, shard, k).start()
                feat_piece(shard, g, k)

            each_piece(take)
            if kind == 0:
                cot_across().wait_recv()
                cot_copy(1, cot_pass, 2 * other + 1, g, mid).start()
                for j in range(early):
                    for_chunk(j, lambda j=j: w_copy(0, 0, d, j, mid).start())

    neighbours = (jnp.where(inner, edge, mid), far_mid, far_edge)
    for kind, shard in enumerate(neighbours):
        for_each_plane(lambda plane: crossed(kind, shard, 1 - plane).wait_recv())
        if kind < 2:
            crossed_feat(shard)

    tokens_load.wait()
    gain_load.wait()
    counts_load.wait()
    raw_ref[...] = jnp.zeros_like(raw_ref)

    @pl.loop(0, 2 * n)
    def _(c):
        at = at_rows(c, down_rows // 2)
        raw_ref[...] += jnp.dot(
            tokens_ref[:, at], down_all[at, :], preferred_element_type=jnp.float32
        )

    def to_peer(sent, arrived, source, target, mp):
        return remote(source, target, small_send.at[sent], small_recv.at[arrived], mp=mp)

    raw = raw_ref[...]
    square_out[...] = jnp.broadcast_to(
        jnp.sum(raw * raw, axis=1, keepdims=True), (count, 128)
    ).T[:8]
    for o in range(1, n):
        to_peer(0, 0, square_out, square_in.at[o - 1], lax.rem(m + o, n)).start()
    to_peer(0, 0, square_in, square_in, far_mid).wait_recv()
    value = square_out[...]
    for o in range(1, n):
        value += square_in[o - 1]
    squares = jnp.broadcast_to(value[:1], (128, count)).T[:, :1]
    root = jnp.sqrt(squares / (width * n) + 1e-06)
    root_ref[...] = jnp.broadcast_to(root, root_ref.shape)
    gain = gain_ref[...].reshape(1, width)
    latent_out[...] = (raw / root * gain).astype(latent_out.dtype)

    def latent_at(slot, who):
        return latents.at[at_rows(slot, count), at_rows(who, width)]

    def latent_inward(to):
        return remote(
            latent_out, latent_at(2 * g + role, m), latent_send.at[to],
            latent_recv.at[2 * g + role], groups=to, dp=mid,
        )

    def latent_arrival(slot):
        held = latent_at(slot, m)
        return remote(held, held, latent_send.at[0], latent_recv.at[slot], dp=far_mid)

    def latent_spread(slot, o):
        held = latent_at(slot, m)
        return remote(
            held, held, latent_send.at[2], latent_recv.at[n], mp=lax.rem(m + o, n)
        )

    def latents_spread():
        held = latents.at[:, pl.ds(0, (n - 1) * width)]
        return remote(held, held, latent_send.at[2], latent_recv.at[n], dp=far_mid)

    slots = (2 * g, 2 * other, 2 * g + 1, 2 * other + 1)

    cut = depth - 128
    grad_parts = ((0, cut), (cut, 128))

    def add_grad(sum_ref, shard, row, rows, t):
        at = at_rows(t, tile)
        sum_ref[:, row:row + rows] += contract_last(
            cots[:, at], w_all[w_rows(shard, row, rows), at]
        )

    def grad_copy(shard, slot, part):
        row, rows = grad_parts[part]
        return remote(
            grad_out.at[at_rows(slot, count), w_rows(shard, row, rows)],
            grad_in.at[g * n + m, :, pl.ds(row, rows)],
            grad_send.at[0], grad_recv.at[0],
            groups=slot // 2, dp=mid if slot % 2 == 0 else edge, mp=shard,
        )

    def is_self(shard, slot):
        return jnp.logical_and(g == slot // 2, m == shard)

    def each_grad(shard, part, act):
        for slot in range(n):
            if slot % 2 == 1:
                act(grad_copy(shard, slot, part))
                continue
            pl.when(jnp.logical_not(is_self(shard, slot)))(
                lambda slot=slot: act(grad_copy(shard, slot, part))
            )

    half_count = count // 2
    late_owners = (far_edge, lax.rem(far_edge + 2, n))

    def late_copy(slot, side, part):
        row, rows = grad_parts[part]
        source = pl.ds(pl.multiple_of(slot * count + side * half_count, 16), half_count)
        return remote(
            grad_out.at[source, w_rows(far_edge, row, rows)],
            late_in.at[g * n + m, :, pl.ds(row, rows)],
            grad_send.at[2], grad_recv.at[2], groups=slot // 2,
            dp=mid if slot % 2 == 0 else edge, mp=late_owners[side],
        )

    def send_late(sum_ref, part):
        row, rows = grad_parts[part]
        grad_out[:, w_rows(far_edge, row, rows)] = sum_ref[:, row:row + rows].astype(
            grad_out.dtype
        )
        for slot in range(n):
            for side in range(2):
                if slot % 2 == 1:
                    late_copy(slot, side, part).start()
                    continue
                itself = is_self(late_owners[side], slot)
                pl.when(jnp.logical_not(itself))(
                    lambda slot=slot, side=side: late_copy(slot, side, part).start()
                )
        for side in range(2):

            @pl.when(m == late_owners[side])
            def _():
                source = pl.ds(
                    pl.multiple_of(2 * g * count + side * half_count, 16), half_count
                )
                late_in[g * n + m, :, row:row + rows] = grad_out[
                    source, w_rows(far_edge, row, rows)
                ]

    def send_grad(sum_ref, shard, part):
        row, rows = grad_parts[part]
        grad_out[:, w_rows(shard, row, rows)] = sum_ref[:, row:row + rows].astype(
            grad_out.dtype
        )
        each_grad(shard, part, lambda c: c.start())

        @pl.when(m == shard)
        def _():
            grad_in[g * n + m, :, row:row + rows] = grad_out[
                at_rows(2 * g, count), w_rows(shard, row, rows)
            ]

    def whole_grad(shard):
        total[...] = jnp.zeros_like(total)

        @pl.loop(0, half // tile)
        def _(t):
            add_grad(total, shard, 0, depth, t)

        for part in range(2):
            send_grad(total, shard, part)

    def query_parts(j):
        row, rows, first, size = spans[j]
        if row + rows < depth:
            return ()
        return ((first, size, j == 0),)

    def query_copy(slot, first, size):
        return remote(
            query_out.at[at_rows(slot, count), pl.ds(first, size)],
            queries_ref.at[:, pl.ds(pl.multiple_of(g * step + first, 128), size)],
            query_sem.at[2], query_sem.at[g],
            groups=slot // 2, dp=mid if slot % 2 == 0 else edge,
        )

    def query_keep(first, size):
        return pltpu.make_async_copy(
            query_out.at[at_rows(2 * g, count), pl.ds(first, size)],
            queries_ref.at[:, pl.ds(pl.multiple_of(g * step + first, 128), size)],
            query_sem.at[3],
        )

    def send_queries(j):
        for first, size, once in query_parts(j):

            def act():
                for slot in range(n):
                    if slot % 2 == 1:
                        query_copy(slot, first, size).start()
                        continue
                    mine = g == slot // 2
                    pl.when(jnp.logical_not(mine))(
                        lambda slot=slot: query_copy(slot, first, size).start()
                    )
                query_keep(first, size).start()

            if once:
                pl.when(g == 0)(act)
            else:
                act()

    def keep_row(t):
        column = lax.broadcasted_iota(jnp.int32, (1, tile), 1) + (g * step + t * tile)
        return (column < counts_ref[m] * HD).astype(jnp.float32)

    ends = sum(row > 0 for row, rows, first, size in spans)
    first_late = min(first for row, rows, first, size in spans if row > 0)

    def late_at(t):
        return pl.ds(pl.multiple_of(t * tile - first_late, tile), tile)

    def query_sum(shard, row, rows, at):
        return jnp.dot(
            latents[:, w_rows(shard, row, rows)], w_all[w_rows(shard, row, rows), at],
            preferred_element_type=jnp.float32,
        )

    def query_start(t):
        at = at_rows(t, tile)
        product = query_sum(far_edge, 0, cut, at)
        for shard in (d, edge, far_mid):
            product += query_sum(shard, 0, depth, at)
        query_part[:, late_at(t)] = product

    def query_end(t):
        at = at_rows(t, tile)
        finish_query(t, query_part[:, late_at(t)] + query_sum(far_edge, cut, depth - cut, at))

    def query_tile(t):
        at = at_rows(t, tile)
        finish_query(
            t, jnp.dot(latents[...], w_all[:, at], preferred_element_type=jnp.float32)
        )

    def finish_query(t, product):
        at = at_rows(t, tile)
        query_out[:, at] = (product * keep_row(t)).astype(query_out.dtype)
        dots = product * cots[:, at].astype(jnp.float32)
        for part in range(tile // 128):
            dot_total[...] += dots[:, part * 128:(part + 1) * 128]

    def dot_copy(slot, to):
        return remote(
            dot_out.at[slot], dot_in.at[g * n + m], grad_send.at[1], grad_recv.at[1],
            groups=slot // 2,
            dp=mid if slot % 2 == 0 else edge, mp=to,
        )

    def each_dot(act):
        for slot in range(n):
            for to in range(n):
                if slot % 2 == 1:
                    act(dot_copy(slot, to))
                    continue
                pl.when(jnp.logical_not(is_self(to, slot)))(
                    lambda slot=slot, to=to: act(dot_copy(slot, to))
                )

    def send_dots():
        for slot in range(n):
            column = jnp.sum(dot_total[at_rows(slot, count), :], axis=1, keepdims=True)
            dot_out[slot] = jnp.broadcast_to(column, (count, 128)).T[:8]
        each_dot(lambda c: c.start())
        dot_in[g * n + m] = dot_out[2 * g]

    def finish_chunk(j):
        row, rows, first, size = spans[j]
        for_chunk(j, w_copy(0, 2, far_edge, j, far_mid).wait_recv)
        if j == 0:
            return
        if j == 1:
            first, size = 0, first + size

        @pl.loop(first // tile, (first + size) // tile)
        def _(t):
            add_grad(last_total, far_edge, row, rows, t)

        if row == 0 and rows == cut:
            send_late(last_total, 0)
        if j == chunks - 1:
            send_late(last_total, 1)
        body = query_tile if rows == depth else query_end if row > 0 else query_start
        pl.loop(first // tile, (first + size) // tile)(body)
        if j == chunks - 1:
            send_dots()
        if row > 0 and j < chunks - 1:
            return
        for i in range(j if row == 0 else chunks - ends, j + 1):
            if i == 1:
                send_queries(0)
            send_queries(i)

    def gathered(sem, held):
        return remote(held, held, grad_send.at[sem], grad_recv.at[sem], groups=other)

    def all_sources(sem, buffer):
        pl.when(inner)(lambda: gathered(sem, buffer.at[pl.ds(0, 2 * n - 1)]).wait_recv())
        pl.when(outer)(lambda: gathered(sem, buffer).wait_recv())

    late = m == far_edge

    def own_block():
        all_sources(0, grad_in)
        grad_latent = grad_in[0].astype(jnp.float32)
        for source in range(1, 2 * n):
            grad_latent += grad_in[source].astype(jnp.float32)
        return gain_ref[...].reshape(1, width) * grad_latent / root_ref[:, :1]

    def to_others(sem, held):
        return [
            remote(held, held, peer_send.at[sem], peer_recv.at[sem], mp=lax.rem(m + o, n))
            for o in (2, 1, 3)
        ]

    def from_others(sem, buffer, blocks):
        held = buffer.at[pl.ds(0, blocks)]
        return remote(held, held, peer_send.at[sem], peer_recv.at[sem], groups=other)

    def early_block(ready):
        @pl.when(jnp.logical_and(jnp.logical_not(late), ready))
        def _():
            block_all[m] = own_block()
            for c in to_others(1, block_all.at[m]):
                c.start()

    gain_copy = remote(
        gain_ref, gain_far, peer_send.at[3], peer_recv.at[3], mp=lax.rem(m + 2, n)
    )

    def start_raw():
        gain_copy.start()
        raw_all[m] = raw_ref[...]
        for c in to_others(0, raw_all.at[m]):
            c.start()

    @pl.when(outer)
    def _():
        latent_inward(0).start()
        latent_inward(1).start()
        for j in range(early, chunks):
            for_chunk(j, lambda j=j: w_copy(0, 0, d, j, mid).start())
        crossed_feat(far_edge)
        start_raw()
        keep_feat()

    def pass_on(j):
        def act():
            w_copy(0, 0, edge, j, far_mid).wait_recv()
            w_copy(1, 2, edge, j, far_mid).start()

        for_chunk(j, act)

    @pl.when(inner)
    def _():
        latents[at_rows(2 * g, count), at_rows(m, width)] = latent_out[...]
        latent_inward(other).start()
        for o in range(1, n):
            latent_spread(slots[0], o).start()
        crossed_feat(far_edge)
        keep_feat()
        for j in range(early):
            pass_on(j)
        for slot in slots[1:]:
            latent_arrival(slot).wait_recv()
            for o in range(1, n):
                latent_spread(slot, o).start()

        for slot in slots[1:]:
            cot_arrival(slot).wait_recv()

        @pl.loop(0, half // tile)
        def _(t):
            at = at_rows(t, tile)
            cots[:, at] = cots[:, at] * keep_row(t).astype(cots.dtype)

        @pl.when(g == 1)
        def _():
            cots[:, :extra] = jnp.zeros((n * count, extra), cots.dtype)

        whole_grad(d)
        for_each_plane(lambda plane: w_moved(0, far_mid, plane).wait_recv())
        whole_grad(far_mid)
        latents_spread().wait_recv()
        start_raw()
        last_total[...] = jnp.zeros_like(last_total)
        dot_total[...] = jnp.zeros_like(dot_total)
        passed = early
        for j in range(chunks):
            for _ in range(min((0, 1, 2)[j] if j < 3 else chunks, chunks - passed)):
                pass_on(passed)
                passed += 1
            finish_chunk(j)
            if j == 3:
                whole_grad(edge)
            if j == 2:
                early_block(m != edge)
            if j == 5:
                early_block(m == edge)

    to_peer(0, 0, square_in, square_in, far_mid).wait_send()
    for o in range(1, n):
        feat_whole(lax.rem(m + o, n), m).wait_send()
        feat_whole(m, lax.rem(m + o, n)).wait_recv()
    for kind, shard in enumerate(neighbours):
        for_each_plane(lambda plane: crossed(kind, shard, plane).wait_send())
    down_sent(0)
    cot_copy(0, cot_half(g), 2 * g, g, mid).wait_send()

    def w_own_sent(plane):
        w_moved(0, d, plane).wait_send()

    for_each_plane(w_own_sent)
    latent_inward(other).wait_send()

    @pl.when(outer)
    def _():
        cot_copy(1, cot_half(g), 2 * g, g, mid).wait_send()
        cot_across().wait_send()
        latent_inward(g).wait_send()

    @pl.when(inner)
    def _():
        for way in range(1, 5):
            down_sent(way)
        latents_spread().wait_send()

    early_block(outer)
    all_sources(1, dot_in)
    dots = dot_in[0]
    for source in range(1, 2 * n):
        dots += dot_in[source]
    inner_dot = jnp.broadcast_to(dots[:1], (128, count)).T[:, :1]
    root = root_ref[:, :1]
    slope = inner_dot / (width * n * (root * root))

    slope_ref[...] = jnp.broadcast_to(slope, slope_ref.shape)
    owner = jnp.logical_or(m == late_owners[0], m == late_owners[1])
    visitor = jnp.logical_not(owner)
    mine = pl.ds(
        pl.multiple_of((1 - late.astype(jnp.int32)) * half_count, half_count), half_count
    )
    gain_copy.wait_recv()
    from_others(0, raw_all, n - 1).wait_recv()

    @pl.when(owner)
    def _():
        all_sources(2, late_in)
        summed = late_in[0].astype(jnp.float32)
        for source in range(1, 2 * n):
            summed += late_in[source].astype(jnp.float32)
        gain = jnp.where(late, gain_ref[...].reshape(1, width), gain_far[...].reshape(1, width))
        value = gain * summed / root_ref[mine, :1]
        value -= raw_all[far_edge, mine, :] * slope_ref[mine, :1]
        grad_all[far_edge, mine, :] = value.astype(grad_all.dtype)
        for c in to_others(2, grad_all.at[far_edge, mine, :]):
            c.start()

    row_tile = down_rows

    def add_block(who, first, last):
        @pl.loop(0, down_rows // row_tile)
        def _(c):
            rows = at_rows(c, row_tile)
            value = contract_last(grad_all[who], down_feat[rows, at_rows(who, width)])
            if not first:
                value += token_total[:, rows]
            if last:
                token_out[:, rows] = value.astype(token_out.dtype)
            else:
                token_total[:, rows] = value

    pl.when(late)(lambda: from_others(1, block_all, n - 1).wait_recv())
    pl.when(jnp.logical_not(late))(lambda: from_others(1, block_all, n - 2).wait_recv())
    for who in (1, 2, edge):
        grad_all[who] = (block_all[who] - raw_all[who] * slope).astype(grad_all.dtype)
        add_block(who, isinstance(who, int) and who == 1, False)

    pl.when(visitor)(lambda: from_others(2, grad_all, 1).wait_recv())
    theirs = pl.ds(pl.multiple_of(late.astype(jnp.int32) * half_count, half_count), half_count)

    def other_half():
        held = grad_all.at[far_edge, theirs, :]
        return remote(held, held, peer_send.at[2], peer_recv.at[2], groups=other)

    pl.when(owner)(lambda: other_half().wait_recv())
    add_block(far_edge, False, True)
    token_keep = pltpu.make_async_copy(token_out, grad_tokens_ref, local_sem.at[0])
    token_keep.start()

    def query_arrival(plane):
        first = plane * cols - plane * (half - extra)
        part = queries_ref.at[:, pl.ds(first, half - plane * extra)]
        return remote(part, part, query_sem.at[2], query_sem.at[plane], groups=other)

    for plane in range(2):
        away = jnp.logical_not(jnp.logical_and(inner, g == plane))
        pl.when(away)(lambda plane=plane: query_arrival(plane).wait_recv())

    @pl.when(inner)
    def _():
        for_each_plane(lambda plane: w_moved(1, edge, plane).wait_send())
        for plane in range(2):

            @pl.when(g == plane)
            def _():
                size = half - plane * extra
                part = query_out.at[pl.ds(0, (n - 1) * count), pl.ds(0, size)]
                remote(
                    part, part, query_sem.at[2], query_sem.at[plane], groups=other
                ).wait_send()
                query_keep(half - size, size).wait()

        def early_sent(blocks):
            held = down_all.at[pl.ds(0, blocks * count), pl.ds(0, depth)]
            gathered(0, held).wait_send()

        pl.when(late)(lambda: early_sent(3 * n))
        pl.when(jnp.logical_not(late))(lambda: early_sent(3 * n - 1))
        pl.when(owner)(lambda: gathered(2, late_in.at[pl.ds(0, 2 * n - 1)]).wait_send())
        pl.when(visitor)(lambda: gathered(2, late_in).wait_send())
        gathered(1, raw_ref.at[pl.ds(0, (n * n - 1) * 8), pl.ds(0, 128)]).wait_send()

    from_others(0, raw_all, n - 1).wait_send()
    pl.when(jnp.logical_not(late))(lambda: from_others(1, block_all, n - 1).wait_send())
    pl.when(owner)(lambda: from_others(2, late_in, n - 1).wait_send())
    gain_copy.wait_send()
    token_keep.wait()


def project(tokens, w_down, gain, w_up, head_counts, cotangent):
    n = lax.axis_size("dp")
    count, cols = cotangent.shape
    depth = w_up.shape[0]
    down_rows, width = w_down.shape
    half = (cols // 128 + 1) // 2 * 128
    tile = 256 if half % 256 == 0 else 128
    tiles = half // tile
    ends = min(2, tiles - 1)
    body = tiles - ends
    sizes = []
    while sum(sizes) < body:
        left = body - sum(sizes)
        sizes.append(min(2, left))
    parts = len(sizes)
    cut = depth - 128
    spans = [(0, depth, sum(sizes[:i]) * tile, sizes[i] * tile) for i in range(parts)]
    extra = 2 * half - cols
    spans[0] = (0, depth, extra, sizes[0] * tile - extra)
    spans.insert(0, (0, depth, 0, extra))
    spans.append((0, cut, body * tile, ends * tile))
    for i in range(ends):
        spans.append((cut, 128, (body + i) * tile, tile))
    spans = tuple(spans)
    parts = len(spans)
    pieces = 2
    hbm = pl.BlockSpec(memory_space=pl.ANY)
    bf16, f32 = jnp.bfloat16, jnp.float32
    dma = pltpu.SemaphoreType.DMA
    return pl.pallas_call(
        functools.partial(project_kernel, n, spans, tile, pieces),
        out_shape=(
            jax.ShapeDtypeStruct((count, cols), bf16),
            jax.ShapeDtypeStruct((count, down_rows), bf16),
        ),
        in_specs=[hbm] * 6,
        out_specs=(hbm, hbm),
        scratch_shapes=[
            pltpu.VMEM(gain.shape, f32),
            pltpu.SMEM(head_counts.shape, jnp.int32),
            pltpu.VMEM(tokens.shape, bf16),
            pltpu.VMEM((count, cols), bf16),
            pltpu.VMEM((count, half), bf16),
            pltpu.VMEM((n * down_rows, width), bf16),
            pltpu.VMEM((down_rows, n * width), bf16),
            pltpu.VMEM((n * depth, half), bf16),
            pltpu.VMEM((n * count, half), bf16),
            pltpu.VMEM((n * count, half), bf16),
            pltpu.VMEM((n * count, n * width), bf16),
            pltpu.VMEM((count, width), bf16),
            pltpu.VMEM((n * count, n * depth), bf16),
            pltpu.VMEM((2 * n, count, depth), bf16),
            pltpu.VMEM((2 * n, count // 2, depth), bf16),
            pltpu.VMEM(gain.shape, f32),
            pltpu.VMEM((count, 128), f32),
            pltpu.VMEM((n * count, depth), f32),
            pltpu.VMEM((n * count, depth), f32),
            pltpu.VMEM((count, width), f32),
            pltpu.VMEM((count, 128), f32),
            pltpu.VMEM((8, count), f32),
            pltpu.VMEM((n - 1, 8, count), f32),
            pltpu.VMEM((n * count, 128), f32),
            pltpu.VMEM((n, 8, count), f32),
            pltpu.VMEM((2 * n, 8, count), f32),
            pltpu.VMEM((n, count, width), f32),
            pltpu.VMEM((n, count, width), f32),
            pltpu.VMEM((n, count, width), bf16),
            pltpu.VMEM((n * count, ends * tile), f32),
            pltpu.VMEM((count, down_rows), f32),
            pltpu.VMEM((count, down_rows), bf16),
            dma((6,)),
            dma((5,)),
            dma((3, pieces + 1)),
            dma((3,)),
            dma((3,)),
            dma((n,)),
            dma((n,)),
            dma((3,)),
            dma((n + 1,)),
            dma((3,)),
            dma((n + 1,)),
            dma((2,)),
            dma((2 * parts + 1,)),
            dma((4,)),
            dma((3,)),
            dma((3,)),
            dma((1,)),
            dma((1,)),
            dma((4,)),
            dma((4,)),
        ],
        compiler_params=pltpu.CompilerParams(
            collective_id=0, has_side_effects=True, vmem_limit_bytes=60 * 2**20
        ),
    )(tokens, w_down, gain, w_up, head_counts, cotangent)


def store_kernel(parts, queries_in, grad_in, queries_out, grad_out, held, grad, sem):
    rows = held.shape[0] // parts

    def span(k):
        return pl.ds(k * rows, rows)

    reads = [
        pltpu.make_async_copy(queries_in.at[span(k)], held.at[span(k)], sem.at[0, k])
        for k in range(parts)
    ] + [pltpu.make_async_copy(grad_in, grad, sem.at[0, parts])]
    writes = [
        pltpu.make_async_copy(held.at[span(k)], queries_out.at[span(k)], sem.at[1, k])
        for k in range(parts)
    ] + [pltpu.make_async_copy(grad, grad_out, sem.at[1, parts])]
    for read in reads:
        read.start()
    for read, write in zip(reads, writes):
        read.wait()
        write.start()
    for write in writes:
        write.wait()


def store(queries, grad_tokens):
    parts = 4
    hbm = pl.BlockSpec(memory_space=pl.ANY)
    return pl.pallas_call(
        functools.partial(store_kernel, parts),
        out_shape=(
            jax.ShapeDtypeStruct(queries.shape, queries.dtype),
            jax.ShapeDtypeStruct(grad_tokens.shape, grad_tokens.dtype),
        ),
        in_specs=[hbm] * 2,
        out_specs=(hbm,) * 2,
        scratch_shapes=[
            pltpu.VMEM(queries.shape, queries.dtype),
            pltpu.VMEM(grad_tokens.shape, grad_tokens.dtype),
            pltpu.SemaphoreType.DMA((2, parts + 1)),
        ],
    )(queries, grad_tokens)


def move_weights_body(tokens, w_down, gain, w_up, head_counts, cotangent):
    return store(*project(tokens, w_down, gain, w_up, head_counts, cotangent))


def solution(mesh):
    in_specs = (
        P(("groups", "dp"), None),
        P("dp", "mp"),
        P("mp"),
        P("dp", "mp"),
        P(),
        P(("groups", "dp"), "mp"),
    )
    out_specs = (P(("groups", "dp"), "mp"), P(("groups", "dp"), "mp"))
    square = mesh.shape["dp"] == mesh.shape["mp"] == 4 and mesh.shape["groups"] == 2
    body = move_weights_body if square else gather_weights_body
    return jax.shard_map(body, mesh=mesh, in_specs=in_specs, out_specs=out_specs, check_vma=False)
```

```python
import functools

import jax
import jax.numpy as jnp
from jax import lax
from jax.experimental import pallas as pl
from jax.experimental.pallas import tpu as pltpu
from jax.sharding import PartitionSpec as P

HD = 192
MESH = pl.DeviceIdType.MESH


def contract_last(left, right):
    return lax.dot_general(
        left, right, (((1,), (1,)), ((), ())), preferred_element_type=jnp.float32
    )


def keep_mask_of(head_counts, block_cols):
    position = lax.axis_index("mp")
    held_heads = lax.dynamic_slice_in_dim(head_counts, position, 1, 0)
    slot_index = jnp.arange(block_cols, dtype=jnp.int32) // HD
    return (slot_index < held_heads).astype(jnp.float32)


def gather_weights_body(tokens, w_down, gain, w_up, head_counts, cotangent):
    latent_width = w_down.shape[1] * lax.axis_size("mp")
    keep_mask = keep_mask_of(head_counts, w_up.shape[1])
    down_whole = lax.all_gather(w_down, "dp", axis=0, tiled=True)
    latent_raw = jnp.dot(tokens, down_whole, preferred_element_type=jnp.float32)
    squares = lax.psum(jnp.sum(latent_raw * latent_raw, axis=1, keepdims=True), "mp")
    root_mean = jnp.sqrt(squares / latent_width + 1e-06)
    latent_local = (latent_raw / root_mean * gain).astype(jnp.bfloat16)
    latent = lax.all_gather(latent_local, "mp", axis=1, tiled=True)
    masked = cotangent * keep_mask.astype(jnp.bfloat16)
    up_whole = lax.all_gather(w_up, "dp", axis=0, tiled=True)
    query_total = jnp.dot(latent, up_whole, preferred_element_type=jnp.float32)
    grad_partial = contract_last(masked, up_whole)
    queries = (query_total * keep_mask).astype(jnp.bfloat16)
    grad_latent = lax.psum_scatter(
        grad_partial.astype(jnp.bfloat16), "mp", scatter_dimension=1, tiled=True
    ).astype(jnp.float32)
    inner_dot = lax.psum(jnp.sum(gain * grad_latent * latent_raw, axis=1, keepdims=True), "mp")
    grad_raw = (
        gain * grad_latent / root_mean - latent_raw * inner_dot / (latent_width * root_mean**3)
    ).astype(jnp.bfloat16)
    partial_value = contract_last(grad_raw, down_whole).astype(jnp.bfloat16)
    grad_tokens = lax.psum_scatter(partial_value, "mp", scatter_dimension=1, tiled=True)
    return (queries, grad_tokens)


def project_kernel(
    n, spans, tile, pieces, tokens_hbm, down_hbm, gain_hbm, w_hbm, counts_hbm, cot_hbm,
    queries_ref, grad_tokens_ref, gain_ref, counts_ref, tokens_ref, cot_ref, cot_pass, down_all, down_feat, w_all,
    cots, query_out, latents, latent_out, grad_out, grad_in, late_in, gain_far, slope_ref, total, last_total, raw_ref,
    root_ref, square_out, square_in, dot_total, dot_out, dot_in, raw_all, block_all, grad_all, query_part,
    token_total, token_out, local_sem, down_send, down_recv, across_send, across_recv,
    feat_send, feat_recv, cot_send, cot_recv, latent_send, latent_recv, w_send, w_recv,
    query_sem, grad_send, grad_recv, small_send, small_recv, peer_send, peer_recv,
):
    g, d, m = lax.axis_index("groups"), lax.axis_index("dp"), lax.axis_index("mp")
    other = 1 - g
    upper = (d >= 2).astype(jnp.int32)
    mid, edge = 1 + upper, 3 * upper
    far_mid, far_edge = 2 - upper, 3 - 3 * upper
    inner = d == mid
    outer = jnp.logical_not(inner)
    role = 1 - inner.astype(jnp.int32)
    count, cols = cot_ref.shape
    depth = w_hbm.shape[0]
    down_rows, width = down_hbm.shape
    half = cots.shape[1]
    step = cols - half
    extra = half - step
    spare_rows = extra * depth // width
    plane_rows = (down_rows - spare_rows) // 2
    piece_rows = plane_rows // pieces
    chunks = len(spans)

    def at_rows(k, size):
        return pl.ds(pl.multiple_of(k * size, size), size)

    down_load = pltpu.make_async_copy(
        down_hbm, down_all.at[at_rows(d, down_rows)], local_sem.at[0]
    )
    cot_load = pltpu.make_async_copy(cot_hbm, cot_ref, local_sem.at[1])
    w_load = pltpu.make_async_copy(
        w_hbm.at[:, pl.ds(pl.multiple_of(g * step, 128), half)],
        w_all.at[at_rows(d, depth)], local_sem.at[2],
    )
    tokens_load = pltpu.make_async_copy(tokens_hbm, tokens_ref, local_sem.at[3])
    gain_load = pltpu.make_async_copy(gain_hbm, gain_ref, local_sem.at[4])
    counts_load = pltpu.make_async_copy(counts_hbm, counts_ref, local_sem.at[5])

    barrier = pltpu.get_barrier_semaphore()

    def greet(**where):
        pl.semaphore_signal(barrier, inc=1, device_id=where, device_id_type=MESH)

    for plane in range(2):
        for place in (0, 1):
            for who in range(n):
                there = mid if place == 0 else edge
                itself = jnp.logical_and(
                    g == plane, jnp.logical_and(role == place, m == who)
                )
                distant = jnp.logical_and(
                    g != plane,
                    jnp.logical_and(role != place, (m >= 2) != (who >= 2)),
                )
                pl.when(jnp.logical_not(jnp.logical_or(itself, distant)))(
                    lambda plane=plane, there=there, who=who: greet(
                        groups=plane, dp=there, mp=who
                    )
                )
    pl.when(inner)(lambda: greet(dp=far_mid))
    down_load.start()
    cot_load.start()
    w_load.start()
    tokens_load.start()
    gain_load.start()
    counts_load.start()
    down_load.wait()
    pl.when(inner)(lambda: pl.semaphore_wait(barrier, 4 * n - 2))
    pl.when(outer)(lambda: pl.semaphore_wait(barrier, 4 * n - 3))

    def remote(source, target, send, recv, **where):
        return pltpu.make_async_remote_copy(
            src_ref=source, dst_ref=target, send_sem=send, recv_sem=recv,
            device_id=where, device_id_type=MESH,
        )

    def down_span(plane, k):
        if k == pieces:
            return plane_rows, spare_rows
        return plane * (plane_rows + spare_rows) + k * piece_rows, piece_rows

    def down_piece(shard, plane, k):
        start, rows = down_span(plane, k)
        return down_all.at[pl.ds(pl.multiple_of(shard * down_rows + start, 16), rows)]

    def down_copy(way, kind, shard, k, to):
        held = down_piece(shard, g, k)
        return remote(held, held, down_send.at[way], down_recv.at[kind, k], dp=to)

    def down_across(kind, shard, k):
        held = down_piece(shard, g, k)
        return remote(held, held, across_send.at[kind], across_recv.at[kind], groups=other)

    def for_each_plane(body):
        for plane in range(2):
            pl.when(g == plane)(lambda plane=plane: body(plane))

    def moved_rows(shard, plane):
        rows = plane_rows + plane * spare_rows
        start = shard * down_rows + plane * plane_rows
        return down_all.at[pl.ds(pl.multiple_of(start, 16), rows)]

    def down_sent(way):
        def wait(plane):
            held = moved_rows(d, plane)
            remote(
                held, held, down_send.at[way], down_recv.at[0, 0], dp=far_mid
            ).wait_send()

        for_each_plane(wait)

    def crossed(kind, shard, plane):
        held = moved_rows(shard, plane)
        return remote(held, held, across_send.at[kind], across_recv.at[kind], groups=other)

    def each_piece(act):
        for k in range(pieces):
            act(k)
        pl.when(g == 1)(lambda: act(pieces))

    def cot_half(plane):
        return cot_ref.at[:, pl.ds(pl.multiple_of(plane * step, 128), half)]

    def cot_copy(way, source, slot, plane, to):
        return remote(
            source, cots.at[at_rows(slot, count)], cot_send.at[way], cot_recv.at[slot],
            groups=plane, dp=to,
        )

    def cot_across():
        return remote(
            cot_half(other), cot_pass, cot_send.at[2], cot_recv.at[n], groups=other
        )

    def cot_arrival(slot):
        held = cots.at[at_rows(slot, count)]
        return remote(held, held, cot_send.at[0], cot_recv.at[slot], dp=far_mid)

    def w_rows(shard, row, rows):
        return pl.ds(pl.multiple_of(shard * depth + row, 128), rows)

    def w_piece(shard, j):
        row, rows, first, size = spans[j]
        return w_all.at[w_rows(shard, row, rows), pl.ds(first, size)]

    def w_copy(way, kind, shard, j, to):
        held = w_piece(shard, j)
        sem = w_recv.at[2 * chunks] if kind == 1 else w_recv.at[kind // 2 * chunks + j]
        return remote(held, held, w_send.at[way], sem, dp=to)

    def w_moved(way, shard, plane):
        first = plane * extra
        held = w_all.at[at_rows(shard, depth), pl.ds(first, half - first)]
        return remote(held, held, w_send.at[way], w_recv.at[2 * chunks], dp=far_mid)

    def for_chunk(j, act):
        if j == 0:
            pl.when(g == 0)(act)
        else:
            act()

    def keep_cot():
        cots[at_rows(2 * g, count), :] = cot_ref[
            :, pl.ds(pl.multiple_of(g * step, 128), half)
        ]

    def feat_copy(shard, plane, k):
        start, rows = down_span(plane, k)
        return remote(
            down_piece(shard, plane, k),
            down_feat.at[pl.ds(pl.multiple_of(start, 16), rows), at_rows(m, width)],
            feat_send.at[shard], feat_recv.at[m], mp=shard,
        )

    def feat_piece(shard, plane, k):
        pl.when(shard != m)(lambda: feat_copy(shard, plane, k).start())

    def crossed_feat(shard):
        for k in range(pieces):
            feat_piece(shard, other, k)
        pl.when(g == 0)(lambda: feat_piece(shard, other, pieces))

    def feat_whole(sent, arrived):
        held = down_feat.at[:, at_rows(arrived, width)]
        return remote(held, held, feat_send.at[sent], feat_recv.at[arrived], groups=other)

    def keep_feat():
        @pl.loop(0, down_rows // 128)
        def _(k):
            source = m * down_rows + k * 128
            down_feat[at_rows(k, 128), at_rows(m, width)] = down_all[
                pl.ds(pl.multiple_of(source, 128), 128), :
            ]

    early = 4

    @pl.when(inner)
    def _():
        def start_own(k):
            down_copy(0, 1, d, k, far_mid).start()
            down_copy(1, 0, d, k, edge).start()

        each_piece(start_own)
        for k in range(pieces + 1):
            feat_piece(d, 0, k)
        for k in range(pieces):
            feat_piece(d, 1, k)
        cot_load.wait()
        keep_cot()

        @pl.when(g == 1)
        def _():
            for shard in (edge, far_mid, far_edge):
                w_all[at_rows(shard, depth), :extra] = jnp.zeros((depth, extra), w_all.dtype)

        def pass_near(k):
            for kind, sent, shard, way, to in (
                (0, 2, edge, 2, far_mid), (1, 1, far_mid, 3, edge)
            ):
                down_copy(way, kind, shard, k, to).wait_recv()
                down_copy(way, sent, shard, k, to).start()
                down_across(kind, shard, k).start()
                feat_piece(shard, g, k)

        each_piece(pass_near)
        w_load.wait()
        for j in range(chunks):
            for_chunk(j, lambda j=j: w_copy(0, 1, d, j, far_mid).start())

        def pass_far(k):
            down_copy(4, 2, far_edge, k, edge).wait_recv()
            down_copy(4, 2, far_edge, k, edge).start()
            down_across(2, far_edge, k).start()
            feat_piece(far_edge, g, k)

        each_piece(pass_far)
        cot_copy(0, cot_half(other), 2 * g, other, d).start()

    @pl.when(outer)
    def _():
        each_piece(lambda k: down_copy(0, 0, d, k, mid).start())
        cot_load.wait()
        cot_across().start()
        cot_copy(0, cot_half(g), 2 * g + 1, g, mid).start()
        for k in range(pieces + 1):
            feat_piece(d, 0, k)
        for k in range(pieces):
            feat_piece(d, 1, k)
        w_load.wait()
        for kind, shard in enumerate((mid, far_mid, far_edge)):

            def take(k):
                down_copy(0, kind, shard, k, mid).wait_recv()
                down_across(kind, shard, k).start()
                feat_piece(shard, g, k)

            each_piece(take)
            if kind == 0:
                cot_across().wait_recv()
                cot_copy(1, cot_pass, 2 * other + 1, g, mid).start()
                for j in range(early):
                    for_chunk(j, lambda j=j: w_copy(0, 0, d, j, mid).start())

    neighbours = (jnp.where(inner, edge, mid), far_mid, far_edge)
    for kind, shard in enumerate(neighbours):
        for_each_plane(lambda plane: crossed(kind, shard, 1 - plane).wait_recv())
        if kind < 2:
            crossed_feat(shard)

    tokens_load.wait()
    gain_load.wait()
    counts_load.wait()
    raw_ref[...] = jnp.zeros_like(raw_ref)

    @pl.loop(0, 2 * n)
    def _(c):
        at = at_rows(c, down_rows // 2)
        raw_ref[...] += jnp.dot(
            tokens_ref[:, at], down_all[at, :], preferred_element_type=jnp.float32
        )

    def to_peer(sent, arrived, source, target, mp):
        return remote(source, target, small_send.at[sent], small_recv.at[arrived], mp=mp)

    raw = raw_ref[...]
    square_out[...] = jnp.broadcast_to(
        jnp.sum(raw * raw, axis=1, keepdims=True), (count, 128)
    ).T[:8]
    for o in range(1, n):
        to_peer(0, 0, square_out, square_in.at[o - 1], lax.rem(m + o, n)).start()
    to_peer(0, 0, square_in, square_in, far_mid).wait_recv()
    value = square_out[...]
    for o in range(1, n):
        value += square_in[o - 1]
    squares = jnp.broadcast_to(value[:1], (128, count)).T[:, :1]
    root = jnp.sqrt(squares / (width * n) + 1e-06)
    root_ref[...] = jnp.broadcast_to(root, root_ref.shape)
    gain = gain_ref[...].reshape(1, width)
    latent_out[...] = (raw / root * gain).astype(latent_out.dtype)

    def latent_at(slot, who):
        return latents.at[at_rows(slot, count), at_rows(who, width)]

    def latent_inward(to):
        return remote(
            latent_out, latent_at(2 * g + role, m), latent_send.at[to],
            latent_recv.at[2 * g + role], groups=to, dp=mid,
        )

    def latent_arrival(slot):
        held = latent_at(slot, m)
        return remote(held, held, latent_send.at[0], latent_recv.at[slot], dp=far_mid)

    def latent_spread(slot, o):
        held = latent_at(slot, m)
        return remote(
            held, held, latent_send.at[2], latent_recv.at[n], mp=lax.rem(m + o, n)
        )

    def latents_spread():
        held = latents.at[:, pl.ds(0, (n - 1) * width)]
        return remote(held, held, latent_send.at[2], latent_recv.at[n], dp=far_mid)

    slots = (2 * g, 2 * other, 2 * g + 1, 2 * other + 1)

    cut = depth - 128
    grad_parts = ((0, cut), (cut, 128))

    def add_grad(sum_ref, shard, row, rows, t):
        at = at_rows(t, tile)
        sum_ref[:, row:row + rows] += contract_last(
            cots[:, at], w_all[w_rows(shard, row, rows), at]
        )

    def grad_copy(shard, slot, part):
        row, rows = grad_parts[part]
        return remote(
            grad_out.at[at_rows(slot, count), w_rows(shard, row, rows)],
            grad_in.at[g * n + m, :, pl.ds(row, rows)],
            grad_send.at[0], grad_recv.at[0],
            groups=slot // 2, dp=mid if slot % 2 == 0 else edge, mp=shard,
        )

    def is_self(shard, slot):
        return jnp.logical_and(g == slot // 2, m == shard)

    def each_grad(shard, part, act):
        for slot in range(n):
            if slot % 2 == 1:
                act(grad_copy(shard, slot, part))
                continue
            pl.when(jnp.logical_not(is_self(shard, slot)))(
                lambda slot=slot: act(grad_copy(shard, slot, part))
            )

    half_count = count // 2
    late_owners = (far_edge, lax.rem(far_edge + 2, n))

    def late_copy(slot, side, part):
        row, rows = grad_parts[part]
        source = pl.ds(pl.multiple_of(slot * count + side * half_count, 16), half_count)
        return remote(
            grad_out.at[source, w_rows(far_edge, row, rows)],
            late_in.at[g * n + m, :, pl.ds(row, rows)],
            grad_send.at[2], grad_recv.at[2], groups=slot // 2,
            dp=mid if slot % 2 == 0 else edge, mp=late_owners[side],
        )

    def send_late(sum_ref, part):
        row, rows = grad_parts[part]
        grad_out[:, w_rows(far_edge, row, rows)] = sum_ref[:, row:row + rows].astype(
            grad_out.dtype
        )
        for slot in range(n):
            for side in range(2):
                if slot % 2 == 1:
                    late_copy(slot, side, part).start()
                    continue
                itself = is_self(late_owners[side], slot)
                pl.when(jnp.logical_not(itself))(
                    lambda slot=slot, side=side: late_copy(slot, side, part).start()
                )
        for side in range(2):

            @pl.when(m == late_owners[side])
            def _():
                source = pl.ds(
                    pl.multiple_of(2 * g * count + side * half_count, 16), half_count
                )
                late_in[g * n + m, :, row:row + rows] = grad_out[
                    source, w_rows(far_edge, row, rows)
                ]

    def send_grad(sum_ref, shard, part):
        row, rows = grad_parts[part]
        grad_out[:, w_rows(shard, row, rows)] = sum_ref[:, row:row + rows].astype(
            grad_out.dtype
        )
        each_grad(shard, part, lambda c: c.start())

        @pl.when(m == shard)
        def _():
            grad_in[g * n + m, :, row:row + rows] = grad_out[
                at_rows(2 * g, count), w_rows(shard, row, rows)
            ]

    def whole_grad(shard):
        total[...] = jnp.zeros_like(total)

        @pl.loop(0, half // tile)
        def _(t):
            add_grad(total, shard, 0, depth, t)

        for part in range(2):
            send_grad(total, shard, part)

    def query_parts(j):
        row, rows, first, size = spans[j]
        if row + rows < depth:
            return ()
        return ((first, size, j == 0),)

    def query_copy(slot, first, size):
        return remote(
            query_out.at[at_rows(slot, count), pl.ds(first, size)],
            queries_ref.at[:, pl.ds(pl.multiple_of(g * step + first, 128), size)],
            query_sem.at[2], query_sem.at[g],
            groups=slot // 2, dp=mid if slot % 2 == 0 else edge,
        )

    def query_keep(first, size):
        return pltpu.make_async_copy(
            query_out.at[at_rows(2 * g, count), pl.ds(first, size)],
            queries_ref.at[:, pl.ds(pl.multiple_of(g * step + first, 128), size)],
            query_sem.at[3],
        )

    def send_queries(j):
        for first, size, once in query_parts(j):

            def act():
                for slot in range(n):
                    if slot % 2 == 1:
                        query_copy(slot, first, size).start()
                        continue
                    mine = g == slot // 2
                    pl.when(jnp.logical_not(mine))(
                        lambda slot=slot: query_copy(slot, first, size).start()
                    )
                query_keep(first, size).start()

            if once:
                pl.when(g == 0)(act)
            else:
                act()

    def keep_row(t):
        column = lax.broadcasted_iota(jnp.int32, (1, tile), 1) + (g * step + t * tile)
        return (column < counts_ref[m] * HD).astype(jnp.float32)

    ends = sum(row > 0 for row, rows, first, size in spans)
    first_late = min(first for row, rows, first, size in spans if row > 0)

    def late_at(t):
        return pl.ds(pl.multiple_of(t * tile - first_late, tile), tile)

    def query_sum(shard, row, rows, at):
        return jnp.dot(
            latents[:, w_rows(shard, row, rows)], w_all[w_rows(shard, row, rows), at],
            preferred_element_type=jnp.float32,
        )

    def query_start(t):
        at = at_rows(t, tile)
        product = query_sum(far_edge, 0, cut, at)
        for shard in (d, edge, far_mid):
            product += query_sum(shard, 0, depth, at)
        query_part[:, late_at(t)] = product

    def query_end(t):
        at = at_rows(t, tile)
        finish_query(t, query_part[:, late_at(t)] + query_sum(far_edge, cut, depth - cut, at))

    def query_tile(t):
        at = at_rows(t, tile)
        finish_query(
            t, jnp.dot(latents[...], w_all[:, at], preferred_element_type=jnp.float32)
        )

    def finish_query(t, product):
        at = at_rows(t, tile)
        query_out[:, at] = (product * keep_row(t)).astype(query_out.dtype)
        dots = product * cots[:, at].astype(jnp.float32)
        for part in range(tile // 128):
            dot_total[...] += dots[:, part * 128:(part + 1) * 128]

    def dot_copy(slot, to):
        return remote(
            dot_out.at[slot], dot_in.at[g * n + m], grad_send.at[1], grad_recv.at[1],
            groups=slot // 2,
            dp=mid if slot % 2 == 0 else edge, mp=to,
        )

    def each_dot(act):
        for slot in range(n):
            for to in range(n):
                if slot % 2 == 1:
                    act(dot_copy(slot, to))
                    continue
                pl.when(jnp.logical_not(is_self(to, slot)))(
                    lambda slot=slot, to=to: act(dot_copy(slot, to))
                )

    def send_dots():
        for slot in range(n):
            column = jnp.sum(dot_total[at_rows(slot, count), :], axis=1, keepdims=True)
            dot_out[slot] = jnp.broadcast_to(column, (count, 128)).T[:8]
        each_dot(lambda c: c.start())
        dot_in[g * n + m] = dot_out[2 * g]

    def finish_chunk(j):
        row, rows, first, size = spans[j]
        for_chunk(j, w_copy(0, 2, far_edge, j, far_mid).wait_recv)
        if j == 0:
            return
        if j == 1:
            first, size = 0, first + size

        @pl.loop(first // tile, (first + size) // tile)
        def _(t):
            add_grad(last_total, far_edge, row, rows, t)

        if row == 0 and rows == cut:
            send_late(last_total, 0)
        if j == chunks - 1:
            send_late(last_total, 1)
        body = query_tile if rows == depth else query_end if row > 0 else query_start
        pl.loop(first // tile, (first + size) // tile)(body)
        if j == chunks - 1:
            send_dots()
        if row > 0 and j < chunks - 1:
            return
        for i in range(j if row == 0 else chunks - ends, j + 1):
            if i == 1:
                send_queries(0)
            send_queries(i)

    def gathered(sem, held):
        return remote(held, held, grad_send.at[sem], grad_recv.at[sem], groups=other)

    def all_sources(sem, buffer):
        pl.when(inner)(lambda: gathered(sem, buffer.at[pl.ds(0, 2 * n - 1)]).wait_recv())
        pl.when(outer)(lambda: gathered(sem, buffer).wait_recv())

    late = m == far_edge

    def own_block():
        all_sources(0, grad_in)
        grad_latent = grad_in[0].astype(jnp.float32)
        for source in range(1, 2 * n):
            grad_latent += grad_in[source].astype(jnp.float32)
        return gain_ref[...].reshape(1, width) * grad_latent / root_ref[:, :1]

    def to_others(sem, held):
        return [
            remote(held, held, peer_send.at[sem], peer_recv.at[sem], mp=lax.rem(m + o, n))
            for o in (2, 1, 3)
        ]

    def from_others(sem, buffer, blocks):
        held = buffer.at[pl.ds(0, blocks)]
        return remote(held, held, peer_send.at[sem], peer_recv.at[sem], groups=other)

    def early_block(ready):
        @pl.when(jnp.logical_and(jnp.logical_not(late), ready))
        def _():
            block_all[m] = own_block()
            for c in to_others(1, block_all.at[m]):
                c.start()

    gain_copy = remote(
        gain_ref, gain_far, peer_send.at[3], peer_recv.at[3], mp=lax.rem(m + 2, n)
    )

    def start_raw():
        gain_copy.start()
        raw_all[m] = raw_ref[...]
        for c in to_others(0, raw_all.at[m]):
            c.start()

    @pl.when(outer)
    def _():
        latent_inward(0).start()
        latent_inward(1).start()
        for j in range(early, chunks):
            for_chunk(j, lambda j=j: w_copy(0, 0, d, j, mid).start())
        crossed_feat(far_edge)
        start_raw()
        keep_feat()

    def pass_on(j):
        def act():
            w_copy(0, 0, edge, j, far_mid).wait_recv()
            w_copy(1, 2, edge, j, far_mid).start()

        for_chunk(j, act)

    @pl.when(inner)
    def _():
        latents[at_rows(2 * g, count), at_rows(m, width)] = latent_out[...]
        latent_inward(other).start()
        for o in range(1, n):
            latent_spread(slots[0], o).start()
        crossed_feat(far_edge)
        keep_feat()
        for j in range(early):
            pass_on(j)
        for slot in slots[1:]:
            latent_arrival(slot).wait_recv()
            for o in range(1, n):
                latent_spread(slot, o).start()

        for slot in slots[1:]:
            cot_arrival(slot).wait_recv()

        @pl.loop(0, half // tile)
        def _(t):
            at = at_rows(t, tile)
            cots[:, at] = cots[:, at] * keep_row(t).astype(cots.dtype)

        @pl.when(g == 1)
        def _():
            cots[:, :extra] = jnp.zeros((n * count, extra), cots.dtype)

        whole_grad(d)
        for_each_plane(lambda plane: w_moved(0, far_mid, plane).wait_recv())
        whole_grad(far_mid)
        latents_spread().wait_recv()
        start_raw()
        last_total[...] = jnp.zeros_like(last_total)
        dot_total[...] = jnp.zeros_like(dot_total)
        passed = early
        for j in range(chunks):
            for _ in range(min((0, 1, 2)[j] if j < 3 else chunks, chunks - passed)):
                pass_on(passed)
                passed += 1
            finish_chunk(j)
            if j == 3:
                whole_grad(edge)
            if j == 2:
                early_block(m != edge)
            if j == 5:
                early_block(m == edge)

    to_peer(0, 0, square_in, square_in, far_mid).wait_send()
    for o in range(1, n):
        feat_whole(lax.rem(m + o, n), m).wait_send()
        feat_whole(m, lax.rem(m + o, n)).wait_recv()
    for kind, shard in enumerate(neighbours):
        for_each_plane(lambda plane: crossed(kind, shard, plane).wait_send())
    down_sent(0)
    cot_copy(0, cot_half(g), 2 * g, g, mid).wait_send()

    def w_own_sent(plane):
        w_moved(0, d, plane).wait_send()

    for_each_plane(w_own_sent)
    latent_inward(other).wait_send()

    @pl.when(outer)
    def _():
        cot_copy(1, cot_half(g), 2 * g, g, mid).wait_send()
        cot_across().wait_send()
        latent_inward(g).wait_send()

    @pl.when(inner)
    def _():
        for way in range(1, 5):
            down_sent(way)
        latents_spread().wait_send()

    early_block(outer)
    all_sources(1, dot_in)
    dots = dot_in[0]
    for source in range(1, 2 * n):
        dots += dot_in[source]
    inner_dot = jnp.broadcast_to(dots[:1], (128, count)).T[:, :1]
    root = root_ref[:, :1]
    slope = inner_dot / (width * n * (root * root))

    slope_ref[...] = jnp.broadcast_to(slope, slope_ref.shape)
    owner = jnp.logical_or(m == late_owners[0], m == late_owners[1])
    visitor = jnp.logical_not(owner)
    mine = pl.ds(
        pl.multiple_of((1 - late.astype(jnp.int32)) * half_count, half_count), half_count
    )
    gain_copy.wait_recv()
    from_others(0, raw_all, n - 1).wait_recv()

    @pl.when(owner)
    def _():
        all_sources(2, late_in)
        summed = late_in[0].astype(jnp.float32)
        for source in range(1, 2 * n):
            summed += late_in[source].astype(jnp.float32)
        gain = jnp.where(late, gain_ref[...].reshape(1, width), gain_far[...].reshape(1, width))
        value = gain * summed / root_ref[mine, :1]
        value -= raw_all[far_edge, mine, :] * slope_ref[mine, :1]
        grad_all[far_edge, mine, :] = value.astype(grad_all.dtype)
        for c in to_others(2, grad_all.at[far_edge, mine, :]):
            c.start()

    row_tile = down_rows

    def add_block(who, first, last):
        @pl.loop(0, down_rows // row_tile)
        def _(c):
            rows = at_rows(c, row_tile)
            value = contract_last(grad_all[who], down_feat[rows, at_rows(who, width)])
            if not first:
                value += token_total[:, rows]
            if last:
                token_out[:, rows] = value.astype(token_out.dtype)
            else:
                token_total[:, rows] = value

    pl.when(late)(lambda: from_others(1, block_all, n - 1).wait_recv())
    pl.when(jnp.logical_not(late))(lambda: from_others(1, block_all, n - 2).wait_recv())
    for who in (1, 2, edge):
        grad_all[who] = (block_all[who] - raw_all[who] * slope).astype(grad_all.dtype)
        add_block(who, isinstance(who, int) and who == 1, False)

    pl.when(visitor)(lambda: from_others(2, grad_all, 1).wait_recv())
    theirs = pl.ds(pl.multiple_of(late.astype(jnp.int32) * half_count, half_count), half_count)

    def other_half():
        held = grad_all.at[far_edge, theirs, :]
        return remote(held, held, peer_send.at[2], peer_recv.at[2], groups=other)

    pl.when(owner)(lambda: other_half().wait_recv())
    add_block(far_edge, False, True)
    token_keep = pltpu.make_async_copy(token_out, grad_tokens_ref, local_sem.at[0])
    token_keep.start()

    def query_arrival(plane):
        first = plane * cols - plane * (half - extra)
        part = queries_ref.at[:, pl.ds(first, half - plane * extra)]
        return remote(part, part, query_sem.at[2], query_sem.at[plane], groups=other)

    for plane in range(2):
        away = jnp.logical_not(jnp.logical_and(inner, g == plane))
        pl.when(away)(lambda plane=plane: query_arrival(plane).wait_recv())

    @pl.when(inner)
    def _():
        for_each_plane(lambda plane: w_moved(1, edge, plane).wait_send())
        for plane in range(2):

            @pl.when(g == plane)
            def _():
                size = half - plane * extra
                part = query_out.at[pl.ds(0, (n - 1) * count), pl.ds(0, size)]
                remote(
                    part, part, query_sem.at[2], query_sem.at[plane], groups=other
                ).wait_send()
                query_keep(half - size, size).wait()

        def early_sent(blocks):
            held = down_all.at[pl.ds(0, blocks * count), pl.ds(0, depth)]
            gathered(0, held).wait_send()

        pl.when(late)(lambda: early_sent(3 * n))
        pl.when(jnp.logical_not(late))(lambda: early_sent(3 * n - 1))
        pl.when(owner)(lambda: gathered(2, late_in.at[pl.ds(0, 2 * n - 1)]).wait_send())
        pl.when(visitor)(lambda: gathered(2, late_in).wait_send())
        gathered(1, raw_ref.at[pl.ds(0, (n * n - 1) * 8), pl.ds(0, 128)]).wait_send()

    from_others(0, raw_all, n - 1).wait_send()
    pl.when(jnp.logical_not(late))(lambda: from_others(1, block_all, n - 1).wait_send())
    pl.when(owner)(lambda: from_others(2, late_in, n - 1).wait_send())
    gain_copy.wait_send()
    token_keep.wait()


def project(tokens, w_down, gain, w_up, head_counts, cotangent):
    n = lax.axis_size("dp")
    count, cols = cotangent.shape
    depth = w_up.shape[0]
    down_rows, width = w_down.shape
    half = (cols // 128 + 1) // 2 * 128
    tile = 256 if half % 256 == 0 else 128
    tiles = half // tile
    ends = min(2, tiles - 1)
    body = tiles - ends
    sizes = []
    while sum(sizes) < body:
        left = body - sum(sizes)
        sizes.append(min(2, left))
    parts = len(sizes)
    cut = depth - 128
    spans = [(0, depth, sum(sizes[:i]) * tile, sizes[i] * tile) for i in range(parts)]
    extra = 2 * half - cols
    spans[0] = (0, depth, extra, sizes[0] * tile - extra)
    spans.insert(0, (0, depth, 0, extra))
    spans.append((0, cut, body * tile, ends * tile))
    for i in range(ends):
        spans.append((cut, 128, (body + i) * tile, tile))
    spans = tuple(spans)
    parts = len(spans)
    pieces = 2
    hbm = pl.BlockSpec(memory_space=pl.ANY)
    bf16, f32 = jnp.bfloat16, jnp.float32
    dma = pltpu.SemaphoreType.DMA
    return pl.pallas_call(
        functools.partial(project_kernel, n, spans, tile, pieces),
        out_shape=(
            jax.ShapeDtypeStruct((count, cols), bf16),
            jax.ShapeDtypeStruct((count, down_rows), bf16),
        ),
        in_specs=[hbm] * 6,
        out_specs=(hbm, hbm),
        scratch_shapes=[
            pltpu.VMEM(gain.shape, f32),
            pltpu.SMEM(head_counts.shape, jnp.int32),
            pltpu.VMEM(tokens.shape, bf16),
            pltpu.VMEM((count, cols), bf16),
            pltpu.VMEM((count, half), bf16),
            pltpu.VMEM((n * down_rows, width), bf16),
            pltpu.VMEM((down_rows, n * width), bf16),
            pltpu.VMEM((n * depth, half), bf16),
            pltpu.VMEM((n * count, half), bf16),
            pltpu.VMEM((n * count, half), bf16),
            pltpu.VMEM((n * count, n * width), bf16),
            pltpu.VMEM((count, width), bf16),
            pltpu.VMEM((n * count, n * depth), bf16),
            pltpu.VMEM((2 * n, count, depth), bf16),
            pltpu.VMEM((2 * n, count // 2, depth), bf16),
            pltpu.VMEM(gain.shape, f32),
            pltpu.VMEM((count, 128), f32),
            pltpu.VMEM((n * count, depth), f32),
            pltpu.VMEM((n * count, depth), f32),
            pltpu.VMEM((count, width), f32),
            pltpu.VMEM((count, 128), f32),
            pltpu.VMEM((8, count), f32),
            pltpu.VMEM((n - 1, 8, count), f32),
            pltpu.VMEM((n * count, 128), f32),
            pltpu.VMEM((n, 8, count), f32),
            pltpu.VMEM((2 * n, 8, count), f32),
            pltpu.VMEM((n, count, width), f32),
            pltpu.VMEM((n, count, width), f32),
            pltpu.VMEM((n, count, width), bf16),
            pltpu.VMEM((n * count, ends * tile), f32),
            pltpu.VMEM((count, down_rows), f32),
            pltpu.VMEM((count, down_rows), bf16),
            dma((6,)),
            dma((5,)),
            dma((3, pieces + 1)),
            dma((3,)),
            dma((3,)),
            dma((n,)),
            dma((n,)),
            dma((3,)),
            dma((n + 1,)),
            dma((3,)),
            dma((n + 1,)),
            dma((2,)),
            dma((2 * parts + 1,)),
            dma((4,)),
            dma((3,)),
            dma((3,)),
            dma((1,)),
            dma((1,)),
            dma((4,)),
            dma((4,)),
        ],
        compiler_params=pltpu.CompilerParams(
            collective_id=0, has_side_effects=True, vmem_limit_bytes=60 * 2**20
        ),
    )(tokens, w_down, gain, w_up, head_counts, cotangent)


def store_kernel(parts, queries_in, grad_in, queries_out, grad_out, held, grad, sem):
    rows = held.shape[0] // parts

    def span(k):
        return pl.ds(k * rows, rows)

    reads = [
        pltpu.make_async_copy(queries_in.at[span(k)], held.at[span(k)], sem.at[0, k])
        for k in range(parts)
    ] + [pltpu.make_async_copy(grad_in, grad, sem.at[0, parts])]
    writes = [
        pltpu.make_async_copy(held.at[span(k)], queries_out.at[span(k)], sem.at[1, k])
        for k in range(parts)
    ] + [pltpu.make_async_copy(grad, grad_out, sem.at[1, parts])]
    for read in reads:
        read.start()
    for read, write in zip(reads, writes):
        read.wait()
        write.start()
    for write in writes:
        write.wait()


def store(queries, grad_tokens):
    parts = 4
    hbm = pl.BlockSpec(memory_space=pl.ANY)
    return pl.pallas_call(
        functools.partial(store_kernel, parts),
        out_shape=(
            jax.ShapeDtypeStruct(queries.shape, queries.dtype),
            jax.ShapeDtypeStruct(grad_tokens.shape, grad_tokens.dtype),
        ),
        in_specs=[hbm] * 2,
        out_specs=(hbm,) * 2,
        scratch_shapes=[
            pltpu.VMEM(queries.shape, queries.dtype),
            pltpu.VMEM(grad_tokens.shape, grad_tokens.dtype),
            pltpu.SemaphoreType.DMA((2, parts + 1)),
        ],
    )(queries, grad_tokens)


def move_weights_body(tokens, w_down, gain, w_up, head_counts, cotangent):
    return store(*project(tokens, w_down, gain, w_up, head_counts, cotangent))


def solution(mesh):
    in_specs = (
        P(("groups", "dp"), None),
        P("dp", "mp"),
        P("mp"),
        P("dp", "mp"),
        P(),
        P(("groups", "dp"), "mp"),
    )
    out_specs = (P(("groups", "dp"), "mp"), P(("groups", "dp"), "mp"))
    square = mesh.shape["dp"] == mesh.shape["mp"] == 4 and mesh.shape["groups"] == 2
    body = move_weights_body if square else gather_weights_body
    return jax.shard_map(body, mesh=mesh, in_specs=in_specs, out_specs=out_specs, check_vma=False)
```
